128 devices in a mesh: tm: 4 (over x), space: 32 (over z, y, core).
Axes of the slice: x: 4, y: 4, z: 4, core: 2. Of those that a mesh axis runs over, the one named last changes fastest.
Arguments:
- source: float32 [32, 2048, 1024], P('tm', 'space'), may hold values from -6 to 6
- guess: float32 [32, 2048, 1024], P('tm', 'space'), may hold values from -6 to 6
- start_state: float32 [2048, 1024], P('space'), may hold values from -6 to 6
- conduct: float32 [2048, 1024], P('space'), may hold values from 0.5 to 4
Outputs:
- solution_field: float32 [32, 2048, 1024], P('tm', 'space')
- residual: float32 [32, 2048, 1024], P('tm', 'space')
The draws below stay inside these ranges and needn't reach their ends.
All inputs are finite; a program needn't handle non-finite values.
Results may differ from the reference program's by a relative error of at most 0.00002.
Values sent between devices are 32-bit elements; how exact they have to be, the bound alone decides.
No kernel may reach another device: no remote copies, remote signals or barrier semaphores. Data moves between devices by JAX's collectives and lax.ppermute only.
A program may use at most 64 MiB of HBM per device.

```python
import math
import jax
import jax.numpy as jnp

COLS = 1024
NT = 32
NR = 2048


def levels(rng, extent, cuts, smallest, high):
    loudness = 1.0
    for position, blocks in cuts:
        heights = jax.random.uniform(jax.random.fold_in(jax.random.fold_in(rng, 6), position), (blocks,), jnp.float32, smallest / len(cuts), high / len(cuts))
        loudness = loudness * jnp.repeat(jnp.exp(heights), extent[position] // blocks).reshape((-1,) + (1,) * (len(extent) - 1 - position))
    return loudness


def normal_values(rng, extent, width, reach, pieces=(), kind=jnp.bfloat16):
    entries = width * jax.random.normal(rng, extent, jnp.float32)
    if pieces:
        entries = entries * levels(rng, extent, pieces, -0.22, 0.18)
    return jnp.clip(entries, -reach, reach).astype(kind)


def setup_inputs(seed: int = 0) -> dict:
    key_list = jax.random.split(jax.random.key(seed), 5)
    source = normal_values(key_list[0], (NT, NR, COLS), 1.0, 6.0, ((0, 4), (1, 32)), jnp.float32)
    guess = normal_values(key_list[1], (NT, NR, COLS), 1.0, 6.0, ((0, 4), (1, 32)), jnp.float32)
    start_state = normal_values(key_list[2], (NR, COLS), 1.0, 6.0, ((0, 32),), jnp.float32)
    conduct = jnp.clip(jnp.exp(math.log(4.0) - 2.0794415 * jax.random.uniform(key_list[3], (NR, COLS), jnp.float32) ** levels(key_list[3], (NR, COLS), ((0, 32),), -0.2, 0.2)), 0.5, 4.0)
    return dict(source=source, guess=guess, start_state=start_state, conduct=conduct)


damping = 0.8


def apply_operator(field, conduct):
    padded = jnp.pad(field, ((0, 0), (1, 1), (1, 1)))
    beside = padded[:, 2:, 1:-1] + padded[:, :-2, 1:-1] + padded[:, 1:-1, 2:] + padded[:, 1:-1, :-2]
    return field + conduct * (4.0 * field - beside)


def approx_inverse(resid, conduct):
    diagonal = 1.0 + 4.0 * conduct
    first_sweep = resid / diagonal
    return first_sweep + (resid - apply_operator(first_sweep, conduct)) / diagonal


def fine_residual(field, before, source, conduct):
    earlier = jnp.concatenate([before[None], field[:-1]], axis=0)
    return source + earlier - apply_operator(field, conduct)


def shifted(coarse):
    return jnp.concatenate([jnp.zeros_like(coarse[:1]), coarse[:-1]], axis=0)


def reference(source, guess, start_state, conduct):
    resid0 = fine_residual(guess, start_state, source, conduct)
    smooth1 = guess + damping * approx_inverse(resid0, conduct)
    resid1 = fine_residual(smooth1, start_state, source, conduct)
    half_steps = source.shape[0] // 2
    pairs = resid1.reshape(half_steps, 2, source.shape[1], source.shape[2])
    restricted = pairs[:, 0] + pairs[:, 1]
    coarse_cond = 2.0 * conduct
    correction = damping * approx_inverse(restricted, coarse_cond)
    for sweep in range(2):
        defect = restricted + shifted(correction) - apply_operator(correction, coarse_cond)
        correction = correction + damping * approx_inverse(defect, coarse_cond)
    even_steps = 0.5 * (shifted(correction) + correction)
    fine_corr = jnp.stack([even_steps, correction], axis=1).reshape(source.shape)
    smooth2 = smooth1 + fine_corr
    resid2 = fine_residual(smooth2, start_state, source, conduct)
    smooth3 = smooth2 + damping * approx_inverse(resid2, conduct)
    resid3 = fine_residual(smooth3, start_state, source, conduct)
    return smooth3, resid3
```

```python
import jax
import jax.numpy as jnp
from jax import lax
from jax.experimental import pallas as pl
from jax.experimental.pallas import tpu as pltpu
from jax.sharding import PartitionSpec as P


F32 = jnp.float32
ROWS = 64
HALO = 11
EXT = ROWS + 2 * HALO
DAMP = 0.8
C, D, INV, Q, K, KD, KINV, KQ, ST = range(9)
FULL = pl.BlockSpec(memory_space=pltpu.VMEM)
SMEM = pl.BlockSpec(memory_space=pltpu.SMEM)
ANY = pl.BlockSpec(memory_space=pl.ANY)


def ext(steps):
    return jax.ShapeDtypeStruct((steps, EXT, 8, 128), F32)


def rows_of(count):
    return jax.ShapeDtypeStruct((count, 8, 128), F32)


def view(x):
    steps = x.shape[0]
    return x.reshape(steps, ROWS // 8, 8, 8, 128).transpose(0, 1, 3, 2, 4).reshape(steps * ROWS * 8, 128)


def unview(y, steps):
    return y.reshape(steps, ROWS // 8, 8, 8, 128).transpose(0, 1, 3, 2, 4).reshape(steps, ROWS, 1024)


def at(ref, step, row):
    return ref[pl.ds(step * ROWS * 8 + (row // 8) * 64 + row % 8, 8, 8), :]


def tile_at(step, tile, row):
    return pl.ds(step * ROWS * 8 + tile * 64 + row, 8, 8)


def beside_maker():
    lane = lax.broadcasted_iota(jnp.int32, (8, 128), 1)
    sub = lax.broadcasted_iota(jnp.int32, (8, 128), 0)
    first, last = lane == 0, lane == 127
    top, bottom = sub == 0, sub == 7

    def beside(x):
        before = jnp.where(top, 0.0, pltpu.roll(x, 1, 0))
        after = jnp.where(bottom, 0.0, pltpu.roll(x, 7, 0))
        return pltpu.roll(jnp.where(last, before, x), 1, 1) + pltpu.roll(jnp.where(first, after, x), 127, 1)

    return beside


def around(beside, ref, step, r):
    return ref[step, r - 1] + ref[step, r + 1] + beside(ref[step, r])


def sweep(low, high, unroll, body):
    low, high = low + HALO, high + HALO
    count = high - low
    unroll = min(unroll, count)
    blocks = -(-count // unroll)
    if blocks == 1:
        for j in range(unroll):
            body(low + j)
        return

    def step(i, carry):
        start = jnp.minimum(low + i * unroll, high - unroll)
        for j in range(unroll):
            body(start + j)
        return carry

    lax.fori_loop(0, blocks, step, 0)


def coefficients(co, r, c):
    diag = 1.0 + 4.0 * c
    coarse = 1.0 + 8.0 * c
    recip = 1.0 / diag
    coarse_recip = 1.0 / coarse
    co[C, r] = c
    co[D, r] = diag
    co[INV, r] = DAMP * recip
    co[Q, r] = c * recip
    co[K, r] = 2.0 * c
    co[KD, r] = coarse
    co[KINV, r] = DAMP * coarse_recip
    co[KQ, r] = 2.0 * c * coarse_recip


class Stages:
    def __init__(self, beside, co):
        self.beside, self.co = beside, co

    def fine_defect(self, out, field, earlier, source, steps):
        def body(r):
            c, d, inv = self.co[C, r], self.co[D, r], self.co[INV, r]
            for t in steps:
                out[t, r] = (source[t, r] + earlier(t, r) - d * field[t, r] + c * around(self.beside, field, t, r)) * inv

        return body

    def coarse_defect(self, out, field, earlier, rhs, steps):
        def body(r):
            k, kd, kinv = self.co[K, r], self.co[KD, r], self.co[KINV, r]
            for m in steps:
                out[m, r] = (rhs[m, r] + earlier(m, r) - kd * field[m, r] + k * around(self.beside, field, m, r)) * kinv

        return body

    def smoothed(self, out, field, defect, steps, plane):
        def body(r):
            q = self.co[plane, r]
            for t in steps:
                base = defect[t, r] if field is None else field[t, r] + defect[t, r]
                out[t, r] = base + q * around(self.beside, defect, t, r)

        return body

    def restricted(self, out, scaled, field, earlier, source, pairs):
        def body(r):
            c, d, kinv = self.co[C, r], self.co[D, r], self.co[KINV, r]
            for m in pairs:
                parts = [
                    source[t, r] + earlier(t, r) - d * field[t, r] + c * around(self.beside, field, t, r)
                    for t in (2 * m, 2 * m + 1)
                ]
                both = parts[0] + parts[1]
                out[m, r] = both
                scaled[m, r] = both * kinv

        return body


def edge_pack(is_first, guess, source, start, conduct, top, bottom):
    for out, low in ((top, 0), (bottom, ROWS - HALO)):
        for j in range(HALO):
            for t in range(8):
                out[t, j] = at(guess, t, low + j)
                out[8 + t, j] = at(source, t, low + j)
            out[16, j] = at(conduct, 0, low + j)
            out[17, j] = at(start, 0, low + j) * is_first[0]


def last_step_pack(guess, source, conduct, out, g, e):
    beside = beside_maker()

    def fill(i, carry):
        for j in range(8):
            r = 8 * i + j
            for t in (6, 7):
                g[t - 6, r] = guess[tile_at(t, i, j), :]
            out[r] = g[1, r]
        return carry

    lax.fori_loop(0, ROWS // 8, fill, 0)

    def cond_at(r):
        return conduct[pl.ds((r // 8) * 64 + r % 8, 8, 8), :]

    def defect(i, carry):
        start = jnp.minimum(1 + i * 16, 63 - 16)
        for j in range(16):
            r = start + j
            c = cond_at(r)
            d = 1.0 + 4.0 * c
            right = source[pl.ds(7 * 512 + (r // 8) * 64 + r % 8, 8, 8), :]
            e[r] = (right + g[0, r] - d * g[1, r] + c * around(beside, g, 1, r)) * (DAMP / d)
        return carry

    lax.fori_loop(0, 4, defect, 0)

    def smooth(i, carry):
        start = jnp.minimum(2 + i * 16, 62 - 16)
        for j in range(16):
            r = start + j
            c = cond_at(r)
            q = c / (1.0 + 4.0 * c)
            out[ROWS - 2 + r] = g[1, r] + e[r] + q * (e[r - 1] + e[r + 1] + beside(e[r]))
        return carry

    lax.fori_loop(0, 4, smooth, 0)


def interior(is_first, guess, source, start, conduct, g, s, co, u, rs, e0, e1, e2, tmp):
    beside = beside_maker()

    def fill(i, carry):
        for j in range(8):
            r = HALO + 8 * i + j
            for t in range(8):
                g[t, r] = guess[tile_at(t, i, j), :]
                s[t, r] = source[tile_at(t, i, j), :]
            coefficients(co, r, conduct[tile_at(0, i, j), :])
            co[ST, r] = start[tile_at(0, i, j), :] * is_first[0]
        return carry

    lax.fori_loop(0, ROWS // 8, fill, 0)
    st = Stages(beside, co)
    sweep(1, 63, 8, st.fine_defect(tmp, g, lambda t, r: g[t - 1, r], s, range(1, 8)))
    sweep(2, 62, 8, st.smoothed(u, g, tmp, range(1, 8), Q))
    sweep(3, 61, 8, st.restricted(rs, tmp, u, lambda t, r: u[t - 1, r], s, range(1, 4)))
    sweep(4, 60, 16, st.smoothed(e0, None, tmp, range(1, 4), KQ))
    sweep(5, 59, 16, st.coarse_defect(tmp, e0, lambda m, r: e0[m - 1, r], rs, (2, 3)))
    sweep(6, 58, 16, st.smoothed(e1, e0, tmp, (2, 3), KQ))
    sweep(7, 57, 16, st.coarse_defect(tmp, e1, lambda m, r: e1[m - 1, r], rs, (3,)))
    sweep(8, 56, 16, st.smoothed(e2, e1, tmp, (3,), KQ))


def edge_first(above, below, g_in, s_in, co_in, u_in, g, s, co, u, out, tmp):
    del g_in, s_in, co_in, u_in
    beside = beside_maker()
    for source, low in ((above, 0), (below, HALO + ROWS)):

        def fill(j, carry):
            for t in range(8):
                g[t, low + j] = source[t, j]
                s[t, low + j] = source[8 + t, j]
            coefficients(co, low + j, source[16, j])
            co[ST, low + j] = source[17, j]
            return carry

        lax.fori_loop(0, HALO, fill, 0)
    st = Stages(beside, co)
    for low, high in ((-10, 3), (61, 74)):
        sweep(low, high, 16, st.fine_defect(tmp, g, lambda t, r: g[t - 1, r], s, (7,)))
    for low, high in ((-9, 2), (62, 73)):
        sweep(low, high, 16, st.smoothed(u, g, tmp, (7,), Q))
    for j in range(10):
        out[j] = g[7, HALO - 10 + j]
        out[10 + j] = g[7, HALO + ROWS + j]
        out[20 + j] = u[7, HALO - 8 + j]
        out[30 + j] = u[7, HALO + 62 + j]


def edges(g, s, co, u_in, rs_in, e0_in, e1_in, e2_in, u, rs, e0, e1, e2, out, tmp):
    del u_in, rs_in, e0_in, e1_in, e2_in
    beside = beside_maker()
    st = Stages(beside, co)

    def both(inner, depth, unroll, body):
        sweep(-depth, inner, unroll, body)
        sweep(ROWS - inner, ROWS + depth, unroll, body)

    both(3, 10, 13, st.fine_defect(tmp, g, lambda t, r: g[t - 1, r], s, range(1, 7)))
    both(2, 9, 11, st.smoothed(u, g, tmp, range(1, 7), Q))
    both(3, 8, 11, st.restricted(rs, tmp, u, lambda t, r: u[t - 1, r], s, range(1, 4)))

    def scale(r):
        for m in range(1, 4):
            tmp[m, r] = rs[m, r] * co[KINV, r]

    sweep(3, 5, 2, scale)
    sweep(59, 61, 2, scale)
    both(4, 7, 11, st.smoothed(e0, None, tmp, range(1, 4), KQ))
    both(7, 6, 13, st.coarse_defect(tmp, e0, lambda m, r: e0[m - 1, r], rs, (2, 3)))
    both(6, 5, 11, st.smoothed(e1, e0, tmp, (2, 3), KQ))
    both(9, 4, 13, st.coarse_defect(tmp, e1, lambda m, r: e1[m - 1, r], rs, (3,)))
    both(8, 3, 11, st.smoothed(e2, e1, tmp, (3,), KQ))

    def copy(i, carry):
        for j in range(19):
            r = jnp.minimum(i * 19 + j, 75)
            out[r] = e0[3, HALO - 6 + r]
            q = jnp.minimum(r, 71)
            out[76 + q] = e1[3, HALO - 4 + q]
            p = jnp.minimum(r, 69)
            out[148 + p] = e2[3, HALO - 3 + p]
        return carry

    lax.fori_loop(0, 4, copy, 0)


def middle(t0, t1, g, s, co, u_in, rs_in, e0_in, e1_in, e2_in, u, rs, e0, e1, e2, before, sol7, send, gb, tmp, u2):
    del u_in, rs_in, e0_in, e1_in, e2_in
    beside = beside_maker()
    st = Stages(beside, co)

    def fill(i, carry):
        for j in range(8):
            r = i * 8 + j
            gb[HALO + r] = t0[r] + co[ST, HALO + r]
            q = jnp.minimum(r, 59)
            before[HALO + 2 + q] = t0[ROWS + q] + co[ST, HALO + 2 + q]
        return carry

    lax.fori_loop(0, ROWS // 8, fill, 0)
    for j in range(10):
        gb[HALO - 10 + j] = t1[j] + co[ST, HALO - 10 + j]
        gb[HALO + ROWS + j] = t1[10 + j] + co[ST, HALO + ROWS + j]
        before[HALO - 8 + j] = t1[20 + j] + co[ST, HALO - 8 + j]
        before[HALO + 62 + j] = t1[30 + j] + co[ST, HALO + 62 + j]
    sweep(-10, 74, 21, st.fine_defect(tmp, g, lambda t, r: gb[r], s, (0,)))
    sweep(-9, 73, 21, st.smoothed(u, g, tmp, (0,), Q))
    sweep(-8, 72, 16, st.restricted(rs, tmp, u, lambda t, r: u[0, r] if t else before[r], s, (0,)))
    sweep(-7, 71, 20, st.smoothed(e0, None, tmp, (0,), KQ))
    sweep(-6, 70, 19, st.coarse_defect(tmp, e0, lambda m, r: e0[0, r], rs, (1,)))
    sweep(-5, 69, 19, st.smoothed(e1, e0, tmp, (1,), KQ))
    sweep(-4, 68, 18, st.coarse_defect(tmp, e1, lambda m, r: e1[1, r], rs, (2,)))

    def corrected(r):
        q = co[KQ, r]
        late = e1[2, r] + tmp[2, r] + q * around(beside, tmp, 2, r)
        e2[2, r] = late
        u2[0, r] = u[6, r] + 0.5 * (late + e2[3, r])
        u2[1, r] = u[7, r] + e2[3, r]

    sweep(-3, 67, 18, corrected)

    def defect(r):
        tmp[0, r] = (
            s[7, r] + u2[0, r] - co[D, r] * u2[1, r] + co[C, r] * around(beside, u2, 1, r)
        ) * co[INV, r]

    sweep(-2, 66, 17, defect)

    def final(r):
        sol7[0, r] = u2[1, r] + tmp[0, r] + co[Q, r] * around(beside, tmp, 0, r)

    sweep(-1, 65, 17, final)

    def copy(i, carry):
        for j in range(8):
            send[tile_at(0, i, j), :] = sol7[0, HALO + 8 * i + j]
        return carry

    lax.fori_loop(0, ROWS // 8, copy, 0)


def last(t2, s, co, u, rs, e0, e1_in, e2_in, before, sol7, sol_out, res_out, base, e1, u2, tmp, sol, sol_nat, res_nat, sems):
    beside = beside_maker()
    st = Stages(beside, co)

    def first_defect(r):
        tmp[0, r] = (
            rs[0, r] + t2[r - (HALO - 6)] - co[KD, r] * e0[0, r] + co[K, r] * around(beside, e0, 0, r)
        ) * co[KINV, r]

    sweep(-6, 70, 19, first_defect)
    sweep(-5, 69, 19, st.smoothed(e1, e0, tmp, (0,), KQ))

    def carry_over(r):
        e1[1, r] = e1_in[1, r]

    sweep(-5, 69, 19, carry_over)

    def second_defect(r):
        k, kd, kinv = co[K, r], co[KD, r], co[KINV, r]
        earlier = (t2[76 + r - (HALO - 4)], e1[0, r])
        for m in (0, 1):
            tmp[m, r] = (rs[m, r] + earlier[m] - kd * e1[m, r] + k * around(beside, e1, m, r)) * kinv

    sweep(-4, 68, 18, second_defect)

    def corrected(r):
        q = co[KQ, r]
        boundary = t2[148 + r - (HALO - 3)]
        e20 = e1[0, r] + tmp[0, r] + q * around(beside, tmp, 0, r)
        e21 = e1[1, r] + tmp[1, r] + q * around(beside, tmp, 1, r)
        e22, e23 = e2_in[2, r], e2_in[3, r]
        u2[7, r] = before[r] + boundary
        u2[0, r] = u[0, r] + 0.5 * (boundary + e20)
        u2[1, r] = u[1, r] + e20
        u2[2, r] = u[2, r] + 0.5 * (e20 + e21)
        u2[3, r] = u[3, r] + e21
        u2[4, r] = u[4, r] + 0.5 * (e21 + e22)
        u2[5, r] = u[5, r] + e22
        u2[6, r] = u[6, r] + 0.5 * (e22 + e23)

    sweep(-3, 67, 10, corrected)
    sweep(-2, 66, 8, st.fine_defect(tmp, u2, lambda t, r: u2[(t - 1) % 8, r], s, range(7)))
    final = st.smoothed(sol, u2, tmp, range(7), Q)

    def final_all(r):
        final(r)
        sol[7, r] = sol7[0, r]

    sweep(-1, 0, 1, final_all)
    sweep(64, 65, 1, final_all)

    def solve(i, carry):
        for j in range(8):
            r = HALO + 8 * i + j
            final_all(r)
            for t in range(8):
                sol_nat[tile_at(t, i, j), :] = sol[t, r]
        return carry

    lax.fori_loop(0, ROWS // 8, solve, 0)
    copy_sol = pltpu.make_async_copy(sol_nat, sol_out, sems.at[0])
    copy_sol.start()

    def resid(i, carry):
        for j in range(8):
            r = HALO + 8 * i + j
            c, d = co[C, r], co[D, r]
            for t in range(8):
                earlier = sol[t - 1, r] if t else co[ST, r]
                value = s[t, r] + earlier - d * sol[t, r] + c * around(beside, sol, t, r)
                if t:
                    res_nat[tile_at(t - 1, i, j), :] = value
                else:
                    base[tile_at(0, i, j), :] = value
        return carry

    lax.fori_loop(0, ROWS // 8, resid, 0)
    copy_res = pltpu.make_async_copy(res_nat, res_out.at[pl.ds(ROWS * 8, 7 * ROWS * 8)], sems.at[1])
    copy_res.start()
    copy_sol.wait()
    copy_res.wait()


def finish(res_in, base, t3, res_out, total, sem):
    del res_in
    total[...] = base[...] + t3[...]
    copy = pltpu.make_async_copy(total, res_out.at[pl.ds(0, ROWS * 8)], sem)
    copy.start()
    copy.wait()


def call(kernel, ins, outs, scratch=(), aliases=None, specs=None, out_specs=None, limit=24):
    return pl.pallas_call(
        kernel,
        out_shape=outs,
        in_specs=specs or [FULL] * len(ins),
        out_specs=out_specs or [FULL] * len(outs),
        scratch_shapes=list(scratch),
        input_output_aliases=aliases or {},
        compiler_params=pltpu.CompilerParams(vmem_limit_bytes=limit * 2**20),
    )(*ins)


def along(block, axis, distance):
    count = lax.axis_size(axis)
    return lax.ppermute(block, axis, [(i, i + distance) for i in range(count) if 0 <= i + distance < count])


def cycle(source, guess, start_state, conduct):
    is_first = (lax.axis_index("tm") == 0).astype(F32).reshape(1)
    guess_v, source_v = view(guess), view(source)
    start_v, conduct_v = view(start_state[None]), view(conduct[None])
    halo = jax.ShapeDtypeStruct((18, HALO, 8, 128), F32)
    vmem = lambda steps: pltpu.VMEM((steps, EXT, 8, 128), F32)

    top, bottom = call(
        edge_pack, (is_first, guess_v, source_v, start_v, conduct_v), [halo, halo], specs=[SMEM] + [FULL] * 4, limit=4
    )
    above = along(bottom, "space", 1)
    below = along(top, "space", -1)
    (send0,) = call(
        last_step_pack,
        (guess_v, source_v, conduct_v),
        [rows_of(124)],
        [pltpu.VMEM((2, ROWS, 8, 128), F32), pltpu.VMEM((ROWS, 8, 128), F32)],
        limit=4,
    )
    t0 = along(send0, "tm", 1)
    g, s, co, u, rs, e0, e1, e2 = call(
        interior,
        (is_first, guess_v, source_v, start_v, conduct_v),
        [ext(8), ext(8), ext(9), ext(8), ext(4), ext(4), ext(4), ext(4)],
        [vmem(8)],
        specs=[SMEM] + [FULL] * 4,
        limit=6,
    )
    g, s, co, u, send1 = call(
        edge_first,
        (above, below, g, s, co, u),
        [ext(8), ext(8), ext(9), ext(8), rows_of(40)],
        [vmem(8)],
        aliases={2: 0, 3: 1, 4: 2, 5: 3},
        limit=6,
    )
    t1 = along(send1, "tm", 1)
    u, rs, e0, e1, e2, send2 = call(
        edges,
        (g, s, co, u, rs, e0, e1, e2),
        [ext(8), ext(4), ext(4), ext(4), ext(4), rows_of(218)],
        [vmem(8)],
        aliases={3: 0, 4: 1, 5: 2, 6: 3, 7: 4},
        limit=6,
    )
    t2 = along(send2, "tm", 1)
    u, rs, e0, e1, e2, before, sol7, send3 = call(
        middle,
        (t0, t1, g, s, co, u, rs, e0, e1, e2),
        [
            ext(8), ext(4), ext(4), ext(4), ext(4), rows_of(EXT), ext(1),
            jax.ShapeDtypeStruct((ROWS * 8, 128), F32),
        ],
        [pltpu.VMEM((EXT, 8, 128), F32), vmem(4), vmem(2)],
        aliases={5: 0, 6: 1, 7: 2, 8: 3, 9: 4},
        limit=6,
    )
    t3 = along(send3, "tm", 1)
    nat = jax.ShapeDtypeStruct((8 * ROWS * 8, 128), F32)
    one = jax.ShapeDtypeStruct((ROWS * 8, 128), F32)
    sol, res, base = call(
        last,
        (t2, s, co, u, rs, e0, e1, e2, before, sol7),
        [nat, nat, one],
        [
            vmem(2), vmem(8), vmem(8), vmem(8),
            pltpu.VMEM(nat.shape, F32), pltpu.VMEM((7 * ROWS * 8, 128), F32), pltpu.SemaphoreType.DMA((2,)),
        ],
        out_specs=[ANY, ANY, FULL],
        limit=16,
    )
    (res,) = call(
        finish,
        (res, base, t3),
        [nat],
        [pltpu.VMEM((ROWS * 8, 128), F32), pltpu.SemaphoreType.DMA],
        aliases={0: 0},
        specs=[ANY, FULL, FULL],
        out_specs=[ANY],
        limit=4,
    )
    return unview(sol, 8), unview(res, 8)


def solution(mesh):
    return jax.shard_map(
        cycle,
        mesh=mesh,
        in_specs=(P("tm", "space", None), P("tm", "space", None), P("space", None), P("space", None)),
        out_specs=(P("tm", "space", None), P("tm", "space", None)),
        check_vma=False,
    )
```

```python
import jax
import jax.numpy as jnp
from jax import lax
from jax.experimental import pallas as pl
from jax.experimental.pallas import tpu as pltpu
from jax.sharding import PartitionSpec as P


F32 = jnp.float32
ROWS = 64
HALO = 11
EXT = ROWS + 2 * HALO
DAMP = 0.8
C, D, INV, Q, K, KD, KINV, KQ, ST = range(9)
FULL = pl.BlockSpec(memory_space=pltpu.VMEM)
SMEM = pl.BlockSpec(memory_space=pltpu.SMEM)
ANY = pl.BlockSpec(memory_space=pltpu.HBM)


def ext(steps):
    return jax.ShapeDtypeStruct((steps, EXT, 8, 128), F32)


def rows_of(count):
    return jax.ShapeDtypeStruct((count, 8, 128), F32)


def view(x):
    steps = x.shape[0]
    return x.reshape(steps, ROWS // 8, 8, 8, 128).transpose(0, 1, 3, 2, 4).reshape(steps * ROWS * 8, 128)


def unview(y, steps):
    return y.reshape(steps, ROWS // 8, 8, 8, 128).transpose(0, 1, 3, 2, 4).reshape(steps, ROWS, 1024)


def tile_at(step, tile, row):
    return pl.ds(step * ROWS * 8 + tile * 64 + row, 8, 8)


def beside_maker():
    lane = lax.broadcasted_iota(jnp.int32, (8, 128), 1)
    sub = lax.broadcasted_iota(jnp.int32, (8, 128), 0)
    first, last = lane == 0, lane == 127
    top, bottom = sub == 0, sub == 7

    def beside(x):
        before = jnp.where(top, 0.0, pltpu.roll(x, 1, 0))
        after = jnp.where(bottom, 0.0, pltpu.roll(x, 7, 0))
        return pltpu.roll(jnp.where(last, before, x), 1, 1) + pltpu.roll(jnp.where(first, after, x), 127, 1)

    return beside


def around(beside, ref, step, r):
    return ref[step, r - 1] + ref[step, r + 1] + beside(ref[step, r])


def sweep(low, high, unroll, body):
    low, high = low + HALO, high + HALO
    count = high - low
    unroll = min(unroll, count)
    blocks = -(-count // unroll)
    if blocks == 1:
        for j in range(unroll):
            body(low + j)
        return

    def step(i, carry):
        start = jnp.minimum(low + i * unroll, high - unroll)
        for j in range(unroll):
            body(start + j)
        return carry

    lax.fori_loop(0, blocks, step, 0)


def coefficients(co, r, c):
    diag = 1.0 + 4.0 * c
    coarse = 1.0 + 8.0 * c
    recip = 1.0 / diag
    coarse_recip = 1.0 / coarse
    co[C, r] = c
    co[D, r] = diag
    co[INV, r] = DAMP * recip
    co[Q, r] = c * recip
    co[K, r] = 2.0 * c
    co[KD, r] = coarse
    co[KINV, r] = DAMP * coarse_recip
    co[KQ, r] = 2.0 * c * coarse_recip


class Stages:
    def __init__(self, beside, co):
        self.beside, self.co = beside, co

    def fine_defect(self, out, field, earlier, source, steps):
        def body(r):
            c, d, inv = self.co[C, r], self.co[D, r], self.co[INV, r]
            for t in steps:
                out[t, r] = (source[t, r] + earlier(t, r) - d * field[t, r] + c * around(self.beside, field, t, r)) * inv

        return body

    def coarse_defect(self, out, field, earlier, rhs, steps):
        def body(r):
            k, kd, kinv = self.co[K, r], self.co[KD, r], self.co[KINV, r]
            for m in steps:
                out[m, r] = (rhs[m, r] + earlier(m, r) - kd * field[m, r] + k * around(self.beside, field, m, r)) * kinv

        return body

    def smoothed(self, out, field, defect, steps, plane):
        def body(r):
            q = self.co[plane, r]
            for t in steps:
                base = defect[t, r] if field is None else field[t, r] + defect[t, r]
                out[t, r] = base + q * around(self.beside, defect, t, r)

        return body

    def restricted(self, out, scaled, field, earlier, source, pairs):
        def body(r):
            c, d, kinv = self.co[C, r], self.co[D, r], self.co[KINV, r]
            for m in pairs:
                parts = [
                    source[t, r] + earlier(t, r) - d * field[t, r] + c * around(self.beside, field, t, r)
                    for t in (2 * m, 2 * m + 1)
                ]
                both = parts[0] + parts[1]
                out[m, r] = both
                scaled[m, r] = both * kinv

        return body


def edge_pack(is_first, is_odd, guess, source, start, conduct, near, far, gb, sb, tb, cb, sems):
    copies = []
    for n, (src, dst) in enumerate(((guess, gb), (source, sb), (start, tb), (conduct, cb))):
        for m, low in enumerate((0, 384)):
            copies.append(pltpu.make_async_copy(src.at[:, pl.ds(low, 128)], dst.at[:, m], sems.at[n, m]))
    for copy in copies:
        copy.start()
    for copy in copies:
        copy.wait()
    odd = is_odd[0]
    for out, side in ((near, 1 - odd), (far, odd)):

        def body(j, carry):
            r = j + 5 * side
            here = pl.ds((r // 8) * 64 + r % 8, 8, 8)
            for t in range(8):
                out[t, j] = gb[t, side, here, :]
                out[8 + t, j] = sb[t, side, here, :]
            out[16, j] = cb[0, side, here, :]
            out[17, j] = tb[0, side, here, :] * is_first[0]
            return carry

        lax.fori_loop(0, HALO, body, 0)


def last_step_pack(guess, source, conduct, out, g, e):
    beside = beside_maker()

    def fill(i, carry):
        for j in range(8):
            r = 8 * i + j
            for t in (6, 7):
                g[t - 6, r] = guess[tile_at(t, i, j), :]
            out[r] = g[1, r]
        return carry

    lax.fori_loop(0, ROWS // 8, fill, 0)

    def cond_at(r):
        return conduct[pl.ds((r // 8) * 64 + r % 8, 8, 8), :]

    def defect(i, carry):
        start = jnp.minimum(1 + i * 16, 63 - 16)
        for j in range(16):
            r = start + j
            c = cond_at(r)
            d = 1.0 + 4.0 * c
            right = source[pl.ds(7 * 512 + (r // 8) * 64 + r % 8, 8, 8), :]
            e[r] = (right + g[0, r] - d * g[1, r] + c * around(beside, g, 1, r)) * (DAMP / d)
        return carry

    lax.fori_loop(0, 4, defect, 0)

    def smooth(i, carry):
        start = jnp.minimum(2 + i * 16, 62 - 16)
        for j in range(16):
            r = start + j
            c = cond_at(r)
            q = c / (1.0 + 4.0 * c)
            out[ROWS - 2 + r] = g[1, r] + e[r] + q * (e[r - 1] + e[r + 1] + beside(e[r]))
        return carry

    lax.fori_loop(0, 4, smooth, 0)


def interior(is_first, guess, source, start, conduct, g, s, co, u, rs, e0, e1, tmp):
    beside = beside_maker()

    def fill(i, carry):
        for j in range(8):
            r = HALO + 8 * i + j
            for t in range(8):
                g[t, r] = guess[tile_at(t, i, j), :]
                s[t, r] = source[tile_at(t, i, j), :]
            coefficients(co, r, conduct[tile_at(0, i, j), :])
            co[ST, r] = start[tile_at(0, i, j), :] * is_first[0]
        return carry

    lax.fori_loop(0, ROWS // 8, fill, 0)
    st = Stages(beside, co)
    sweep(1, 63, 16, st.fine_defect(tmp, g, lambda t, r: g[t - 1, r], s, range(3, 8)))
    sweep(2, 62, 15, st.smoothed(u, g, tmp, range(3, 8), Q))
    sweep(3, 61, 15, st.restricted(rs, tmp, u, lambda t, r: u[t - 1, r], s, (2, 3)))
    sweep(4, 60, 28, st.smoothed(e0, None, tmp, (2, 3), KQ))
    sweep(5, 59, 27, st.coarse_defect(tmp, e0, lambda m, r: e0[m - 1, r], rs, (3,)))
    sweep(6, 58, 26, st.smoothed(e1, e0, tmp, (3,), KQ))


def edge_first(is_odd, near, far, g_in, s_in, co_in, u_in, g, s, co, u, out, tmp):
    del g_in, s_in, co_in, u_in
    beside = beside_maker()
    odd = is_odd[0]
    for source, side in ((near, 1 - odd), (far, odd)):
        low = side * (HALO + ROWS)

        def fill(j, carry):
            for t in range(8):
                g[t, low + j] = source[t, j]
                s[t, low + j] = source[8 + t, j]
            coefficients(co, low + j, source[16, j])
            co[ST, low + j] = source[17, j]
            return carry

        lax.fori_loop(0, HALO, fill, 0)
    st = Stages(beside, co)
    for low, high in ((-10, 3), (61, 74)):
        sweep(low, high, 16, st.fine_defect(tmp, g, lambda t, r: g[t - 1, r], s, (7,)))
    for low, high in ((-9, 2), (62, 73)):
        sweep(low, high, 16, st.smoothed(u, g, tmp, (7,), Q))
    for j in range(10):
        out[j] = g[7, HALO - 10 + j]
        out[10 + j] = g[7, HALO + ROWS + j]
        out[20 + j] = u[7, HALO - 8 + j]
        out[30 + j] = u[7, HALO + 62 + j]


def edges(g, s, co, u_in, rs_in, e0_in, e1_in, u, rs, e0, e1, out, tmp):
    del u_in, rs_in, e0_in, e1_in
    beside = beside_maker()
    st = Stages(beside, co)

    def both(inner, depth, unroll, body):
        sweep(-depth, inner, unroll, body)
        sweep(ROWS - inner, ROWS + depth, unroll, body)

    both(3, 10, 13, st.fine_defect(tmp, g, lambda t, r: g[t - 1, r], s, range(3, 7)))
    both(2, 9, 11, st.smoothed(u, g, tmp, range(3, 7), Q))
    both(3, 8, 11, st.restricted(rs, tmp, u, lambda t, r: u[t - 1, r], s, (2, 3)))

    def scale(r):
        for m in (2, 3):
            tmp[m, r] = rs[m, r] * co[KINV, r]

    sweep(3, 5, 2, scale)
    sweep(59, 61, 2, scale)
    both(4, 7, 11, st.smoothed(e0, None, tmp, (2, 3), KQ))
    both(7, 6, 13, st.coarse_defect(tmp, e0, lambda m, r: e0[m - 1, r], rs, (3,)))
    both(6, 5, 11, st.smoothed(e1, e0, tmp, (3,), KQ))

    def copy(i, carry):
        for j in range(19):
            r = i * 19 + j
            out[r] = e0[3, HALO - 6 + r]
            q = jnp.minimum(r, 71)
            out[76 + q] = e1[3, HALO - 4 + q]
        return carry

    lax.fori_loop(0, 4, copy, 0)


def rest(g, s, co, u_in, rs_in, e0_in, e1_in, u, rs, e0, e1, e2, tmp):
    del u_in, rs_in, e0_in, e1_in
    beside = beside_maker()
    st = Stages(beside, co)
    sweep(-10, 74, 28, st.fine_defect(tmp, g, lambda t, r: g[t - 1, r], s, (1, 2)))
    sweep(-9, 73, 28, st.smoothed(u, g, tmp, (1, 2), Q))
    sweep(-8, 72, 20, st.restricted(rs, tmp, u, lambda t, r: u[t - 1, r], s, (1,)))
    sweep(-7, 71, 26, st.smoothed(e0, None, tmp, (1,), KQ))
    sweep(-6, 70, 26, st.coarse_defect(tmp, e0, lambda m, r: e0[m - 1, r], rs, (2,)))
    sweep(-5, 69, 25, st.smoothed(e1, e0, tmp, (2,), KQ))
    sweep(-4, 68, 24, st.coarse_defect(tmp, e1, lambda m, r: e1[m - 1, r], rs, (3,)))
    sweep(-3, 67, 24, st.smoothed(e2, e1, tmp, (3,), KQ))


def middle(t0, t1, g, s, co, u_in, rs_in, e0_in, e1_in, e2_in, u, rs, e0, e1, e2, before, sol7, send, gb, tmp, u2):
    del u_in, rs_in, e0_in, e1_in, e2_in
    beside = beside_maker()
    st = Stages(beside, co)

    def fill(i, carry):
        for j in range(8):
            r = i * 8 + j
            gb[HALO + r] = t0[r] + co[ST, HALO + r]
            q = jnp.minimum(r, 59)
            before[HALO + 2 + q] = t0[ROWS + q] + co[ST, HALO + 2 + q]
        return carry

    lax.fori_loop(0, ROWS // 8, fill, 0)
    for j in range(10):
        gb[HALO - 10 + j] = t1[j] + co[ST, HALO - 10 + j]
        gb[HALO + ROWS + j] = t1[10 + j] + co[ST, HALO + ROWS + j]
        before[HALO - 8 + j] = t1[20 + j] + co[ST, HALO - 8 + j]
        before[HALO + 62 + j] = t1[30 + j] + co[ST, HALO + 62 + j]
    sweep(-10, 74, 28, st.fine_defect(tmp, g, lambda t, r: gb[r], s, (0,)))
    sweep(-9, 73, 28, st.smoothed(u, g, tmp, (0,), Q))
    sweep(-8, 72, 20, st.restricted(rs, tmp, u, lambda t, r: u[0, r] if t else before[r], s, (0,)))
    sweep(-7, 71, 26, st.smoothed(e0, None, tmp, (0,), KQ))
    sweep(-6, 70, 26, st.coarse_defect(tmp, e0, lambda m, r: e0[0, r], rs, (1,)))
    sweep(-5, 69, 25, st.smoothed(e1, e0, tmp, (1,), KQ))
    sweep(-4, 68, 24, st.coarse_defect(tmp, e1, lambda m, r: e1[1, r], rs, (2,)))

    def corrected(r):
        q = co[KQ, r]
        late = e1[2, r] + tmp[2, r] + q * around(beside, tmp, 2, r)
        e2[2, r] = late
        u2[0, r] = u[6, r] + 0.5 * (late + e2[3, r])
        u2[1, r] = u[7, r] + e2[3, r]

    sweep(-3, 67, 24, corrected)

    def defect(r):
        tmp[0, r] = (
            s[7, r] + u2[0, r] - co[D, r] * u2[1, r] + co[C, r] * around(beside, u2, 1, r)
        ) * co[INV, r]

    sweep(-2, 66, 23, defect)

    def final(r):
        sol7[0, r] = u2[1, r] + tmp[0, r] + co[Q, r] * around(beside, tmp, 0, r)

    sweep(-1, 65, 22, final)

    def copy(i, carry):
        for j in range(10):
            r = i * 10 + j
            send[r] = e2[3, HALO - 3 + r]
            q = jnp.minimum(r, 63)
            send[70 + q] = sol7[0, HALO + q]
        return carry

    lax.fori_loop(0, 7, copy, 0)


def late(t2, s, co, u, rs, e0, e1_in, e2_in, sol7, sol_out, res_out, u2_out, sol2, e1, u2, tmp, sol, sol_nat, res_nat, sems):
    beside = beside_maker()
    st = Stages(beside, co)

    def first_defect(r):
        tmp[0, r] = (
            rs[0, r] + t2[r - (HALO - 6)] - co[KD, r] * e0[0, r] + co[K, r] * around(beside, e0, 0, r)
        ) * co[KINV, r]

    sweep(-6, 70, 26, first_defect)

    def first_smooth(r):
        e1[0, r] = e0[0, r] + tmp[0, r] + co[KQ, r] * around(beside, tmp, 0, r)
        e1[1, r] = e1_in[1, r]

    sweep(-5, 69, 25, first_smooth)

    def second_defect(r):
        k, kd, kinv = co[K, r], co[KD, r], co[KINV, r]
        earlier = (t2[76 + r - (HALO - 4)], e1[0, r])
        for m in (0, 1):
            tmp[m, r] = (rs[m, r] + earlier[m] - kd * e1[m, r] + k * around(beside, e1, m, r)) * kinv

    sweep(-4, 68, 24, second_defect)

    def corrected(r):
        q = co[KQ, r]
        e20 = e1[0, r] + tmp[0, r] + q * around(beside, tmp, 0, r)
        e21 = e1[1, r] + tmp[1, r] + q * around(beside, tmp, 1, r)
        e22, e23 = e2_in[2, r], e2_in[3, r]
        u2_out[0, r] = u[0, r] + 0.5 * e20
        first = u[1, r] + e20
        u2_out[1, r] = first
        u2[1, r] = first
        u2[2, r] = u[2, r] + 0.5 * (e20 + e21)
        u2[3, r] = u[3, r] + e21
        u2[4, r] = u[4, r] + 0.5 * (e21 + e22)
        u2[5, r] = u[5, r] + e22
        u2[6, r] = u[6, r] + 0.5 * (e22 + e23)

    sweep(-3, 67, 18, corrected)
    sweep(-2, 66, 17, st.fine_defect(tmp, u2, lambda t, r: u2[t - 1, r], s, range(2, 7)))
    final = st.smoothed(sol, u2, tmp, range(2, 7), Q)

    def final_all(r):
        final(r)
        sol[7, r] = sol7[0, r]
        sol2[0, r] = sol[2, r]

    sweep(-1, 0, 1, final_all)
    sweep(64, 65, 1, final_all)

    def solve(i, carry):
        for h in range(2):
            for j in range(8):
                r = HALO + 16 * i + 8 * h + j
                final_all(r)
                for t in range(2, 8):
                    sol_nat[tile_at(t - 2, 2 * i + h, j), :] = sol[t, r]
        return carry

    lax.fori_loop(0, ROWS // 16, solve, 0)
    copy_sol = pltpu.make_async_copy(sol_nat, sol_out.at[pl.ds(2 * ROWS * 8, 6 * ROWS * 8)], sems.at[0])
    copy_sol.start()

    def resid(i, carry):
        for h in range(2):
            for j in range(8):
                r = HALO + 16 * i + 8 * h + j
                c, d = co[C, r], co[D, r]
                for t in range(3, 8):
                    res_nat[tile_at(t - 3, 2 * i + h, j), :] = (
                        s[t, r] + sol[t - 1, r] - d * sol[t, r] + c * around(beside, sol, t, r)
                    )
        return carry

    lax.fori_loop(0, ROWS // 16, resid, 0)
    copy_res = pltpu.make_async_copy(res_nat, res_out.at[pl.ds(3 * ROWS * 8, 5 * ROWS * 8)], sems.at[1])
    copy_res.start()
    copy_sol.wait()
    copy_res.wait()


def finish(t3, s, co, before, u2_in, sol2, sol_in, res_in, sol_out, res_out, u2, tmp, sol, sol_nat, res_nat, sems):
    del sol_in, res_in
    beside = beside_maker()

    def corrected(r):
        boundary = t3[r - (HALO - 3)]
        u2[0, r] = before[r] + boundary
        u2[1, r] = u2_in[0, r] + 0.5 * boundary

    sweep(-3, 67, 14, corrected)

    def defect(r):
        c, d, inv = co[C, r], co[D, r], co[INV, r]
        tmp[0, r] = (s[0, r] + u2[0, r] - d * u2[1, r] + c * around(beside, u2, 1, r)) * inv
        tmp[1, r] = (s[1, r] + u2[1, r] - d * u2_in[1, r] + c * around(beside, u2_in, 1, r)) * inv

    sweep(-2, 66, 34, defect)

    def final(r):
        q = co[Q, r]
        sol[0, r] = u2[1, r] + tmp[0, r] + q * around(beside, tmp, 0, r)
        sol[1, r] = u2_in[1, r] + tmp[1, r] + q * around(beside, tmp, 1, r)

    sweep(-1, 65, 33, final)

    def resid(i, carry):
        for h in range(4):
            for j in range(8):
                r = HALO + 32 * i + 8 * h + j
                c, d = co[C, r], co[D, r]
                spot = lambda t: tile_at(t, 4 * i + h, j)
                old = t3[r - HALO + 70] + co[ST, r]
                first, second = sol[0, r], sol[1, r]
                sol_nat[spot(0), :] = first
                sol_nat[spot(1), :] = second
                res_nat[spot(0), :] = s[0, r] + old - d * first + c * around(beside, sol, 0, r)
                res_nat[spot(1), :] = s[1, r] + first - d * second + c * around(beside, sol, 1, r)
                res_nat[spot(2), :] = s[2, r] + second - d * sol2[0, r] + c * around(beside, sol2, 0, r)
        return carry

    lax.fori_loop(0, ROWS // 32, resid, 0)
    copies = (
        pltpu.make_async_copy(sol_nat, sol_out.at[pl.ds(0, 2 * ROWS * 8)], sems.at[0]),
        pltpu.make_async_copy(res_nat, res_out.at[pl.ds(0, 3 * ROWS * 8)], sems.at[1]),
    )
    for copy in copies:
        copy.start()
    for copy in copies:
        copy.wait()


def call(kernel, ins, outs, scratch=(), aliases=None, specs=None, out_specs=None, limit=24):
    return pl.pallas_call(
        kernel,
        out_shape=outs,
        in_specs=specs or [FULL] * len(ins),
        out_specs=out_specs or [FULL] * len(outs),
        scratch_shapes=list(scratch),
        input_output_aliases=aliases or {},
        compiler_params=pltpu.CompilerParams(vmem_limit_bytes=limit * 2**20),
    )(*ins)


def along(block, axis, route):
    count = lax.axis_size(axis)
    pairs = [(i, route(i)) for i in range(count)]
    return lax.ppermute(block, axis, [(i, j) for i, j in pairs if 0 <= j < count])


def ahead(i):
    return i + 1


def on_chip(i):
    return i ^ 1


def off_chip(i):
    return ((i + 1) ^ 1) - 1


def cycle(source, guess, start_state, conduct):
    is_first = (lax.axis_index("tm") == 0).astype(F32).reshape(1)
    is_odd = (lax.axis_index("space") % 2).astype(jnp.int32).reshape(1)
    guess_v, source_v = view(guess), view(source)
    start_v, conduct_v = view(start_state[None]), view(conduct[None])
    halo = jax.ShapeDtypeStruct((18, HALO, 8, 128), F32)
    vmem = lambda steps: pltpu.VMEM((steps, EXT, 8, 128), F32)
    plain = lambda rows: pltpu.VMEM((rows * 8, 128), F32)
    dma = pltpu.SemaphoreType.DMA

    by_step = lambda x: pltpu.with_memory_space_constraint(x.reshape(-1, ROWS * 8, 128), pltpu.HBM)
    near, far = call(
        edge_pack,
        (is_first, is_odd, by_step(guess_v), by_step(source_v), by_step(start_v), by_step(conduct_v)),
        [halo, halo],
        [pltpu.VMEM((n, 2, 128, 128), F32) for n in (8, 8, 1, 1)] + [dma((4, 2))],
        specs=[SMEM, SMEM] + [ANY] * 4,
        limit=6,
    )
    far_in = along(far, "space", off_chip)
    near_in = along(near, "space", on_chip)
    (send0,) = call(
        last_step_pack,
        (guess_v, source_v, conduct_v),
        [rows_of(124)],
        [pltpu.VMEM((2, ROWS, 8, 128), F32), pltpu.VMEM((ROWS, 8, 128), F32)],
        limit=4,
    )
    t0 = along(send0, "tm", ahead)
    g, s, co, u, rs, e0, e1 = call(
        interior,
        (is_first, guess_v, source_v, start_v, conduct_v),
        [ext(8), ext(8), ext(9), ext(8), ext(4), ext(4), ext(4)],
        [vmem(8)],
        specs=[SMEM] + [FULL] * 4,
        limit=6,
    )
    g, s, co, u, send1 = call(
        edge_first,
        (is_odd, near_in, far_in, g, s, co, u),
        [ext(8), ext(8), ext(9), ext(8), rows_of(40)],
        [vmem(8)],
        aliases={3: 0, 4: 1, 5: 2, 6: 3},
        specs=[SMEM] + [FULL] * 6,
        limit=6,
    )
    t1 = along(send1, "tm", ahead)
    u, rs, e0, e1, send2 = call(
        edges,
        (g, s, co, u, rs, e0, e1),
        [ext(8), ext(4), ext(4), ext(4), rows_of(148)],
        [vmem(8)],
        aliases={3: 0, 4: 1, 5: 2, 6: 3},
        limit=6,
    )
    t2 = along(send2, "tm", ahead)
    u, rs, e0, e1, e2 = call(
        rest,
        (g, s, co, u, rs, e0, e1),
        [ext(8), ext(4), ext(4), ext(4), ext(4)],
        [vmem(4)],
        aliases={3: 0, 4: 1, 5: 2, 6: 3},
        limit=4,
    )
    u, rs, e0, e1, e2, before, sol7, send3 = call(
        middle,
        (t0, t1, g, s, co, u, rs, e0, e1, e2),
        [ext(8), ext(4), ext(4), ext(4), ext(4), rows_of(EXT), ext(1), rows_of(134)],
        [pltpu.VMEM((EXT, 8, 128), F32), vmem(4), vmem(2)],
        aliases={5: 0, 6: 1, 7: 2, 8: 3, 9: 4},
        limit=6,
    )
    t3 = along(send3, "tm", ahead)
    nat = jax.ShapeDtypeStruct((8 * ROWS * 8, 128), F32)
    sol, res, u2, sol2 = call(
        late,
        (t2, s, co, u, rs, e0, e1, e2, sol7),
        [nat, nat, ext(2), ext(1)],
        [vmem(2), vmem(8), vmem(8), vmem(8), plain(6 * ROWS), plain(5 * ROWS), dma((2,))],
        out_specs=[ANY, ANY, FULL, FULL],
        limit=16,
    )
    sol, res = call(
        finish,
        (t3, s, co, before, u2, sol2, sol, res),
        [nat, nat],
        [vmem(2), vmem(2), vmem(2), plain(2 * ROWS), plain(3 * ROWS), dma((2,))],
        aliases={6: 0, 7: 1},
        specs=[FULL] * 6 + [ANY] * 2,
        out_specs=[ANY, ANY],
        limit=6,
    )
    return unview(sol, 8), unview(res, 8)


def solution(mesh):
    return jax.shard_map(
        cycle,
        mesh=mesh,
        in_specs=(P("tm", "space", None), P("tm", "space", None), P("space", None), P("space", None)),
        out_specs=(P("tm", "space", None), P("tm", "space", None)),
        check_vma=False,
    )
```

```python
import jax
import jax.numpy as jnp
from jax import lax
from jax.experimental import pallas as pl
from jax.experimental.pallas import tpu as pltpu
from jax.sharding import PartitionSpec as P


F32 = jnp.float32
ROWS = 64
HALO = 11
EXT = ROWS + 2 * HALO
DAMP = 0.8
C, D, INV, Q, K, KD, KINV, KQ, ST = range(9)
FULL = pl.BlockSpec(memory_space=pltpu.VMEM)
SMEM = pl.BlockSpec(memory_space=pltpu.SMEM)
ANY = pl.BlockSpec(memory_space=pltpu.HBM)


def ext(steps):
    return jax.ShapeDtypeStruct((steps, EXT, 8, 128), F32)


def rows_of(count):
    return jax.ShapeDtypeStruct((count, 8, 128), F32)


def view(x):
    steps = x.shape[0]
    return x.reshape(steps, ROWS // 8, 8, 8, 128).transpose(0, 1, 3, 2, 4).reshape(steps * ROWS * 8, 128)


def unview(y, steps):
    return y.reshape(steps, ROWS // 8, 8, 8, 128).transpose(0, 1, 3, 2, 4).reshape(steps, ROWS, 1024)


def tile_at(step, tile, row):
    return pl.ds(step * ROWS * 8 + tile * 64 + row, 8, 8)


def beside_maker():
    lane = lax.broadcasted_iota(jnp.int32, (8, 128), 1)
    sub = lax.broadcasted_iota(jnp.int32, (8, 128), 0)
    first, last = lane == 0, lane == 127
    top, bottom = sub == 0, sub == 7

    def beside(x):
        before = jnp.where(top, 0.0, pltpu.roll(x, 1, 0))
        after = jnp.where(bottom, 0.0, pltpu.roll(x, 7, 0))
        return pltpu.roll(jnp.where(last, before, x), 1, 1) + pltpu.roll(jnp.where(first, after, x), 127, 1)

    return beside


def around(beside, ref, step, r):
    return ref[step, r - 1] + ref[step, r + 1] + beside(ref[step, r])


def sweep(low, high, unroll, body):
    low, high = low + HALO, high + HALO
    count = high - low
    unroll = min(unroll, count)
    blocks = -(-count // unroll)
    if blocks == 1:
        for j in range(unroll):
            body(low + j)
        return

    def step(i, carry):
        start = jnp.minimum(low + i * unroll, high - unroll)
        for j in range(unroll):
            body(start + j)
        return carry

    lax.fori_loop(0, blocks, step, 0)


def coefficients(co, r, c):
    diag = 1.0 + 4.0 * c
    coarse = 1.0 + 8.0 * c
    recip = 1.0 / diag
    coarse_recip = 1.0 / coarse
    co[C, r] = c
    co[D, r] = diag
    co[INV, r] = DAMP * recip
    co[Q, r] = c * recip
    co[K, r] = 2.0 * c
    co[KD, r] = coarse
    co[KINV, r] = DAMP * coarse_recip
    co[KQ, r] = 2.0 * c * coarse_recip


class Stages:
    def __init__(self, beside, co):
        self.beside, self.co = beside, co

    def fine_defect(self, out, field, earlier, source, steps):
        def body(r):
            c, d, inv = self.co[C, r], self.co[D, r], self.co[INV, r]
            for t in steps:
                out[t, r] = (source[t, r] + earlier(t, r) - d * field[t, r] + c * around(self.beside, field, t, r)) * inv

        return body

    def coarse_defect(self, out, field, earlier, rhs, steps):
        def body(r):
            k, kd, kinv = self.co[K, r], self.co[KD, r], self.co[KINV, r]
            for m in steps:
                out[m, r] = (rhs[m, r] + earlier(m, r) - kd * field[m, r] + k * around(self.beside, field, m, r)) * kinv

        return body

    def smoothed(self, out, field, defect, steps, plane):
        def body(r):
            q = self.co[plane, r]
            for t in steps:
                base = defect[t, r] if field is None else field[t, r] + defect[t, r]
                out[t, r] = base + q * around(self.beside, defect, t, r)

        return body

    def restricted(self, out, scaled, field, earlier, source, pairs):
        def body(r):
            c, d, kinv = self.co[C, r], self.co[D, r], self.co[KINV, r]
            for m in pairs:
                parts = [
                    source[t, r] + earlier(t, r) - d * field[t, r] + c * around(self.beside, field, t, r)
                    for t in (2 * m, 2 * m + 1)
                ]
                both = parts[0] + parts[1]
                out[m, r] = both
                scaled[m, r] = both * kinv

        return body


def edge_pack(is_first, is_odd, guess, source, start, conduct, near, far, gb, sb, tb, cb, sems):
    copies = []
    for n, (src, dst) in enumerate(((guess, gb), (source, sb), (start, tb), (conduct, cb))):
        for m, low in enumerate((0, 384)):
            copies.append(pltpu.make_async_copy(src.at[:, pl.ds(low, 128)], dst.at[:, m], sems.at[n, m]))
    for copy in copies:
        copy.start()
    for copy in copies:
        copy.wait()
    odd = is_odd[0]
    for out, side in ((near, 1 - odd), (far, odd)):

        def outer(j, carry):
            r = j + 5 * side
            here = pl.ds((r // 8) * 64 + r % 8, 8, 8)
            for t in range(8):
                out[t * HALO + j] = gb[t, side, here, :]
            return carry

        def inner(j, carry):
            r = j + 6 * side
            here = pl.ds((r // 8) * 64 + r % 8, 8, 8)
            for t in range(8):
                out[8 * HALO + t * 10 + j] = sb[t, side, here, :]
            out[8 * HALO + 80 + j] = cb[0, side, here, :]
            out[8 * HALO + 90 + j] = tb[0, side, here, :] * is_first[0]
            return carry

        lax.fori_loop(0, HALO, outer, 0)
        lax.fori_loop(0, 10, inner, 0)


def last_step_pack(guess, source, conduct, out, g, e):
    beside = beside_maker()

    def fill(i, carry):
        for j in range(8):
            r = 8 * i + j
            for t in (6, 7):
                g[t - 6, r] = guess[tile_at(t, i, j), :]
            out[r] = g[1, r]
        return carry

    lax.fori_loop(0, ROWS // 8, fill, 0)

    def cond_at(r):
        return conduct[pl.ds((r // 8) * 64 + r % 8, 8, 8), :]

    def defect(i, carry):
        start = jnp.minimum(1 + i * 16, 63 - 16)
        for j in range(16):
            r = start + j
            c = cond_at(r)
            d = 1.0 + 4.0 * c
            right = source[pl.ds(7 * 512 + (r // 8) * 64 + r % 8, 8, 8), :]
            e[r] = (right + g[0, r] - d * g[1, r] + c * around(beside, g, 1, r)) * (DAMP / d)
        return carry

    lax.fori_loop(0, 4, defect, 0)

    def smooth(i, carry):
        start = jnp.minimum(2 + i * 16, 62 - 16)
        for j in range(16):
            r = start + j
            c = cond_at(r)
            q = c / (1.0 + 4.0 * c)
            out[ROWS - 2 + r] = g[1, r] + e[r] + q * (e[r - 1] + e[r + 1] + beside(e[r]))
        return carry

    lax.fori_loop(0, 4, smooth, 0)


def interior(is_first, guess, source, start, conduct, g, s, co, u, rs, e0, e1, tmp):
    beside = beside_maker()

    def fill(i, carry):
        for j in range(8):
            r = HALO + 8 * i + j
            for t in range(8):
                g[t, r] = guess[tile_at(t, i, j), :]
                s[t, r] = source[tile_at(t, i, j), :]
            coefficients(co, r, conduct[tile_at(0, i, j), :])
            co[ST, r] = start[tile_at(0, i, j), :] * is_first[0]
        return carry

    lax.fori_loop(0, ROWS // 8, fill, 0)
    st = Stages(beside, co)
    sweep(1, 63, 16, st.fine_defect(tmp, g, lambda t, r: g[t - 1, r], s, range(3, 8)))
    sweep(2, 62, 15, st.smoothed(u, g, tmp, range(3, 8), Q))
    sweep(3, 61, 15, st.restricted(rs, tmp, u, lambda t, r: u[t - 1, r], s, (2, 3)))
    sweep(4, 60, 28, st.smoothed(e0, None, tmp, (2, 3), KQ))
    sweep(5, 59, 27, st.coarse_defect(tmp, e0, lambda m, r: e0[m - 1, r], rs, (3,)))
    sweep(6, 58, 26, st.smoothed(e1, e0, tmp, (3,), KQ))


def edge_first(is_odd, near, far, g_in, s_in, co_in, u_in, g, s, co, u, out, tmp):
    del g_in, s_in, co_in, u_in
    beside = beside_maker()
    odd = is_odd[0]
    for source, side in ((near, 1 - odd), (far, odd)):
        low = side * (HALO + ROWS)
        low_inner = side * (HALO + ROWS - 1) + 1

        def outer(j, carry):
            for t in range(8):
                g[t, low + j] = source[t * HALO + j]
            return carry

        def inner(j, carry):
            for t in range(8):
                s[t, low_inner + j] = source[8 * HALO + t * 10 + j]
            coefficients(co, low_inner + j, source[8 * HALO + 80 + j])
            co[ST, low_inner + j] = source[8 * HALO + 90 + j]
            return carry

        lax.fori_loop(0, HALO, outer, 0)
        lax.fori_loop(0, 10, inner, 0)
    st = Stages(beside, co)
    for low, high in ((-10, 3), (61, 74)):
        sweep(low, high, 16, st.fine_defect(tmp, g, lambda t, r: g[t - 1, r], s, (7,)))
    for low, high in ((-9, 2), (62, 73)):
        sweep(low, high, 16, st.smoothed(u, g, tmp, (7,), Q))
    for j in range(10):
        out[j] = g[7, HALO - 10 + j]
        out[10 + j] = g[7, HALO + ROWS + j]
        out[20 + j] = u[7, HALO - 8 + j]
        out[30 + j] = u[7, HALO + 62 + j]


def edges(g, s, co, u_in, rs_in, e0_in, e1_in, u, rs, e0, e1, out, tmp):
    del u_in, rs_in, e0_in, e1_in
    beside = beside_maker()
    st = Stages(beside, co)

    def both(inner, depth, unroll, body):
        sweep(-depth, inner, unroll, body)
        sweep(ROWS - inner, ROWS + depth, unroll, body)

    both(3, 10, 13, st.fine_defect(tmp, g, lambda t, r: g[t - 1, r], s, range(3, 7)))
    both(2, 9, 11, st.smoothed(u, g, tmp, range(3, 7), Q))
    both(3, 8, 11, st.restricted(rs, tmp, u, lambda t, r: u[t - 1, r], s, (2, 3)))

    def scale(r):
        for m in (2, 3):
            tmp[m, r] = rs[m, r] * co[KINV, r]

    sweep(3, 5, 2, scale)
    sweep(59, 61, 2, scale)
    both(4, 7, 11, st.smoothed(e0, None, tmp, (2, 3), KQ))
    both(7, 6, 13, st.coarse_defect(tmp, e0, lambda m, r: e0[m - 1, r], rs, (3,)))
    both(6, 5, 11, st.smoothed(e1, e0, tmp, (3,), KQ))

    def copy(i, carry):
        for j in range(19):
            r = i * 19 + j
            out[r] = e0[3, HALO - 6 + r]
            q = jnp.minimum(r, 71)
            out[76 + q] = e1[3, HALO - 4 + q]
        return carry

    lax.fori_loop(0, 4, copy, 0)


def rest(g, s, co, u_in, rs_in, e0_in, e1_in, u, rs, e0, e1, e2, send, tmp):
    del u_in, rs_in, e0_in, e1_in
    beside = beside_maker()
    st = Stages(beside, co)
    sweep(-10, 74, 28, st.fine_defect(tmp, g, lambda t, r: g[t - 1, r], s, (1, 2)))
    sweep(-9, 73, 28, st.smoothed(u, g, tmp, (1, 2), Q))
    sweep(-8, 72, 20, st.restricted(rs, tmp, u, lambda t, r: u[t - 1, r], s, (1,)))
    sweep(-7, 71, 26, st.smoothed(e0, None, tmp, (1,), KQ))
    sweep(-6, 70, 26, st.coarse_defect(tmp, e0, lambda m, r: e0[m - 1, r], rs, (2,)))
    sweep(-5, 69, 25, st.smoothed(e1, e0, tmp, (2,), KQ))
    sweep(-4, 68, 24, st.coarse_defect(tmp, e1, lambda m, r: e1[m - 1, r], rs, (3,)))
    smooth = st.smoothed(e2, e1, tmp, (3,), KQ)

    def final(r):
        smooth(r)
        send[r - (HALO - 3)] = e2[3, r]

    sweep(-3, 67, 24, final)


def middle(t0, t1, g, s, co, u_in, rs_in, e0_in, e1_in, e2_in, u, rs, e0, e1, e2, before, sol7, send, gb, tmp, u2):
    del u_in, rs_in, e0_in, e1_in, e2_in
    beside = beside_maker()
    st = Stages(beside, co)

    def fill(i, carry):
        for j in range(8):
            r = i * 8 + j
            gb[HALO + r] = t0[r] + co[ST, HALO + r]
            q = jnp.minimum(r, 59)
            before[HALO + 2 + q] = t0[ROWS + q] + co[ST, HALO + 2 + q]
        return carry

    lax.fori_loop(0, ROWS // 8, fill, 0)
    for j in range(10):
        gb[HALO - 10 + j] = t1[j] + co[ST, HALO - 10 + j]
        gb[HALO + ROWS + j] = t1[10 + j] + co[ST, HALO + ROWS + j]
        before[HALO - 8 + j] = t1[20 + j] + co[ST, HALO - 8 + j]
        before[HALO + 62 + j] = t1[30 + j] + co[ST, HALO + 62 + j]
    sweep(-10, 74, 28, st.fine_defect(tmp, g, lambda t, r: gb[r], s, (0,)))
    sweep(-9, 73, 28, st.smoothed(u, g, tmp, (0,), Q))
    sweep(-8, 72, 20, st.restricted(rs, tmp, u, lambda t, r: u[0, r] if t else before[r], s, (0,)))
    sweep(-7, 71, 26, st.smoothed(e0, None, tmp, (0,), KQ))
    sweep(-6, 70, 26, st.coarse_defect(tmp, e0, lambda m, r: e0[0, r], rs, (1,)))
    sweep(-5, 69, 25, st.smoothed(e1, e0, tmp, (1,), KQ))
    sweep(-4, 68, 24, st.coarse_defect(tmp, e1, lambda m, r: e1[1, r], rs, (2,)))

    def corrected(r):
        q = co[KQ, r]
        late = e1[2, r] + tmp[2, r] + q * around(beside, tmp, 2, r)
        e2[2, r] = late
        u2[0, r] = u[6, r] + 0.5 * (late + e2[3, r])
        u2[1, r] = u[7, r] + e2[3, r]

    sweep(-3, 67, 24, corrected)

    def defect(r):
        tmp[0, r] = (
            s[7, r] + u2[0, r] - co[D, r] * u2[1, r] + co[C, r] * around(beside, u2, 1, r)
        ) * co[INV, r]

    sweep(-2, 66, 23, defect)

    def final(r):
        sol7[0, r] = u2[1, r] + tmp[0, r] + co[Q, r] * around(beside, tmp, 0, r)

    sweep(-1, 65, 22, final)

    def copy(i, carry):
        for j in range(8):
            send[tile_at(0, i, j), :] = sol7[0, HALO + 8 * i + j]
        return carry

    lax.fori_loop(0, ROWS // 8, copy, 0)


def late(t2, s, co, u, rs, e0, e1_in, e2_in, sol7, sol_out, res_out, u2_out, sol2, e1, u2, tmp, sol, sol_nat, res_nat, sems):
    beside = beside_maker()
    st = Stages(beside, co)

    def first_defect(r):
        tmp[0, r] = (
            rs[0, r] + t2[r - (HALO - 6)] - co[KD, r] * e0[0, r] + co[K, r] * around(beside, e0, 0, r)
        ) * co[KINV, r]

    sweep(-6, 70, 26, first_defect)

    def first_smooth(r):
        e1[0, r] = e0[0, r] + tmp[0, r] + co[KQ, r] * around(beside, tmp, 0, r)
        e1[1, r] = e1_in[1, r]

    sweep(-5, 69, 25, first_smooth)

    def second_defect(r):
        k, kd, kinv = co[K, r], co[KD, r], co[KINV, r]
        earlier = (t2[76 + r - (HALO - 4)], e1[0, r])
        for m in (0, 1):
            tmp[m, r] = (rs[m, r] + earlier[m] - kd * e1[m, r] + k * around(beside, e1, m, r)) * kinv

    sweep(-4, 68, 24, second_defect)

    def corrected(r):
        q = co[KQ, r]
        e20 = e1[0, r] + tmp[0, r] + q * around(beside, tmp, 0, r)
        e21 = e1[1, r] + tmp[1, r] + q * around(beside, tmp, 1, r)
        e22, e23 = e2_in[2, r], e2_in[3, r]
        u2_out[0, r] = u[0, r] + 0.5 * e20
        first = u[1, r] + e20
        u2_out[1, r] = first
        u2[1, r] = first
        u2[2, r] = u[2, r] + 0.5 * (e20 + e21)
        u2[3, r] = u[3, r] + e21
        u2[4, r] = u[4, r] + 0.5 * (e21 + e22)
        u2[5, r] = u[5, r] + e22
        u2[6, r] = u[6, r] + 0.5 * (e22 + e23)

    sweep(-3, 67, 18, corrected)
    sweep(-2, 66, 17, st.fine_defect(tmp, u2, lambda t, r: u2[t - 1, r], s, range(2, 7)))
    final = st.smoothed(sol, u2, tmp, range(2, 7), Q)

    def final_all(r):
        final(r)
        sol[7, r] = sol7[0, r]
        sol2[0, r] = sol[2, r]

    sweep(-1, 0, 1, final_all)
    sweep(64, 65, 1, final_all)

    def solve(i, carry):
        for h in range(2):
            for j in range(8):
                r = HALO + 16 * i + 8 * h + j
                final_all(r)
                for t in range(2, 8):
                    sol_nat[tile_at(t - 2, 2 * i + h, j), :] = sol[t, r]
        return carry

    lax.fori_loop(0, ROWS // 16, solve, 0)
    copy_sol = pltpu.make_async_copy(sol_nat, sol_out.at[pl.ds(2 * ROWS * 8, 6 * ROWS * 8)], sems.at[0])
    copy_sol.start()

    def resid(i, carry):
        for h in range(2):
            for j in range(8):
                r = HALO + 16 * i + 8 * h + j
                c, d = co[C, r], co[D, r]
                for t in range(3, 8):
                    res_nat[tile_at(t - 3, 2 * i + h, j), :] = (
                        s[t, r] + sol[t - 1, r] - d * sol[t, r] + c * around(beside, sol, t, r)
                    )
        return carry

    lax.fori_loop(0, ROWS // 16, resid, 0)
    copy_res = pltpu.make_async_copy(res_nat, res_out.at[pl.ds(3 * ROWS * 8, 5 * ROWS * 8)], sems.at[1])
    copy_res.start()
    copy_sol.wait()
    copy_res.wait()


def finish(t3, s, co, before, u2_in, sol2, sol_in, res_in, sol_out, res_out, base, u2, tmp, sol, sol_nat, res_nat, sems):
    del sol_in, res_in
    beside = beside_maker()

    def corrected(r):
        boundary = t3[r - (HALO - 3)]
        u2[0, r] = before[r] + boundary
        u2[1, r] = u2_in[0, r] + 0.5 * boundary

    sweep(-3, 67, 14, corrected)

    def defect(r):
        c, d, inv = co[C, r], co[D, r], co[INV, r]
        tmp[0, r] = (s[0, r] + u2[0, r] - d * u2[1, r] + c * around(beside, u2, 1, r)) * inv
        tmp[1, r] = (s[1, r] + u2[1, r] - d * u2_in[1, r] + c * around(beside, u2_in, 1, r)) * inv

    sweep(-2, 66, 34, defect)

    def final(r):
        q = co[Q, r]
        sol[0, r] = u2[1, r] + tmp[0, r] + q * around(beside, tmp, 0, r)
        sol[1, r] = u2_in[1, r] + tmp[1, r] + q * around(beside, tmp, 1, r)

    sweep(-1, 65, 33, final)

    def resid(i, carry):
        for h in range(4):
            for j in range(8):
                r = HALO + 32 * i + 8 * h + j
                c, d = co[C, r], co[D, r]
                spot = lambda t: tile_at(t, 4 * i + h, j)
                first, second = sol[0, r], sol[1, r]
                sol_nat[spot(0), :] = first
                sol_nat[spot(1), :] = second
                base[spot(0), :] = s[0, r] + co[ST, r] - d * first + c * around(beside, sol, 0, r)
                res_nat[spot(0), :] = s[1, r] + first - d * second + c * around(beside, sol, 1, r)
                res_nat[spot(1), :] = s[2, r] + second - d * sol2[0, r] + c * around(beside, sol2, 0, r)
        return carry

    lax.fori_loop(0, ROWS // 32, resid, 0)
    copies = (
        pltpu.make_async_copy(sol_nat, sol_out.at[pl.ds(0, 2 * ROWS * 8)], sems.at[0]),
        pltpu.make_async_copy(res_nat, res_out.at[pl.ds(ROWS * 8, 2 * ROWS * 8)], sems.at[1]),
    )
    for copy in copies:
        copy.start()
    for copy in copies:
        copy.wait()


def tail(t4, base, res_in, res_out, total, sem):
    del res_in
    total[...] = base[...] + t4[...]
    copy = pltpu.make_async_copy(total, res_out.at[pl.ds(0, ROWS * 8)], sem)
    copy.start()
    copy.wait()


def call(kernel, ins, outs, scratch=(), aliases=None, specs=None, out_specs=None, limit=24):
    return pl.pallas_call(
        kernel,
        out_shape=outs,
        in_specs=specs or [FULL] * len(ins),
        out_specs=out_specs or [FULL] * len(outs),
        scratch_shapes=list(scratch),
        input_output_aliases=aliases or {},
        compiler_params=pltpu.CompilerParams(vmem_limit_bytes=limit * 2**20),
    )(*ins)


def along(block, axis, route):
    count = lax.axis_size(axis)
    pairs = [(i, route(i)) for i in range(count)]
    return lax.ppermute(block, axis, [(i, j) for i, j in pairs if 0 <= j < count])


def ahead(i):
    return i + 1


def on_chip(i):
    return i ^ 1


def off_chip(i):
    return ((i + 1) ^ 1) - 1


def cycle(source, guess, start_state, conduct):
    is_first = (lax.axis_index("tm") == 0).astype(F32).reshape(1)
    is_odd = (lax.axis_index("space") % 2).astype(jnp.int32).reshape(1)
    guess_v, source_v = view(guess), view(source)
    start_v, conduct_v = view(start_state[None]), view(conduct[None])
    halo = rows_of(8 * HALO + 100)
    vmem = lambda steps: pltpu.VMEM((steps, EXT, 8, 128), F32)
    plain = lambda rows: pltpu.VMEM((rows * 8, 128), F32)
    dma = pltpu.SemaphoreType.DMA
    nat = jax.ShapeDtypeStruct((8 * ROWS * 8, 128), F32)
    one = jax.ShapeDtypeStruct((ROWS * 8, 128), F32)

    by_step = lambda x: pltpu.with_memory_space_constraint(x.reshape(-1, ROWS * 8, 128), pltpu.HBM)
    near, far = call(
        edge_pack,
        (is_first, is_odd, by_step(guess_v), by_step(source_v), by_step(start_v), by_step(conduct_v)),
        [halo, halo],
        [pltpu.VMEM((n, 2, 128, 128), F32) for n in (8, 8, 1, 1)] + [dma((4, 2))],
        specs=[SMEM, SMEM] + [ANY] * 4,
        limit=6,
    )
    far_in = along(far, "space", off_chip)
    near_in = along(near, "space", on_chip)
    (send0,) = call(
        last_step_pack,
        (guess_v, source_v, conduct_v),
        [rows_of(124)],
        [pltpu.VMEM((2, ROWS, 8, 128), F32), pltpu.VMEM((ROWS, 8, 128), F32)],
        limit=4,
    )
    t0 = along(send0, "tm", ahead)
    g, s, co, u, rs, e0, e1 = call(
        interior,
        (is_first, guess_v, source_v, start_v, conduct_v),
        [ext(8), ext(8), ext(9), ext(8), ext(4), ext(4), ext(4)],
        [vmem(8)],
        specs=[SMEM] + [FULL] * 4,
        limit=6,
    )
    g, s, co, u, send1 = call(
        edge_first,
        (is_odd, near_in, far_in, g, s, co, u),
        [ext(8), ext(8), ext(9), ext(8), rows_of(40)],
        [vmem(8)],
        aliases={3: 0, 4: 1, 5: 2, 6: 3},
        specs=[SMEM] + [FULL] * 6,
        limit=6,
    )
    t1 = along(send1, "tm", ahead)
    u, rs, e0, e1, send2 = call(
        edges,
        (g, s, co, u, rs, e0, e1),
        [ext(8), ext(4), ext(4), ext(4), rows_of(148)],
        [vmem(8)],
        aliases={3: 0, 4: 1, 5: 2, 6: 3},
        limit=6,
    )
    t2 = along(send2, "tm", ahead)
    u, rs, e0, e1, e2, send3 = call(
        rest,
        (g, s, co, u, rs, e0, e1),
        [ext(8), ext(4), ext(4), ext(4), ext(4), rows_of(70)],
        [vmem(4)],
        aliases={3: 0, 4: 1, 5: 2, 6: 3},
        limit=4,
    )
    t3 = along(send3, "tm", ahead)
    u, rs, e0, e1, e2, before, sol7, send4 = call(
        middle,
        (t0, t1, g, s, co, u, rs, e0, e1, e2),
        [ext(8), ext(4), ext(4), ext(4), ext(4), rows_of(EXT), ext(1), one],
        [pltpu.VMEM((EXT, 8, 128), F32), vmem(4), vmem(2)],
        aliases={5: 0, 6: 1, 7: 2, 8: 3, 9: 4},
        limit=6,
    )
    t4 = along(send4, "tm", ahead)
    sol, res, u2, sol2 = call(
        late,
        (t2, s, co, u, rs, e0, e1, e2, sol7),
        [nat, nat, ext(2), ext(1)],
        [vmem(2), vmem(8), vmem(8), vmem(8), plain(6 * ROWS), plain(5 * ROWS), dma((2,))],
        out_specs=[ANY, ANY, FULL, FULL],
        limit=16,
    )
    sol, res, base = call(
        finish,
        (t3, s, co, before, u2, sol2, sol, res),
        [nat, nat, one],
        [vmem(2), vmem(2), vmem(2), plain(2 * ROWS), plain(2 * ROWS), dma((2,))],
        aliases={6: 0, 7: 1},
        specs=[FULL] * 6 + [ANY] * 2,
        out_specs=[ANY, ANY, FULL],
        limit=6,
    )
    (res,) = call(
        tail,
        (t4, base, res),
        [nat],
        [plain(ROWS), dma],
        aliases={2: 0},
        specs=[FULL, FULL, ANY],
        out_specs=[ANY],
        limit=2,
    )
    return unview(sol, 8), unview(res, 8)


def solution(mesh):
    return jax.shard_map(
        cycle,
        mesh=mesh,
        in_specs=(P("tm", "space", None), P("tm", "space", None), P("space", None), P("space", None)),
        out_specs=(P("tm", "space", None), P("tm", "space", None)),
        check_vma=False,
    )
```

```python
import jax
import jax.numpy as jnp
from jax import lax
from jax.experimental import pallas as pl
from jax.experimental.pallas import tpu as pltpu
from jax.sharding import PartitionSpec as P


F32 = jnp.float32
ROWS = 64
HALO = 11
EXT = ROWS + 2 * HALO
DAMP = 0.8
C, D, INV, Q, K, KD, KINV, KQ, ST = range(9)
FULL = pl.BlockSpec(memory_space=pltpu.VMEM)
SMEM = pl.BlockSpec(memory_space=pltpu.SMEM)
ANY = pl.BlockSpec(memory_space=pltpu.HBM)


def ext(steps):
    return jax.ShapeDtypeStruct((steps, EXT, 8, 128), F32)


def rows_of(count):
    return jax.ShapeDtypeStruct((count, 8, 128), F32)


def view(x):
    steps = x.shape[0]
    return x.reshape(steps, ROWS // 8, 8, 8, 128).transpose(0, 1, 3, 2, 4).reshape(steps * ROWS * 8, 128)


def unview(y, steps):
    return y.reshape(steps, ROWS // 8, 8, 8, 128).transpose(0, 1, 3, 2, 4).reshape(steps, ROWS, 1024)


def at(ref, step, row):
    return ref[pl.ds(step * ROWS * 8 + (row // 8) * 64 + row % 8, 8, 8), :]


def tile_at(step, tile, row):
    return pl.ds(step * ROWS * 8 + tile * 64 + row, 8, 8)


def beside_maker():
    lane = lax.broadcasted_iota(jnp.int32, (8, 128), 1)
    sub = lax.broadcasted_iota(jnp.int32, (8, 128), 0)
    first, last = lane == 0, lane == 127
    top, bottom = sub == 0, sub == 7

    def beside(x):
        before = jnp.where(top, 0.0, pltpu.roll(x, 1, 0))
        after = jnp.where(bottom, 0.0, pltpu.roll(x, 7, 0))
        return pltpu.roll(jnp.where(last, before, x), 1, 1) + pltpu.roll(jnp.where(first, after, x), 127, 1)

    return beside


def around(beside, ref, step, r):
    return ref[step, r - 1] + ref[step, r + 1] + beside(ref[step, r])


def sweep(low, high, unroll, body):
    low, high = low + HALO, high + HALO
    count = high - low
    unroll = min(unroll, count)
    blocks = -(-count // unroll)
    if blocks == 1:
        for j in range(unroll):
            body(low + j)
        return

    def step(i, carry):
        start = jnp.minimum(low + i * unroll, high - unroll)
        for j in range(unroll):
            body(start + j)
        return carry

    lax.fori_loop(0, blocks, step, 0)


def coefficients(co, r, c):
    diag = 1.0 + 4.0 * c
    coarse = 1.0 + 8.0 * c
    recip = 1.0 / diag
    coarse_recip = 1.0 / coarse
    co[C, r] = c
    co[D, r] = diag
    co[INV, r] = DAMP * recip
    co[Q, r] = c * recip
    co[K, r] = 2.0 * c
    co[KD, r] = coarse
    co[KINV, r] = DAMP * coarse_recip
    co[KQ, r] = 2.0 * c * coarse_recip


class Stages:
    def __init__(self, beside, co):
        self.beside, self.co = beside, co

    def fine_defect(self, out, field, earlier, source, steps):
        def body(r):
            c, d, inv = self.co[C, r], self.co[D, r], self.co[INV, r]
            for t in steps:
                out[t, r] = (source[t, r] + earlier(t, r) - d * field[t, r] + c * around(self.beside, field, t, r)) * inv

        return body

    def coarse_defect(self, out, field, earlier, rhs, steps):
        def body(r):
            k, kd, kinv = self.co[K, r], self.co[KD, r], self.co[KINV, r]
            for m in steps:
                out[m, r] = (rhs[m, r] + earlier(m, r) - kd * field[m, r] + k * around(self.beside, field, m, r)) * kinv

        return body

    def smoothed(self, out, field, defect, steps, plane):
        def body(r):
            q = self.co[plane, r]
            for t in steps:
                base = defect[t, r] if field is None else field[t, r] + defect[t, r]
                out[t, r] = base + q * around(self.beside, defect, t, r)

        return body

    def restricted(self, out, scaled, field, earlier, source, pairs):
        def body(r):
            c, d, kinv = self.co[C, r], self.co[D, r], self.co[KINV, r]
            for m in pairs:
                parts = [
                    source[t, r] + earlier(t, r) - d * field[t, r] + c * around(self.beside, field, t, r)
                    for t in (2 * m, 2 * m + 1)
                ]
                both = parts[0] + parts[1]
                out[m, r] = both
                scaled[m, r] = both * kinv

        return body


def edge_pack(is_first, is_odd, guess, source, start, conduct, near, far, gb, sb, tb, cb, sems):
    copies = []
    for n, (src, dst) in enumerate(((guess, gb), (source, sb), (start, tb), (conduct, cb))):
        for m, low in enumerate((0, 384)):
            copies.append(pltpu.make_async_copy(src.at[:, pl.ds(low, 128)], dst.at[:, m], sems.at[n, m]))
    for copy in copies:
        copy.start()
    for copy in copies:
        copy.wait()
    odd = is_odd[0]
    for out, side in ((near, 1 - odd), (far, odd)):

        def outer(j, carry):
            r = j + 5 * side
            here = pl.ds((r // 8) * 64 + r % 8, 8, 8)
            for t in range(8):
                out[t * HALO + j] = gb[t, side, here, :]
            return carry

        def inner(j, carry):
            r = j + 6 * side
            here = pl.ds((r // 8) * 64 + r % 8, 8, 8)
            for t in range(8):
                out[8 * HALO + t * 10 + j] = sb[t, side, here, :]
            out[8 * HALO + 80 + j] = cb[0, side, here, :]
            out[8 * HALO + 90 + j] = tb[0, side, here, :] * is_first[0]
            return carry

        lax.fori_loop(0, HALO, outer, 0)
        lax.fori_loop(0, 10, inner, 0)


def last_step_pack(guess, source, conduct, out, g, e):
    beside = beside_maker()

    def fill(i, carry):
        for j in range(8):
            r = 8 * i + j
            for t in (6, 7):
                g[t - 6, r] = guess[tile_at(t, i, j), :]
            out[r] = g[1, r]
        return carry

    lax.fori_loop(0, ROWS // 8, fill, 0)

    def cond_at(r):
        return conduct[pl.ds((r // 8) * 64 + r % 8, 8, 8), :]

    def defect(i, carry):
        start = 1 + i * 31
        for j in range(31):
            r = start + j
            c = cond_at(r)
            d = 1.0 + 4.0 * c
            right = source[pl.ds(7 * 512 + (r // 8) * 64 + r % 8, 8, 8), :]
            e[r] = (right + g[0, r] - d * g[1, r] + c * around(beside, g, 1, r)) * (DAMP / d)
        return carry

    lax.fori_loop(0, 2, defect, 0)

    def smooth(i, carry):
        start = 2 + i * 30
        for j in range(30):
            r = start + j
            c = cond_at(r)
            q = c / (1.0 + 4.0 * c)
            out[ROWS - 2 + r] = g[1, r] + e[r] + q * (e[r - 1] + e[r + 1] + beside(e[r]))
        return carry

    lax.fori_loop(0, 2, smooth, 0)
    for n, r in enumerate((0, ROWS - 1)):
        out[124 + n] = at(source, 7, r) + g[0, r]
    for n, r in enumerate((1, 2, 61, 62)):
        out[126 + n] = e[r]


def interior(is_first, guess, source, start, conduct, g, s, co, u, rs, e0, e1, tmp):
    beside = beside_maker()

    def fill(i, carry):
        for j in range(8):
            r = HALO + 8 * i + j
            for t in range(8):
                g[t, r] = guess[tile_at(t, i, j), :]
                s[t, r] = source[tile_at(t, i, j), :]
            coefficients(co, r, conduct[tile_at(0, i, j), :])
            co[ST, r] = start[tile_at(0, i, j), :] * is_first[0]
        return carry

    lax.fori_loop(0, ROWS // 8, fill, 0)
    st = Stages(beside, co)
    sweep(1, 63, 16, st.fine_defect(tmp, g, lambda t, r: g[t - 1, r], s, range(3, 8)))
    sweep(2, 62, 15, st.smoothed(u, g, tmp, range(3, 8), Q))
    sweep(3, 61, 15, st.restricted(rs, tmp, u, lambda t, r: u[t - 1, r], s, (2, 3)))
    sweep(4, 60, 28, st.smoothed(e0, None, tmp, (2, 3), KQ))
    sweep(5, 59, 27, st.coarse_defect(tmp, e0, lambda m, r: e0[m - 1, r], rs, (3,)))
    sweep(6, 58, 26, st.smoothed(e1, e0, tmp, (3,), KQ))


def edges(is_odd, near, far, g_in, s_in, co_in, u_in, rs_in, e0_in, e1_in, g, s, co, u, rs, e0, e1, out, tmp):
    del g_in, s_in, co_in, u_in, rs_in, e0_in, e1_in
    beside = beside_maker()
    odd = is_odd[0]
    for source, side in ((near, 1 - odd), (far, odd)):
        low = side * (HALO + ROWS)
        low_inner = side * (HALO + ROWS - 1) + 1

        def outer(j, carry):
            for t in range(8):
                g[t, low + j] = source[t * HALO + j]
            return carry

        def inner(j, carry):
            for t in range(8):
                s[t, low_inner + j] = source[8 * HALO + t * 10 + j]
            coefficients(co, low_inner + j, source[8 * HALO + 80 + j])
            co[ST, low_inner + j] = source[8 * HALO + 90 + j]
            return carry

        lax.fori_loop(0, HALO, outer, 0)
        lax.fori_loop(0, 10, inner, 0)
    st = Stages(beside, co)

    def both(inner, depth, unroll, body):
        sweep(-depth, inner, unroll, body)
        sweep(ROWS - inner, ROWS + depth, unroll, body)

    both(3, 10, 13, st.fine_defect(tmp, g, lambda t, r: g[t - 1, r], s, range(3, 8)))
    both(2, 9, 11, st.smoothed(u, g, tmp, range(3, 8), Q))
    both(3, 8, 11, st.restricted(rs, tmp, u, lambda t, r: u[t - 1, r], s, (2, 3)))

    def scale(r):
        for m in (2, 3):
            tmp[m, r] = rs[m, r] * co[KINV, r]

    sweep(3, 5, 2, scale)
    sweep(59, 61, 2, scale)
    both(4, 7, 11, st.smoothed(e0, None, tmp, (2, 3), KQ))
    both(7, 6, 13, st.coarse_defect(tmp, e0, lambda m, r: e0[m - 1, r], rs, (3,)))
    both(6, 5, 11, st.smoothed(e1, e0, tmp, (3,), KQ))

    def copy(i, carry):
        for j in range(19):
            r = i * 19 + j
            out[r] = e0[3, HALO - 6 + r]
            q = jnp.minimum(r, 71)
            out[76 + q] = e1[3, HALO - 4 + q]
        return carry

    lax.fori_loop(0, 4, copy, 0)


def rest(g, s, co, u_in, rs_in, e0_in, e1_in, u, rs, e0, e1, e2, send, tmp):
    del u_in, rs_in, e0_in, e1_in
    beside = beside_maker()
    st = Stages(beside, co)
    sweep(-10, 74, 42, st.fine_defect(tmp, g, lambda t, r: g[t - 1, r], s, (1, 2)))
    sweep(-9, 73, 41, st.smoothed(u, g, tmp, (1, 2), Q))
    sweep(-8, 72, 90, st.restricted(rs, tmp, u, lambda t, r: u[t - 1, r], s, (1,)))
    sweep(-7, 71, 90, st.smoothed(e0, None, tmp, (1,), KQ))
    sweep(-6, 70, 90, st.coarse_defect(tmp, e0, lambda m, r: e0[m - 1, r], rs, (2,)))
    sweep(-5, 69, 90, st.smoothed(e1, e0, tmp, (2,), KQ))
    sweep(-4, 68, 90, st.coarse_defect(tmp, e1, lambda m, r: e1[m - 1, r], rs, (3,)))
    smooth = st.smoothed(e2, e1, tmp, (3,), KQ)

    def final(r):
        smooth(r)
        send[r - (HALO - 3)] = e2[3, r]

    sweep(-3, 67, 90, final)


def relay(is_odd, t0, near, far):
    odd = is_odd[0]
    for out, side in ((near, 1 - odd), (far, odd)):
        for j in range(10):
            out[j] = t0[54 * side + j]
        for j in range(6):
            out[10 + j] = t0[ROWS + 54 * side + j]
        for j in range(2):
            out[16 + j] = t0[126 + 2 * side + j]
        out[18] = t0[124 + side]


def middle(
    is_odd, t0, near, far, g, s, co, u_in, rs_in, e0_in, e1_in, e2_in,
    u, rs, e0, e1, e2, before, sol7, send, gb, er, br, tmp, u2,
):
    del u_in, rs_in, e0_in, e1_in, e2_in
    beside = beside_maker()
    st = Stages(beside, co)
    odd = is_odd[0]

    def fill(i, carry):
        for j in range(16):
            r = i * 16 + j
            gb[0, HALO + r] = t0[r]
            q = jnp.minimum(r, 59)
            before[HALO + 2 + q] = t0[ROWS + q] + co[ST, HALO + 2 + q]
        return carry

    lax.fori_loop(0, ROWS // 16, fill, 0)
    for source, side in ((near, 1 - odd), (far, odd)):
        for j in range(10):
            gb[0, 1 + 74 * side + j] = source[j]
        for j in range(6):
            r = 3 + 74 * side + j
            before[r] = source[10 + j] + co[ST, r]
        for j in range(2):
            er[8 + 68 * side + j] = source[16 + j]
        br[10 + 65 * side] = source[18]
    for n, r in enumerate((HALO, HALO + 63)):
        br[r] = t0[124 + n]
    for n, r in enumerate((1, 2, 61, 62)):
        er[HALO + r] = t0[126 + n]
    for r in (10, 11, 74, 75):
        er[r] = (br[r] - co[D, r] * gb[0, r] + co[C, r] * around(beside, gb, 0, r)) * co[INV, r]
    for r in (9, 10, 11, 12, 73, 74, 75, 76):
        edge = gb[0, r] + er[r] + co[Q, r] * (er[r - 1] + er[r + 1] + beside(er[r]))
        before[r] = edge + co[ST, r]
    sweep(-10, 74, 90, st.fine_defect(tmp, g, lambda t, r: gb[0, r] + co[ST, r], s, (0,)))
    sweep(-9, 73, 90, st.smoothed(u, g, tmp, (0,), Q))
    sweep(-8, 72, 90, st.restricted(rs, tmp, u, lambda t, r: u[0, r] if t else before[r], s, (0,)))
    sweep(-7, 71, 90, st.smoothed(e0, None, tmp, (0,), KQ))
    sweep(-6, 70, 90, st.coarse_defect(tmp, e0, lambda m, r: e0[0, r], rs, (1,)))
    sweep(-5, 69, 90, st.smoothed(e1, e0, tmp, (1,), KQ))
    sweep(-4, 68, 90, st.coarse_defect(tmp, e1, lambda m, r: e1[1, r], rs, (2,)))

    def corrected(r):
        q = co[KQ, r]
        late = e1[2, r] + tmp[2, r] + q * around(beside, tmp, 2, r)
        e2[2, r] = late
        u2[0, r] = u[6, r] + 0.5 * (late + e2[3, r])
        u2[1, r] = u[7, r] + e2[3, r]

    sweep(-3, 67, 90, corrected)

    def defect(r):
        tmp[0, r] = (
            s[7, r] + u2[0, r] - co[D, r] * u2[1, r] + co[C, r] * around(beside, u2, 1, r)
        ) * co[INV, r]

    sweep(-2, 66, 90, defect)

    def final(r):
        sol7[0, r] = u2[1, r] + tmp[0, r] + co[Q, r] * around(beside, tmp, 0, r)

    sweep(-1, 65, 90, final)

    def copy(i, carry):
        for j in range(8):
            send[tile_at(0, i, j), :] = sol7[0, HALO + 8 * i + j]
        return carry

    lax.fori_loop(0, ROWS // 8, copy, 0)


def late(t2, s, co, u, rs, e0, e1_in, e2_in, sol7, sol_out, res_out, u2_out, sol2, e1, u2, tmp, sol, sol_nat, res_nat, sems):
    beside = beside_maker()
    st = Stages(beside, co)

    def first_defect(r):
        tmp[0, r] = (
            rs[0, r] + t2[r - (HALO - 6)] - co[KD, r] * e0[0, r] + co[K, r] * around(beside, e0, 0, r)
        ) * co[KINV, r]

    sweep(-6, 70, 26, first_defect)

    def first_smooth(r):
        e1[0, r] = e0[0, r] + tmp[0, r] + co[KQ, r] * around(beside, tmp, 0, r)
        e1[1, r] = e1_in[1, r]

    sweep(-5, 69, 25, first_smooth)

    def second_defect(r):
        k, kd, kinv = co[K, r], co[KD, r], co[KINV, r]
        earlier = (t2[76 + r - (HALO - 4)], e1[0, r])
        for m in (0, 1):
            tmp[m, r] = (rs[m, r] + earlier[m] - kd * e1[m, r] + k * around(beside, e1, m, r)) * kinv

    sweep(-4, 68, 24, second_defect)

    def corrected(r):
        q = co[KQ, r]
        e20 = e1[0, r] + tmp[0, r] + q * around(beside, tmp, 0, r)
        e21 = e1[1, r] + tmp[1, r] + q * around(beside, tmp, 1, r)
        e22, e23 = e2_in[2, r], e2_in[3, r]
        u2_out[0, r] = u[0, r] + 0.5 * e20
        first = u[1, r] + e20
        u2_out[1, r] = first
        u2[1, r] = first
        u2[2, r] = u[2, r] + 0.5 * (e20 + e21)
        u2[3, r] = u[3, r] + e21
        u2[4, r] = u[4, r] + 0.5 * (e21 + e22)
        u2[5, r] = u[5, r] + e22
        u2[6, r] = u[6, r] + 0.5 * (e22 + e23)

    sweep(-3, 67, 18, corrected)
    sweep(-2, 66, 17, st.fine_defect(tmp, u2, lambda t, r: u2[t - 1, r], s, range(2, 7)))
    final = st.smoothed(sol, u2, tmp, range(2, 7), Q)

    def final_all(r):
        final(r)
        sol[7, r] = sol7[0, r]
        sol2[0, r] = sol[2, r]

    sweep(-1, 0, 1, final_all)
    sweep(64, 65, 1, final_all)

    def solve(i, carry):
        for h in range(2):
            for j in range(8):
                r = HALO + 16 * i + 8 * h + j
                final_all(r)
                for t in range(2, 8):
                    sol_nat[tile_at(t - 2, 2 * i + h, j), :] = sol[t, r]
        return carry

    lax.fori_loop(0, ROWS // 16, solve, 0)
    copy_sol = pltpu.make_async_copy(sol_nat, sol_out.at[pl.ds(2 * ROWS * 8, 6 * ROWS * 8)], sems.at[0])
    copy_sol.start()

    def resid(i, carry):
        for h in range(2):
            for j in range(8):
                r = HALO + 16 * i + 8 * h + j
                c, d = co[C, r], co[D, r]
                for t in range(3, 8):
                    res_nat[tile_at(t - 3, 2 * i + h, j), :] = (
                        s[t, r] + sol[t - 1, r] - d * sol[t, r] + c * around(beside, sol, t, r)
                    )
        return carry

    lax.fori_loop(0, ROWS // 16, resid, 0)
    copy_res = pltpu.make_async_copy(res_nat, res_out.at[pl.ds(3 * ROWS * 8, 5 * ROWS * 8)], sems.at[1])
    copy_res.start()
    copy_sol.wait()
    copy_res.wait()


def finish(t3, s, co, before, u2_in, sol2, sol_in, res_in, sol_out, res_out, base, u2, tmp, sol, sol_nat, res_nat, sems):
    del sol_in, res_in
    beside = beside_maker()

    def corrected(r):
        boundary = t3[r - (HALO - 3)]
        u2[0, r] = before[r] + boundary
        u2[1, r] = u2_in[0, r] + 0.5 * boundary

    sweep(-3, 67, 14, corrected)

    def defect(r):
        c, d, inv = co[C, r], co[D, r], co[INV, r]
        tmp[0, r] = (s[0, r] + u2[0, r] - d * u2[1, r] + c * around(beside, u2, 1, r)) * inv
        tmp[1, r] = (s[1, r] + u2[1, r] - d * u2_in[1, r] + c * around(beside, u2_in, 1, r)) * inv

    sweep(-2, 66, 34, defect)

    def final(r):
        q = co[Q, r]
        sol[0, r] = u2[1, r] + tmp[0, r] + q * around(beside, tmp, 0, r)
        sol[1, r] = u2_in[1, r] + tmp[1, r] + q * around(beside, tmp, 1, r)

    sweep(-1, 65, 33, final)

    def resid(i, carry):
        for h in range(4):
            for j in range(8):
                r = HALO + 32 * i + 8 * h + j
                c, d = co[C, r], co[D, r]
                spot = lambda t: tile_at(t, 4 * i + h, j)
                first, second = sol[0, r], sol[1, r]
                sol_nat[spot(0), :] = first
                sol_nat[spot(1), :] = second
                base[spot(0), :] = s[0, r] + co[ST, r] - d * first + c * around(beside, sol, 0, r)
                res_nat[spot(0), :] = s[1, r] + first - d * second + c * around(beside, sol, 1, r)
                res_nat[spot(1), :] = s[2, r] + second - d * sol2[0, r] + c * around(beside, sol2, 0, r)
        return carry

    lax.fori_loop(0, ROWS // 32, resid, 0)
    copies = (
        pltpu.make_async_copy(sol_nat, sol_out.at[pl.ds(0, 2 * ROWS * 8)], sems.at[0]),
        pltpu.make_async_copy(res_nat, res_out.at[pl.ds(ROWS * 8, 2 * ROWS * 8)], sems.at[1]),
    )
    for copy in copies:
        copy.start()
    for copy in copies:
        copy.wait()


def tail(t4, base, res_in, res_out, total, sem):
    del res_in
    total[...] = base[...] + t4[...]
    copy = pltpu.make_async_copy(total, res_out.at[pl.ds(0, ROWS * 8)], sem)
    copy.start()
    copy.wait()


def call(kernel, ins, outs, scratch=(), aliases=None, specs=None, out_specs=None, limit=24):
    return pl.pallas_call(
        kernel,
        out_shape=outs,
        in_specs=specs or [FULL] * len(ins),
        out_specs=out_specs or [FULL] * len(outs),
        scratch_shapes=list(scratch),
        input_output_aliases=aliases or {},
        compiler_params=pltpu.CompilerParams(vmem_limit_bytes=limit * 2**20),
    )(*ins)


def along(block, axis, route):
    count = lax.axis_size(axis)
    pairs = [(i, route(i)) for i in range(count)]
    return lax.ppermute(block, axis, [(i, j) for i, j in pairs if 0 <= j < count])


def ahead(i):
    return i + 1


def on_chip(i):
    return i ^ 1


def off_chip(i):
    return ((i + 1) ^ 1) - 1


def cycle(source, guess, start_state, conduct):
    is_first = (lax.axis_index("tm") == 0).astype(F32).reshape(1)
    is_odd = (lax.axis_index("space") % 2).astype(jnp.int32).reshape(1)
    guess_v, source_v = view(guess), view(source)
    start_v, conduct_v = view(start_state[None]), view(conduct[None])
    halo = rows_of(8 * HALO + 100)
    vmem = lambda steps: pltpu.VMEM((steps, EXT, 8, 128), F32)
    plain = lambda rows: pltpu.VMEM((rows * 8, 128), F32)
    dma = pltpu.SemaphoreType.DMA
    nat = jax.ShapeDtypeStruct((8 * ROWS * 8, 128), F32)
    one = jax.ShapeDtypeStruct((ROWS * 8, 128), F32)

    by_step = lambda x: pltpu.with_memory_space_constraint(x.reshape(-1, ROWS * 8, 128), pltpu.HBM)
    near, far = call(
        edge_pack,
        (is_first, is_odd, by_step(guess_v), by_step(source_v), by_step(start_v), by_step(conduct_v)),
        [halo, halo],
        [pltpu.VMEM((n, 2, 128, 128), F32) for n in (8, 8, 1, 1)] + [dma((4, 2))],
        specs=[SMEM, SMEM] + [ANY] * 4,
        limit=6,
    )
    far_in = along(far, "space", off_chip)
    near_in = along(near, "space", on_chip)
    (send0,) = call(
        last_step_pack,
        (guess_v, source_v, conduct_v),
        [rows_of(130)],
        [pltpu.VMEM((2, ROWS, 8, 128), F32), pltpu.VMEM((ROWS, 8, 128), F32)],
        limit=4,
    )
    t0 = along(send0, "tm", ahead)
    g, s, co, u, rs, e0, e1 = call(
        interior,
        (is_first, guess_v, source_v, start_v, conduct_v),
        [ext(8), ext(8), ext(9), ext(8), ext(4), ext(4), ext(4)],
        [vmem(8)],
        specs=[SMEM] + [FULL] * 4,
        limit=6,
    )
    g, s, co, u, rs, e0, e1, send2 = call(
        edges,
        (is_odd, near_in, far_in, g, s, co, u, rs, e0, e1),
        [ext(8), ext(8), ext(9), ext(8), ext(4), ext(4), ext(4), rows_of(148)],
        [vmem(8)],
        aliases={n + 3: n for n in range(7)},
        specs=[SMEM] + [FULL] * 9,
        limit=6,
    )
    t2 = along(send2, "tm", ahead)
    near, far = call(relay, (is_odd, t0), [rows_of(19), rows_of(19)], specs=[SMEM, FULL], limit=1)
    far_in = along(far, "space", off_chip)
    near_in = along(near, "space", on_chip)
    u, rs, e0, e1, e2, send3 = call(
        rest,
        (g, s, co, u, rs, e0, e1),
        [ext(8), ext(4), ext(4), ext(4), ext(4), rows_of(70)],
        [vmem(4)],
        aliases={3: 0, 4: 1, 5: 2, 6: 3},
        limit=4,
    )
    t3 = along(send3, "tm", ahead)
    u, rs, e0, e1, e2, before, sol7, send4 = call(
        middle,
        (is_odd, t0, near_in, far_in, g, s, co, u, rs, e0, e1, e2),
        [ext(8), ext(4), ext(4), ext(4), ext(4), rows_of(EXT), ext(1), one],
        [vmem(1), pltpu.VMEM((EXT, 8, 128), F32), pltpu.VMEM((EXT, 8, 128), F32), vmem(4), vmem(2)],
        aliases={n + 7: n for n in range(5)},
        specs=[SMEM] + [FULL] * 11,
        limit=6,
    )
    t4 = along(send4, "tm", ahead)
    sol, res, u2, sol2 = call(
        late,
        (t2, s, co, u, rs, e0, e1, e2, sol7),
        [nat, nat, ext(2), ext(1)],
        [vmem(2), vmem(8), vmem(8), vmem(8), plain(6 * ROWS), plain(5 * ROWS), dma((2,))],
        out_specs=[ANY, ANY, FULL, FULL],
        limit=16,
    )
    sol, res, base = call(
        finish,
        (t3, s, co, before, u2, sol2, sol, res),
        [nat, nat, one],
        [vmem(2), vmem(2), vmem(2), plain(2 * ROWS), plain(2 * ROWS), dma((2,))],
        aliases={6: 0, 7: 1},
        specs=[FULL] * 6 + [ANY] * 2,
        out_specs=[ANY, ANY, FULL],
        limit=6,
    )
    (res,) = call(
        tail,
        (t4, base, res),
        [nat],
        [plain(ROWS), dma],
        aliases={2: 0},
        specs=[FULL, FULL, ANY],
        out_specs=[ANY],
        limit=2,
    )
    return unview(sol, 8), unview(res, 8)


def solution(mesh):
    return jax.shard_map(
        cycle,
        mesh=mesh,
        in_specs=(P("tm", "space", None), P("tm", "space", None), P("space", None), P("space", None)),
        out_specs=(P("tm", "space", None), P("tm", "space", None)),
        check_vma=False,
    )
```

```python
import jax
import jax.numpy as jnp
from jax import lax
from jax.experimental import pallas as pl
from jax.experimental.pallas import tpu as pltpu
from jax.sharding import PartitionSpec as P


F32 = jnp.float32
ROWS = 64
HALO = 11
EXT = ROWS + 2 * HALO
DAMP = 0.8
C, D, INV, Q, K, KD, KINV, KQ, ST = range(9)
FULL = pl.BlockSpec(memory_space=pltpu.VMEM)
SMEM = pl.BlockSpec(memory_space=pltpu.SMEM)
ANY = pl.BlockSpec(memory_space=pltpu.HBM)


def ext(steps):
    return jax.ShapeDtypeStruct((steps, EXT, 8, 128), F32)


def rows_of(count):
    return jax.ShapeDtypeStruct((count, 8, 128), F32)


def view(x):
    steps = x.shape[0]
    return x.reshape(steps, ROWS // 8, 8, 8, 128).transpose(0, 1, 3, 2, 4).reshape(steps * ROWS * 8, 128)


def unview(y, steps):
    return y.reshape(steps, ROWS // 8, 8, 8, 128).transpose(0, 1, 3, 2, 4).reshape(steps, ROWS, 1024)


def at(ref, step, row):
    return ref[pl.ds(step * ROWS * 8 + (row // 8) * 64 + row % 8, 8, 8), :]


def tile_at(step, tile, row):
    return pl.ds(step * ROWS * 8 + tile * 64 + row, 8, 8)


def beside_maker():
    lane = lax.broadcasted_iota(jnp.int32, (8, 128), 1)
    sub = lax.broadcasted_iota(jnp.int32, (8, 128), 0)
    first, last = lane == 0, lane == 127
    top, bottom = sub == 0, sub == 7

    def beside(x):
        before = jnp.where(top, 0.0, pltpu.roll(x, 1, 0))
        after = jnp.where(bottom, 0.0, pltpu.roll(x, 7, 0))
        return pltpu.roll(jnp.where(last, before, x), 1, 1) + pltpu.roll(jnp.where(first, after, x), 127, 1)

    return beside


def around(beside, ref, step, r):
    return ref[step, r - 1] + ref[step, r + 1] + beside(ref[step, r])


def sweep(low, high, unroll, body):
    low, high = low + HALO, high + HALO
    count = high - low
    unroll = min(unroll, count)
    blocks = -(-count // unroll)
    if blocks == 1:
        for j in range(unroll):
            body(low + j)
        return

    def step(i, carry):
        start = jnp.minimum(low + i * unroll, high - unroll)
        for j in range(unroll):
            body(start + j)
        return carry

    lax.fori_loop(0, blocks, step, 0)


def coefficients(co, r, c):
    diag = 1.0 + 4.0 * c
    coarse = 1.0 + 8.0 * c
    recip = 1.0 / diag
    coarse_recip = 1.0 / coarse
    co[C, r] = c
    co[D, r] = diag
    co[INV, r] = DAMP * recip
    co[Q, r] = c * recip
    co[K, r] = 2.0 * c
    co[KD, r] = coarse
    co[KINV, r] = DAMP * coarse_recip
    co[KQ, r] = 2.0 * c * coarse_recip


class Stages:
    def __init__(self, beside, co):
        self.beside, self.co = beside, co

    def fine_defect(self, out, field, earlier, source, steps):
        def body(r):
            c, d, inv = self.co[C, r], self.co[D, r], self.co[INV, r]
            for t in steps:
                out[t, r] = (source[t, r] + earlier(t, r) - d * field[t, r] + c * around(self.beside, field, t, r)) * inv

        return body

    def coarse_defect(self, out, field, earlier, rhs, steps):
        def body(r):
            k, kd, kinv = self.co[K, r], self.co[KD, r], self.co[KINV, r]
            for m in steps:
                out[m, r] = (rhs[m, r] + earlier(m, r) - kd * field[m, r] + k * around(self.beside, field, m, r)) * kinv

        return body

    def smoothed(self, out, field, defect, steps, plane):
        def body(r):
            q = self.co[plane, r]
            for t in steps:
                base = defect[t, r] if field is None else field[t, r] + defect[t, r]
                out[t, r] = base + q * around(self.beside, defect, t, r)

        return body

    def restricted(self, out, scaled, field, earlier, source, pairs):
        def body(r):
            c, d, kinv = self.co[C, r], self.co[D, r], self.co[KINV, r]
            for m in pairs:
                parts = [
                    source[t, r] + earlier(t, r) - d * field[t, r] + c * around(self.beside, field, t, r)
                    for t in (2 * m, 2 * m + 1)
                ]
                both = parts[0] + parts[1]
                out[m, r] = both
                scaled[m, r] = both * kinv

        return body


def edge_pack(is_first, is_odd, guess, source, start, conduct, near, far, gb, sb, tb, cb, sems):
    pairs = ((guess, gb), (source, sb), (start, tb), (conduct, cb))

    def copies(spans):
        return [
            pltpu.make_async_copy(src.at[:, pl.ds(low, size)], dst.at[:, pl.ds(low, size)], sems.at[n, k])
            for k, low, size in spans
            for n, (src, dst) in enumerate(pairs)
        ]

    outer_tiles, inner_tiles = copies(((0, 0, 128), (1, 384, 128))), copies(((2, 128, 256),))
    for copy in outer_tiles + inner_tiles:
        copy.start()
    for copy in outer_tiles:
        copy.wait()
    odd = is_odd[0]
    for out, side in ((near, 1 - odd), (far, odd)):

        def outer(j, carry):
            r = j + 53 * side
            here = pl.ds((r // 8) * 64 + r % 8, 8, 8)
            for t in range(8):
                out[t * HALO + j] = gb[t, here, :]
            return carry

        def inner(j, carry):
            r = j + 54 * side
            here = pl.ds((r // 8) * 64 + r % 8, 8, 8)
            for t in range(8):
                out[8 * HALO + t * 10 + j] = sb[t, here, :]
            out[8 * HALO + 80 + j] = cb[0, here, :]
            out[8 * HALO + 90 + j] = tb[0, here, :] * is_first[0]
            return carry

        lax.fori_loop(0, HALO, outer, 0)
        lax.fori_loop(0, 10, inner, 0)
    for copy in inner_tiles:
        copy.wait()


def last_step_pack(guess, source, conduct, out, g, e):
    beside = beside_maker()

    def fill(i, carry):
        for j in range(8):
            r = 8 * i + j
            for t in (6, 7):
                g[t - 6, r] = guess[tile_at(t, i, j), :]
            out[r] = g[1, r]
        return carry

    lax.fori_loop(0, ROWS // 8, fill, 0)

    def cond_at(r):
        return conduct[pl.ds((r // 8) * 64 + r % 8, 8, 8), :]

    def defect(i, carry):
        start = 1 + i * 31
        for j in range(31):
            r = start + j
            c = cond_at(r)
            d = 1.0 + 4.0 * c
            right = source[pl.ds(7 * 512 + (r // 8) * 64 + r % 8, 8, 8), :]
            e[r] = (right + g[0, r] - d * g[1, r] + c * around(beside, g, 1, r)) * (DAMP / d)
        return carry

    lax.fori_loop(0, 2, defect, 0)

    def smooth(i, carry):
        start = 2 + i * 30
        for j in range(30):
            r = start + j
            c = cond_at(r)
            q = c / (1.0 + 4.0 * c)
            out[ROWS - 2 + r] = g[1, r] + e[r] + q * (e[r - 1] + e[r + 1] + beside(e[r]))
        return carry

    lax.fori_loop(0, 2, smooth, 0)
    for n, r in enumerate((0, ROWS - 1)):
        out[124 + n] = at(source, 7, r) + g[0, r]
    for n, r in enumerate((1, 2, 61, 62)):
        out[126 + n] = e[r]


def interior(is_first, guess, source, start, conduct, g, s, co, u, rs, e0, e1, tmp):
    beside = beside_maker()

    def fill(i, carry):
        for j in range(8):
            r = HALO + 8 * i + j
            for t in range(8):
                g[t, r] = guess[tile_at(t, i, j), :]
                s[t, r] = source[tile_at(t, i, j), :]
            coefficients(co, r, conduct[tile_at(0, i, j), :])
            co[ST, r] = start[tile_at(0, i, j), :] * is_first[0]
        return carry

    lax.fori_loop(0, ROWS // 8, fill, 0)
    st = Stages(beside, co)
    sweep(1, 63, 90, st.fine_defect(tmp, g, lambda t, r: g[t - 1, r], s, range(3, 8)))
    sweep(2, 62, 90, st.smoothed(u, g, tmp, range(3, 8), Q))
    sweep(3, 61, 90, st.restricted(rs, tmp, u, lambda t, r: u[t - 1, r], s, (2, 3)))
    sweep(4, 60, 90, st.smoothed(e0, None, tmp, (2, 3), KQ))
    sweep(5, 59, 90, st.coarse_defect(tmp, e0, lambda m, r: e0[m - 1, r], rs, (3,)))
    sweep(6, 58, 90, st.smoothed(e1, e0, tmp, (3,), KQ))


def edges(is_odd, near, far, g_in, s_in, co_in, u_in, rs_in, e0_in, e1_in, g, s, co, u, rs, e0, e1, out, tmp):
    del g_in, s_in, co_in, u_in, rs_in, e0_in, e1_in
    beside = beside_maker()
    odd = is_odd[0]
    for source, side in ((near, 1 - odd), (far, odd)):
        low = side * (HALO + ROWS)
        low_inner = side * (HALO + ROWS - 1) + 1

        def outer(j, carry):
            for t in range(8):
                g[t, low + j] = source[t * HALO + j]
            return carry

        def inner(j, carry):
            for t in range(8):
                s[t, low_inner + j] = source[8 * HALO + t * 10 + j]
            coefficients(co, low_inner + j, source[8 * HALO + 80 + j])
            co[ST, low_inner + j] = source[8 * HALO + 90 + j]
            return carry

        lax.fori_loop(0, HALO, outer, 0)
        lax.fori_loop(0, 10, inner, 0)
    st = Stages(beside, co)

    def both(inner, depth, unroll, body):
        sweep(-depth, inner, unroll, body)
        sweep(ROWS - inner, ROWS + depth, unroll, body)

    both(3, 10, 13, st.fine_defect(tmp, g, lambda t, r: g[t - 1, r], s, range(3, 8)))
    both(2, 9, 11, st.smoothed(u, g, tmp, range(3, 8), Q))
    both(3, 8, 11, st.restricted(rs, tmp, u, lambda t, r: u[t - 1, r], s, (2, 3)))

    def scale(r):
        for m in (2, 3):
            tmp[m, r] = rs[m, r] * co[KINV, r]

    sweep(3, 5, 2, scale)
    sweep(59, 61, 2, scale)
    both(4, 7, 11, st.smoothed(e0, None, tmp, (2, 3), KQ))
    both(7, 6, 13, st.coarse_defect(tmp, e0, lambda m, r: e0[m - 1, r], rs, (3,)))
    both(6, 5, 11, st.smoothed(e1, e0, tmp, (3,), KQ))

    def copy(i, carry):
        for j in range(19):
            r = i * 19 + j
            out[r] = e0[3, HALO - 6 + r]
            q = jnp.minimum(r, 71)
            out[76 + q] = e1[3, HALO - 4 + q]
        return carry

    lax.fori_loop(0, 4, copy, 0)


def rest(g, s, co, u_in, rs_in, e0_in, e1_in, u, rs, e0, e1, e2, send, tmp):
    del u_in, rs_in, e0_in, e1_in
    beside = beside_maker()
    st = Stages(beside, co)
    sweep(-10, 74, 42, st.fine_defect(tmp, g, lambda t, r: g[t - 1, r], s, (1, 2)))
    sweep(-9, 73, 41, st.smoothed(u, g, tmp, (1, 2), Q))
    sweep(-8, 72, 90, st.restricted(rs, tmp, u, lambda t, r: u[t - 1, r], s, (1,)))
    sweep(-7, 71, 90, st.smoothed(e0, None, tmp, (1,), KQ))
    sweep(-6, 70, 90, st.coarse_defect(tmp, e0, lambda m, r: e0[m - 1, r], rs, (2,)))
    sweep(-5, 69, 90, st.smoothed(e1, e0, tmp, (2,), KQ))
    sweep(-4, 68, 90, st.coarse_defect(tmp, e1, lambda m, r: e1[m - 1, r], rs, (3,)))
    smooth = st.smoothed(e2, e1, tmp, (3,), KQ)

    def final(r):
        smooth(r)
        send[r - (HALO - 3)] = e2[3, r]

    sweep(-3, 67, 90, final)


def relay(is_odd, t0, near, far):
    odd = is_odd[0]
    for out, side in ((near, 1 - odd), (far, odd)):
        for j in range(10):
            out[j] = t0[54 * side + j]
        for j in range(6):
            out[10 + j] = t0[ROWS + 54 * side + j]
        for j in range(2):
            out[16 + j] = t0[126 + 2 * side + j]
        out[18] = t0[124 + side]


def middle(
    is_odd, t0, near, far, g, s, co, u_in, rs_in, e0_in, e1_in, e2_in,
    u, rs, e0, e1, e2, before, sol7, send, gb, er, br, tmp, u2,
):
    del u_in, rs_in, e0_in, e1_in, e2_in
    beside = beside_maker()
    st = Stages(beside, co)
    odd = is_odd[0]

    def fill(i, carry):
        for j in range(16):
            r = i * 16 + j
            gb[0, HALO + r] = t0[r]
            q = jnp.minimum(r, 59)
            before[HALO + 2 + q] = t0[ROWS + q] + co[ST, HALO + 2 + q]
        return carry

    lax.fori_loop(0, ROWS // 16, fill, 0)
    for source, side in ((near, 1 - odd), (far, odd)):
        for j in range(10):
            gb[0, 1 + 74 * side + j] = source[j]
        for j in range(6):
            r = 3 + 74 * side + j
            before[r] = source[10 + j] + co[ST, r]
        for j in range(2):
            er[8 + 68 * side + j] = source[16 + j]
        br[10 + 65 * side] = source[18]
    for n, r in enumerate((HALO, HALO + 63)):
        br[r] = t0[124 + n]
    for n, r in enumerate((1, 2, 61, 62)):
        er[HALO + r] = t0[126 + n]
    for r in (10, 11, 74, 75):
        er[r] = (br[r] - co[D, r] * gb[0, r] + co[C, r] * around(beside, gb, 0, r)) * co[INV, r]
    for r in (9, 10, 11, 12, 73, 74, 75, 76):
        edge = gb[0, r] + er[r] + co[Q, r] * (er[r - 1] + er[r + 1] + beside(er[r]))
        before[r] = edge + co[ST, r]
    sweep(-10, 74, 90, st.fine_defect(tmp, g, lambda t, r: gb[0, r] + co[ST, r], s, (0,)))
    sweep(-9, 73, 90, st.smoothed(u, g, tmp, (0,), Q))
    sweep(-8, 72, 90, st.restricted(rs, tmp, u, lambda t, r: u[0, r] if t else before[r], s, (0,)))
    sweep(-7, 71, 90, st.smoothed(e0, None, tmp, (0,), KQ))
    sweep(-6, 70, 90, st.coarse_defect(tmp, e0, lambda m, r: e0[0, r], rs, (1,)))
    sweep(-5, 69, 90, st.smoothed(e1, e0, tmp, (1,), KQ))
    sweep(-4, 68, 90, st.coarse_defect(tmp, e1, lambda m, r: e1[1, r], rs, (2,)))

    def corrected(r):
        q = co[KQ, r]
        late = e1[2, r] + tmp[2, r] + q * around(beside, tmp, 2, r)
        e2[2, r] = late
        u2[0, r] = u[6, r] + 0.5 * (late + e2[3, r])
        u2[1, r] = u[7, r] + e2[3, r]

    sweep(-3, 67, 90, corrected)

    def defect(r):
        tmp[0, r] = (
            s[7, r] + u2[0, r] - co[D, r] * u2[1, r] + co[C, r] * around(beside, u2, 1, r)
        ) * co[INV, r]

    sweep(-2, 66, 90, defect)

    def final(r):
        sol7[0, r] = u2[1, r] + tmp[0, r] + co[Q, r] * around(beside, tmp, 0, r)

    sweep(-1, 65, 90, final)

    def copy(i, carry):
        for j in range(8):
            send[tile_at(0, i, j), :] = sol7[0, HALO + 8 * i + j]
        return carry

    lax.fori_loop(0, ROWS // 8, copy, 0)


def late(t2, s, co, u, rs, e0, e1_in, e2_in, sol7, sol_out, res_out, u2_out, sol2, e1, u2, tmp, sol, sol_nat, res_nat, sems):
    beside = beside_maker()
    st = Stages(beside, co)

    def first_defect(r):
        tmp[0, r] = (
            rs[0, r] + t2[r - (HALO - 6)] - co[KD, r] * e0[0, r] + co[K, r] * around(beside, e0, 0, r)
        ) * co[KINV, r]

    sweep(-6, 70, 90, first_defect)

    def first_smooth(r):
        e1[0, r] = e0[0, r] + tmp[0, r] + co[KQ, r] * around(beside, tmp, 0, r)
        e1[1, r] = e1_in[1, r]

    sweep(-5, 69, 90, first_smooth)

    def second_defect(r):
        k, kd, kinv = co[K, r], co[KD, r], co[KINV, r]
        earlier = (t2[76 + r - (HALO - 4)], e1[0, r])
        for m in (0, 1):
            tmp[m, r] = (rs[m, r] + earlier[m] - kd * e1[m, r] + k * around(beside, e1, m, r)) * kinv

    sweep(-4, 68, 90, second_defect)

    def corrected(r):
        q = co[KQ, r]
        e20 = e1[0, r] + tmp[0, r] + q * around(beside, tmp, 0, r)
        e21 = e1[1, r] + tmp[1, r] + q * around(beside, tmp, 1, r)
        e22, e23 = e2_in[2, r], e2_in[3, r]
        u2_out[0, r] = u[0, r] + 0.5 * e20
        first = u[1, r] + e20
        u2_out[1, r] = first
        u2[1, r] = first
        u2[2, r] = u[2, r] + 0.5 * (e20 + e21)
        u2[3, r] = u[3, r] + e21
        u2[4, r] = u[4, r] + 0.5 * (e21 + e22)
        u2[5, r] = u[5, r] + e22
        u2[6, r] = u[6, r] + 0.5 * (e22 + e23)

    sweep(-3, 67, 90, corrected)
    sweep(-2, 66, 90, st.fine_defect(tmp, u2, lambda t, r: u2[t - 1, r], s, range(2, 7)))
    final = st.smoothed(sol, u2, tmp, range(2, 7), Q)

    def final_all(r):
        final(r)
        sol[7, r] = sol7[0, r]
        sol2[0, r] = sol[2, r]

    sweep(-1, 0, 90, final_all)
    sweep(64, 65, 90, final_all)

    for i in range(ROWS // 8):
        for j in range(8):
            r = HALO + 8 * i + j
            final_all(r)
            for t in range(2, 8):
                sol_nat[t - 2, tile_at(0, i, j), :] = sol[t, r]
    copies = [pltpu.make_async_copy(sol_nat, sol_out.at[pl.ds(2, 6)], sems.at[0])]
    copies[0].start()
    for part in range(2):
        for i in range(4 * part, 4 * part + 4):
            for j in range(8):
                r = HALO + 8 * i + j
                c, d = co[C, r], co[D, r]
                for t in range(3, 8):
                    res_nat[t - 3, tile_at(0, i, j), :] = (
                        s[t, r] + sol[t - 1, r] - d * sol[t, r] + c * around(beside, sol, t, r)
                    )
        rows = pl.ds(part * ROWS * 4, ROWS * 4)
        copies.append(pltpu.make_async_copy(res_nat.at[:, rows], res_out.at[pl.ds(3, 5), rows], sems.at[1 + part]))
        copies[-1].start()
    for copy in copies:
        copy.wait()


def finish(t3, s, co, before, u2_in, sol2, sol_in, sol_out, res, u2, tmp, sol, sol_nat, sem):
    del sol_in
    beside = beside_maker()

    def corrected(r):
        boundary = t3[r - (HALO - 3)]
        u2[0, r] = before[r] + boundary
        u2[1, r] = u2_in[0, r] + 0.5 * boundary

    sweep(-3, 67, 90, corrected)

    def defect(r):
        c, d, inv = co[C, r], co[D, r], co[INV, r]
        tmp[0, r] = (s[0, r] + u2[0, r] - d * u2[1, r] + c * around(beside, u2, 1, r)) * inv
        tmp[1, r] = (s[1, r] + u2[1, r] - d * u2_in[1, r] + c * around(beside, u2_in, 1, r)) * inv

    sweep(-2, 66, 90, defect)

    def final(r):
        q = co[Q, r]
        sol[0, r] = u2[1, r] + tmp[0, r] + q * around(beside, tmp, 0, r)
        sol[1, r] = u2_in[1, r] + tmp[1, r] + q * around(beside, tmp, 1, r)
        if HALO <= r < HALO + ROWS:
            sol_nat[0, tile_at(0, (r - HALO) // 8, (r - HALO) % 8), :] = sol[0, r]
            sol_nat[1, tile_at(0, (r - HALO) // 8, (r - HALO) % 8), :] = sol[1, r]

    sweep(-1, 65, 90, final)

    copy = pltpu.make_async_copy(sol_nat, sol_out.at[pl.ds(0, 2)], sem)
    copy.start()
    for i in range(ROWS // 8):
        for j in range(8):
            r = HALO + 8 * i + j
            c, d = co[C, r], co[D, r]
            first, second = sol[0, r], sol[1, r]
            spot = tile_at(0, i, j)
            res[0, spot, :] = s[0, r] + co[ST, r] - d * first + c * around(beside, sol, 0, r)
            res[1, spot, :] = s[1, r] + first - d * second + c * around(beside, sol, 1, r)
            res[2, spot, :] = s[2, r] + second - d * sol2[0, r] + c * around(beside, sol2, 0, r)
    copy.wait()


def tail(t4, res, res_in, res_out, total, sems):
    del res_in
    ready = pltpu.make_async_copy(res.at[pl.ds(1, 2)], res_out.at[pl.ds(1, 2)], sems.at[0])
    ready.start()
    total[...] = res[pl.ds(0, 1)] + t4[...][None]
    copy = pltpu.make_async_copy(total, res_out.at[pl.ds(0, 1)], sems.at[1])
    copy.start()
    ready.wait()
    copy.wait()


def call(kernel, ins, outs, scratch=(), aliases=None, specs=None, out_specs=None, limit=24):
    return pl.pallas_call(
        kernel,
        out_shape=outs,
        in_specs=specs or [FULL] * len(ins),
        out_specs=out_specs or [FULL] * len(outs),
        scratch_shapes=list(scratch),
        input_output_aliases=aliases or {},
        compiler_params=pltpu.CompilerParams(vmem_limit_bytes=limit * 2**20),
    )(*ins)


def along(block, axis, route):
    count = lax.axis_size(axis)
    pairs = [(i, route(i)) for i in range(count)]
    return lax.ppermute(block, axis, [(i, j) for i, j in pairs if 0 <= j < count])


def ahead(i):
    return i + 1


def on_chip(i):
    return i ^ 1


def off_chip(i):
    return ((i + 1) ^ 1) - 1


def cycle(source, guess, start_state, conduct):
    is_first = (lax.axis_index("tm") == 0).astype(F32).reshape(1)
    is_odd = (lax.axis_index("space") % 2).astype(jnp.int32).reshape(1)
    guess_v, source_v = view(guess), view(source)
    start_v, conduct_v = view(start_state[None]), view(conduct[None])
    halo = rows_of(8 * HALO + 100)
    vmem = lambda steps: pltpu.VMEM((steps, EXT, 8, 128), F32)
    dma = pltpu.SemaphoreType.DMA
    one = jax.ShapeDtypeStruct((ROWS * 8, 128), F32)

    by_step = lambda x: pltpu.with_memory_space_constraint(x.reshape(-1, ROWS * 8, 128), pltpu.HBM)
    stepped = lambda steps: jax.ShapeDtypeStruct((steps, ROWS * 8, 128), F32)
    near, far, guess_v, source_v, start_v, conduct_v = call(
        edge_pack,
        (is_first, is_odd, by_step(guess_v), by_step(source_v), by_step(start_v), by_step(conduct_v)),
        [halo, halo, stepped(8), stepped(8), stepped(1), stepped(1)],
        [dma((4, 3))],
        specs=[SMEM, SMEM] + [ANY] * 4,
        limit=1,
    )
    guess_v, source_v, start_v, conduct_v = (x.reshape(-1, 128) for x in (guess_v, source_v, start_v, conduct_v))
    far_in = along(far, "space", off_chip)
    near_in = along(near, "space", on_chip)
    (send0,) = call(
        last_step_pack,
        (guess_v, source_v, conduct_v),
        [rows_of(130)],
        [pltpu.VMEM((2, ROWS, 8, 128), F32), pltpu.VMEM((ROWS, 8, 128), F32)],
        limit=4,
    )
    t0 = along(send0, "tm", ahead)
    g, s, co, u, rs, e0, e1 = call(
        interior,
        (is_first, guess_v, source_v, start_v, conduct_v),
        [ext(8), ext(8), ext(9), ext(8), ext(4), ext(4), ext(4)],
        [vmem(8)],
        specs=[SMEM] + [FULL] * 4,
        limit=6,
    )
    g, s, co, u, rs, e0, e1, send2 = call(
        edges,
        (is_odd, near_in, far_in, g, s, co, u, rs, e0, e1),
        [ext(8), ext(8), ext(9), ext(8), ext(4), ext(4), ext(4), rows_of(148)],
        [vmem(8)],
        aliases={n + 3: n for n in range(7)},
        specs=[SMEM] + [FULL] * 9,
        limit=6,
    )
    t2 = along(send2, "tm", ahead)
    near, far = call(relay, (is_odd, t0), [rows_of(19), rows_of(19)], specs=[SMEM, FULL], limit=1)
    far_in = along(far, "space", off_chip)
    near_in = along(near, "space", on_chip)
    u, rs, e0, e1, e2, send3 = call(
        rest,
        (g, s, co, u, rs, e0, e1),
        [ext(8), ext(4), ext(4), ext(4), ext(4), rows_of(70)],
        [vmem(4)],
        aliases={3: 0, 4: 1, 5: 2, 6: 3},
        limit=4,
    )
    t3 = along(send3, "tm", ahead)
    u, rs, e0, e1, e2, before, sol7, send4 = call(
        middle,
        (is_odd, t0, near_in, far_in, g, s, co, u, rs, e0, e1, e2),
        [ext(8), ext(4), ext(4), ext(4), ext(4), rows_of(EXT), ext(1), one],
        [vmem(1), pltpu.VMEM((EXT, 8, 128), F32), pltpu.VMEM((EXT, 8, 128), F32), vmem(4), vmem(2)],
        aliases={n + 7: n for n in range(5)},
        specs=[SMEM] + [FULL] * 11,
        limit=6,
    )
    t4 = along(send4, "tm", ahead)
    nat3 = lambda steps: pltpu.VMEM((steps, ROWS * 8, 128), F32)
    sol, res, u2, sol2 = call(
        late,
        (t2, s, co, u, rs, e0, e1, e2, sol7),
        [stepped(8), stepped(8), ext(2), ext(1)],
        [vmem(2), vmem(8), vmem(8), vmem(8), nat3(6), nat3(5), dma((3,))],
        out_specs=[ANY, ANY, FULL, FULL],
        limit=16,
    )
    sol, first_res = call(
        finish,
        (t3, s, co, before, u2, sol2, sol),
        [stepped(8), stepped(3)],
        [vmem(2), vmem(2), vmem(2), nat3(2), dma],
        aliases={6: 0},
        specs=[FULL] * 6 + [ANY],
        out_specs=[ANY, FULL],
        limit=6,
    )
    (res,) = call(
        tail,
        (t4, first_res, res),
        [stepped(8)],
        [nat3(1), dma((2,))],
        aliases={2: 0},
        specs=[FULL, FULL, ANY],
        out_specs=[ANY],
        limit=2,
    )
    return unview(sol, 8), unview(res, 8)


def solution(mesh):
    return jax.shard_map(
        cycle,
        mesh=mesh,
        in_specs=(P("tm", "space", None), P("tm", "space", None), P("space", None), P("space", None)),
        out_specs=(P("tm", "space", None), P("tm", "space", None)),
        check_vma=False,
    )
```

```python
import jax
import jax.numpy as jnp
from jax import lax
from jax.experimental import pallas as pl
from jax.experimental.pallas import tpu as pltpu
from jax.sharding import PartitionSpec as P


F32 = jnp.float32
ROWS = 64
HALO = 11
EXT = ROWS + 2 * HALO
DAMP = 0.8
C, D, INV, Q, K, KD, KINV, KQ, ST = range(9)
FULL = pl.BlockSpec(memory_space=pltpu.VMEM)
SMEM = pl.BlockSpec(memory_space=pltpu.SMEM)
ANY = pl.BlockSpec(memory_space=pltpu.HBM)


def ext(steps):
    return jax.ShapeDtypeStruct((steps, EXT, 8, 128), F32)


def rows_of(count):
    return jax.ShapeDtypeStruct((count, 8, 128), F32)


def view(x):
    steps = x.shape[0]
    return x.reshape(steps, ROWS // 8, 8, 8, 128).transpose(0, 1, 3, 2, 4).reshape(steps * ROWS * 8, 128)


def unview(y, steps):
    return y.reshape(steps, ROWS // 8, 8, 8, 128).transpose(0, 1, 3, 2, 4).reshape(steps, ROWS, 1024)


def at(ref, step, row):
    return ref[pl.ds(step * ROWS * 8 + (row // 8) * 64 + row % 8, 8, 8), :]


def tile_at(step, tile, row):
    return pl.ds(step * ROWS * 8 + tile * 64 + row, 8, 8)


def beside_maker():
    lane = lax.broadcasted_iota(jnp.int32, (8, 128), 1)
    sub = lax.broadcasted_iota(jnp.int32, (8, 128), 0)
    first, last = lane == 0, lane == 127
    top, bottom = sub == 0, sub == 7

    def beside(x):
        before = jnp.where(top, 0.0, pltpu.roll(x, 1, 0))
        after = jnp.where(bottom, 0.0, pltpu.roll(x, 7, 0))
        return pltpu.roll(jnp.where(last, before, x), 1, 1) + pltpu.roll(jnp.where(first, after, x), 127, 1)

    return beside


def around(beside, ref, step, r):
    return ref[step, r - 1] + ref[step, r + 1] + beside(ref[step, r])


def sweep(low, high, unroll, body):
    low, high = low + HALO, high + HALO
    count = high - low
    unroll = min(unroll, count)
    blocks = -(-count // unroll)
    if blocks == 1:
        for j in range(unroll):
            body(low + j)
        return

    def step(i, carry):
        start = jnp.minimum(low + i * unroll, high - unroll)
        for j in range(unroll):
            body(start + j)
        return carry

    lax.fori_loop(0, blocks, step, 0)


def coefficients(co, r, c):
    diag = 1.0 + 4.0 * c
    coarse = 1.0 + 8.0 * c
    recip = 1.0 / diag
    coarse_recip = 1.0 / coarse
    co[C, r] = c
    co[D, r] = diag
    co[INV, r] = DAMP * recip
    co[Q, r] = c * recip
    co[K, r] = 2.0 * c
    co[KD, r] = coarse
    co[KINV, r] = DAMP * coarse_recip
    co[KQ, r] = 2.0 * c * coarse_recip


class Stages:
    def __init__(self, beside, co):
        self.beside, self.co = beside, co

    def fine_defect(self, out, field, earlier, source, steps):
        def body(r):
            c, d, inv = self.co[C, r], self.co[D, r], self.co[INV, r]
            for t in steps:
                out[t, r] = (source[t, r] + earlier(t, r) - d * field[t, r] + c * around(self.beside, field, t, r)) * inv

        return body

    def coarse_defect(self, out, field, earlier, rhs, steps):
        def body(r):
            k, kd, kinv = self.co[K, r], self.co[KD, r], self.co[KINV, r]
            for m in steps:
                out[m, r] = (rhs[m, r] + earlier(m, r) - kd * field[m, r] + k * around(self.beside, field, m, r)) * kinv

        return body

    def smoothed(self, out, field, defect, steps, plane):
        def body(r):
            q = self.co[plane, r]
            for t in steps:
                base = defect[t, r] if field is None else field[t, r] + defect[t, r]
                out[t, r] = base + q * around(self.beside, defect, t, r)

        return body

    def restricted(self, out, scaled, field, earlier, source, pairs):
        def body(r):
            c, d, kinv = self.co[C, r], self.co[D, r], self.co[KINV, r]
            for m in pairs:
                parts = [
                    source[t, r] + earlier(t, r) - d * field[t, r] + c * around(self.beside, field, t, r)
                    for t in (2 * m, 2 * m + 1)
                ]
                both = parts[0] + parts[1]
                out[m, r] = both
                scaled[m, r] = both * kinv

        return body


def edge_pack(
    is_first, is_odd, guess, source, start, conduct, near, far, near_late, far_late, gb, sb, tb, cb, sems
):
    pairs = ((guess, gb), (source, sb), (start, tb), (conduct, cb))

    def copies(spans):
        return [
            pltpu.make_async_copy(src.at[:, pl.ds(low, size)], dst.at[:, pl.ds(low, size)], sems.at[n, k])
            for k, low, size in spans
            for n, (src, dst) in enumerate(pairs)
        ]

    outer_tiles, inner_tiles = copies(((0, 0, 128), (1, 384, 128))), copies(((2, 128, 256),))
    for copy in outer_tiles + inner_tiles:
        copy.start()
    for copy in outer_tiles:
        copy.wait()
    odd = is_odd[0]

    def grab(out, base, ref, t, low, count, scale=None):
        def body(j, carry):
            r = low + j
            value = ref[t, pl.ds((r // 8) * 64 + r % 8, 8, 8), :]
            out[base + j] = value if scale is None else value * scale
            return carry

        lax.fori_loop(0, count, body, 0, unroll=True)

    for out, late_out, side in ((near, near_late, 1 - odd), (far, far_late, odd)):
        for t in range(2, 8):
            grab(out, (t - 2) * 6, gb, t, 58 * side, 6)
        for t in range(3, 8):
            grab(out, 36 + (t - 3) * 5, sb, t, 59 * side, 5)
        grab(out, 61, cb, 0, 59 * side, 5)
        for t in range(2):
            grab(late_out, t * 11, gb, t, 53 * side, 11)
        for t in range(2, 8):
            grab(late_out, 22 + (t - 2) * 5, gb, t, 6 + 47 * side, 5)
        for t in range(3):
            grab(late_out, 52 + t * 10, sb, t, 54 * side, 10)
        for t in range(3, 8):
            grab(late_out, 82 + (t - 3) * 5, sb, t, 5 + 49 * side, 5)
        grab(late_out, 107, cb, 0, 5 + 49 * side, 5)
        grab(late_out, 112, tb, 0, 54 * side, 10, is_first[0])
    for copy in inner_tiles:
        copy.wait()


def last_step_pack(guess, source, conduct, out, g, e):
    beside = beside_maker()

    def fill(i, carry):
        for j in range(8):
            r = 8 * i + j
            for t in (6, 7):
                g[t - 6, r] = guess[tile_at(t, i, j), :]
            out[r] = g[1, r]
        return carry

    lax.fori_loop(0, ROWS // 8, fill, 0)

    def cond_at(r):
        return conduct[pl.ds((r // 8) * 64 + r % 8, 8, 8), :]

    def defect(i, carry):
        start = 1 + i * 31
        for j in range(31):
            r = start + j
            c = cond_at(r)
            d = 1.0 + 4.0 * c
            right = source[pl.ds(7 * 512 + (r // 8) * 64 + r % 8, 8, 8), :]
            e[r] = (right + g[0, r] - d * g[1, r] + c * around(beside, g, 1, r)) * (DAMP / d)
        return carry

    lax.fori_loop(0, 2, defect, 0)

    def smooth(i, carry):
        start = 2 + i * 30
        for j in range(30):
            r = start + j
            c = cond_at(r)
            q = c / (1.0 + 4.0 * c)
            out[ROWS - 2 + r] = g[1, r] + e[r] + q * (e[r - 1] + e[r + 1] + beside(e[r]))
        return carry

    lax.fori_loop(0, 2, smooth, 0)
    for n, r in enumerate((0, ROWS - 1)):
        out[124 + n] = at(source, 7, r) + g[0, r]
    for n, r in enumerate((1, 2, 61, 62)):
        out[126 + n] = e[r]


def interior(is_first, guess, source, start, conduct, g, s, co, u, rs, e0, e1, tmp):
    beside = beside_maker()

    def fill(i, carry):
        for j in range(8):
            r = HALO + 8 * i + j
            for t in range(8):
                g[t, r] = guess[tile_at(t, i, j), :]
                s[t, r] = source[tile_at(t, i, j), :]
            coefficients(co, r, conduct[tile_at(0, i, j), :])
            co[ST, r] = start[tile_at(0, i, j), :] * is_first[0]
        return carry

    lax.fori_loop(0, ROWS // 8, fill, 0)
    st = Stages(beside, co)
    sweep(1, 63, 90, st.fine_defect(tmp, g, lambda t, r: g[t - 1, r], s, range(3, 8)))
    sweep(2, 62, 90, st.smoothed(u, g, tmp, range(3, 8), Q))
    sweep(3, 61, 90, st.restricted(rs, tmp, u, lambda t, r: u[t - 1, r], s, (2, 3)))
    sweep(4, 60, 90, st.smoothed(e0, None, tmp, (2, 3), KQ))
    sweep(5, 59, 90, st.coarse_defect(tmp, e0, lambda m, r: e0[m - 1, r], rs, (3,)))
    sweep(6, 58, 90, st.smoothed(e1, e0, tmp, (3,), KQ))


def both(inner, depth, body):
    sweep(-depth, inner, 99, body)
    sweep(ROWS - inner, ROWS + depth, 99, body)


def scaled(co, rs, tmp):
    def body(r):
        for m in (2, 3):
            tmp[m, r] = rs[m, r] * co[KINV, r]

    return body


def edges(is_odd, near, far, g_in, s_in, co_in, u_in, rs_in, e0_in, e1_in, g, s, co, u, rs, e0, e1, out, tmp):
    del g_in, s_in, co_in, u_in, rs_in, e0_in, e1_in
    beside = beside_maker()
    odd = is_odd[0]
    for source, side in ((near, 1 - odd), (far, odd)):
        for j in range(6):
            for t in range(2, 8):
                g[t, 5 + 70 * side + j] = source[(t - 2) * 6 + j]
        for j in range(5):
            for t in range(3, 8):
                s[t, 6 + 69 * side + j] = source[36 + (t - 3) * 5 + j]
            coefficients(co, 6 + 69 * side + j, source[61 + j])
    st = Stages(beside, co)

    both(3, 5, st.fine_defect(tmp, g, lambda t, r: g[t - 1, r], s, range(3, 8)))
    both(2, 4, st.smoothed(u, g, tmp, range(3, 8), Q))
    both(3, 3, st.restricted(rs, tmp, u, lambda t, r: u[t - 1, r], s, (2, 3)))
    both(5, -3, scaled(co, rs, tmp))
    both(4, 2, st.smoothed(e0, None, tmp, (2, 3), KQ))
    both(7, 1, st.coarse_defect(tmp, e0, lambda m, r: e0[m - 1, r], rs, (3,)))
    both(6, 0, st.smoothed(e1, e0, tmp, (3,), KQ))
    for r in range(ROWS):
        out[r] = e0[3, HALO + r]
        out[ROWS + r] = e1[3, HALO + r]


def rest(
    is_odd, near, far, g_in, s_in, co_in, u_in, rs_in, e0_in, e1_in, g, s, co, u, rs, e0, e1, e2, send, tmp
):
    del g_in, s_in, co_in, u_in, rs_in, e0_in, e1_in
    beside = beside_maker()
    st = Stages(beside, co)
    odd = is_odd[0]
    for source, side in ((near, 1 - odd), (far, odd)):
        for j in range(11):
            for t in range(2):
                g[t, 75 * side + j] = source[t * 11 + j]
        for j in range(5):
            for t in range(2, 8):
                g[t, 81 * side + j] = source[22 + (t - 2) * 5 + j]
            for t in range(3, 8):
                s[t, 1 + 79 * side + j] = source[82 + (t - 3) * 5 + j]
            coefficients(co, 1 + 79 * side + j, source[107 + j])
        for j in range(10):
            for t in range(3):
                s[t, 1 + 74 * side + j] = source[52 + t * 10 + j]
            co[ST, 1 + 74 * side + j] = source[112 + j]
    both(-3, 10, st.fine_defect(tmp, g, lambda t, r: g[t - 1, r], s, range(3, 8)))
    both(-4, 9, st.smoothed(u, g, tmp, range(3, 8), Q))
    both(-3, 8, st.restricted(rs, tmp, u, lambda t, r: u[t - 1, r], s, (2, 3)))
    both(-1, 3, scaled(co, rs, tmp))
    both(-2, 7, st.smoothed(e0, None, tmp, (2, 3), KQ))
    both(1, 6, st.coarse_defect(tmp, e0, lambda m, r: e0[m - 1, r], rs, (3,)))
    both(0, 5, st.smoothed(e1, e0, tmp, (3,), KQ))
    sweep(-10, 74, 90, st.fine_defect(tmp, g, lambda t, r: g[t - 1, r], s, (1, 2)))
    sweep(-9, 73, 90, st.smoothed(u, g, tmp, (1, 2), Q))
    sweep(-8, 72, 90, st.restricted(rs, tmp, u, lambda t, r: u[t - 1, r], s, (1,)))
    sweep(-7, 71, 90, st.smoothed(e0, None, tmp, (1,), KQ))
    sweep(-6, 70, 90, st.coarse_defect(tmp, e0, lambda m, r: e0[m - 1, r], rs, (2,)))
    sweep(-5, 69, 90, st.smoothed(e1, e0, tmp, (2,), KQ))
    sweep(-4, 68, 90, st.coarse_defect(tmp, e1, lambda m, r: e1[m - 1, r], rs, (3,)))
    smooth = st.smoothed(e2, e1, tmp, (3,), KQ)

    def final(r):
        smooth(r)
        send[r - (HALO - 3)] = e2[3, r]

    sweep(-3, 67, 90, final)


def relay(is_odd, t0, near, far):
    odd = is_odd[0]
    for out, side in ((near, 1 - odd), (far, odd)):
        for j in range(10):
            out[j] = t0[54 * side + j]
        for j in range(6):
            out[10 + j] = t0[ROWS + 54 * side + j]
        for j in range(2):
            out[16 + j] = t0[126 + 2 * side + j]
        out[18] = t0[124 + side]


def middle(
    is_odd, t0, near, far, g, s, co, u_in, rs_in, e0_in, e1_in, e2_in,
    u, rs, e0, e1, e2, before, sol7, send, gb, er, br, tmp, u2,
):
    del u_in, rs_in, e0_in, e1_in, e2_in
    beside = beside_maker()
    st = Stages(beside, co)
    odd = is_odd[0]

    def fill(i, carry):
        for j in range(16):
            r = i * 16 + j
            gb[0, HALO + r] = t0[r]
            q = jnp.minimum(r, 59)
            before[HALO + 2 + q] = t0[ROWS + q] + co[ST, HALO + 2 + q]
        return carry

    lax.fori_loop(0, ROWS // 16, fill, 0)
    for source, side in ((near, 1 - odd), (far, odd)):
        for j in range(10):
            gb[0, 1 + 74 * side + j] = source[j]
        for j in range(6):
            r = 3 + 74 * side + j
            before[r] = source[10 + j] + co[ST, r]
        for j in range(2):
            er[8 + 68 * side + j] = source[16 + j]
        br[10 + 65 * side] = source[18]
    for n, r in enumerate((HALO, HALO + 63)):
        br[r] = t0[124 + n]
    for n, r in enumerate((1, 2, 61, 62)):
        er[HALO + r] = t0[126 + n]
    for r in (10, 11, 74, 75):
        er[r] = (br[r] - co[D, r] * gb[0, r] + co[C, r] * around(beside, gb, 0, r)) * co[INV, r]
    for r in (9, 10, 11, 12, 73, 74, 75, 76):
        edge = gb[0, r] + er[r] + co[Q, r] * (er[r - 1] + er[r + 1] + beside(er[r]))
        before[r] = edge + co[ST, r]
    sweep(-10, 74, 90, st.fine_defect(tmp, g, lambda t, r: gb[0, r] + co[ST, r], s, (0,)))
    sweep(-9, 73, 90, st.smoothed(u, g, tmp, (0,), Q))
    sweep(-8, 72, 90, st.restricted(rs, tmp, u, lambda t, r: u[0, r] if t else before[r], s, (0,)))
    sweep(-7, 71, 90, st.smoothed(e0, None, tmp, (0,), KQ))
    sweep(-6, 70, 90, st.coarse_defect(tmp, e0, lambda m, r: e0[0, r], rs, (1,)))
    sweep(-5, 69, 90, st.smoothed(e1, e0, tmp, (1,), KQ))
    sweep(-4, 68, 90, st.coarse_defect(tmp, e1, lambda m, r: e1[1, r], rs, (2,)))

    def corrected(r):
        q = co[KQ, r]
        late = e1[2, r] + tmp[2, r] + q * around(beside, tmp, 2, r)
        e2[2, r] = late
        u2[0, r] = u[6, r] + 0.5 * (late + e2[3, r])
        u2[1, r] = u[7, r] + e2[3, r]

    sweep(-3, 67, 90, corrected)

    def defect(r):
        tmp[0, r] = (
            s[7, r] + u2[0, r] - co[D, r] * u2[1, r] + co[C, r] * around(beside, u2, 1, r)
        ) * co[INV, r]

    sweep(-2, 66, 90, defect)

    def final(r):
        sol7[0, r] = u2[1, r] + tmp[0, r] + co[Q, r] * around(beside, tmp, 0, r)

    sweep(-1, 65, 90, final)

    def copy(i, carry):
        for j in range(8):
            send[tile_at(0, i, j), :] = sol7[0, HALO + 8 * i + j]
        return carry

    lax.fori_loop(0, ROWS // 8, copy, 0)


def relay_late(is_odd, t2, near, far):
    odd = is_odd[0]
    for out, side in ((near, 1 - odd), (far, odd)):
        for j in range(6):
            out[j] = t2[58 * side + j]
        for j in range(4):
            out[6 + j] = t2[ROWS + 60 * side + j]


def late(
    is_odd, t2, near, far, s, co, u, rs, e0, e1_in, e2_in, sol7, sol_out, res_out, u2_out, sol2,
    old, e1, u2, tmp, sol, sol_nat, res_nat, sems,
):
    beside = beside_maker()
    st = Stages(beside, co)
    odd = is_odd[0]
    for source, side in ((near, 1 - odd), (far, odd)):
        for j in range(6):
            old[0, 5 + 70 * side + j] = source[j]
        for j in range(4):
            old[1, 7 + 68 * side + j] = source[6 + j]

    def earlier_step(n, r):
        return t2[n * ROWS + r - HALO] if HALO <= r < HALO + ROWS else old[n, r]

    def first_defect(r):
        tmp[0, r] = (
            rs[0, r] + earlier_step(0, r) - co[KD, r] * e0[0, r] + co[K, r] * around(beside, e0, 0, r)
        ) * co[KINV, r]

    sweep(-6, 70, 90, first_defect)

    def first_smooth(r):
        e1[0, r] = e0[0, r] + tmp[0, r] + co[KQ, r] * around(beside, tmp, 0, r)
        e1[1, r] = e1_in[1, r]

    sweep(-5, 69, 90, first_smooth)

    def second_defect(r):
        k, kd, kinv = co[K, r], co[KD, r], co[KINV, r]
        earlier = (earlier_step(1, r), e1[0, r])
        for m in (0, 1):
            tmp[m, r] = (rs[m, r] + earlier[m] - kd * e1[m, r] + k * around(beside, e1, m, r)) * kinv

    sweep(-4, 68, 90, second_defect)

    def corrected(r):
        q = co[KQ, r]
        e20 = e1[0, r] + tmp[0, r] + q * around(beside, tmp, 0, r)
        e21 = e1[1, r] + tmp[1, r] + q * around(beside, tmp, 1, r)
        e22, e23 = e2_in[2, r], e2_in[3, r]
        u2_out[0, r] = u[0, r] + 0.5 * e20
        first = u[1, r] + e20
        u2_out[1, r] = first
        u2[1, r] = first
        u2[2, r] = u[2, r] + 0.5 * (e20 + e21)
        u2[3, r] = u[3, r] + e21
        u2[4, r] = u[4, r] + 0.5 * (e21 + e22)
        u2[5, r] = u[5, r] + e22
        u2[6, r] = u[6, r] + 0.5 * (e22 + e23)

    sweep(-3, 67, 90, corrected)
    sweep(-2, 66, 90, st.fine_defect(tmp, u2, lambda t, r: u2[t - 1, r], s, range(2, 7)))
    final = st.smoothed(sol, u2, tmp, range(2, 7), Q)

    def final_all(r):
        final(r)
        sol[7, r] = sol7[0, r]
        sol2[0, r] = sol[2, r]

    sweep(-1, 0, 90, final_all)
    sweep(64, 65, 90, final_all)

    for i in range(ROWS // 8):
        for j in range(8):
            r = HALO + 8 * i + j
            final_all(r)
            for t in range(2, 8):
                sol_nat[t - 2, tile_at(0, i, j), :] = sol[t, r]
    copies = [pltpu.make_async_copy(sol_nat, sol_out.at[pl.ds(2, 6)], sems.at[0])]
    copies[0].start()
    for part in range(2):
        for i in range(4 * part, 4 * part + 4):
            for j in range(8):
                r = HALO + 8 * i + j
                c, d = co[C, r], co[D, r]
                for t in range(3, 8):
                    res_nat[t - 3, tile_at(0, i, j), :] = (
                        s[t, r] + sol[t - 1, r] - d * sol[t, r] + c * around(beside, sol, t, r)
                    )
        rows = pl.ds(part * ROWS * 4, ROWS * 4)
        copies.append(pltpu.make_async_copy(res_nat.at[:, rows], res_out.at[pl.ds(3, 5), rows], sems.at[1 + part]))
        copies[-1].start()
    for copy in copies:
        copy.wait()


def finish(t3, s, co, before, u2_in, sol2, sol_in, sol_out, res, u2, tmp, sol, sol_nat, sem):
    del sol_in
    beside = beside_maker()

    def corrected(r):
        boundary = t3[r - (HALO - 3)]
        u2[0, r] = before[r] + boundary
        u2[1, r] = u2_in[0, r] + 0.5 * boundary

    sweep(-3, 67, 90, corrected)

    def defect(r):
        c, d, inv = co[C, r], co[D, r], co[INV, r]
        tmp[0, r] = (s[0, r] + u2[0, r] - d * u2[1, r] + c * around(beside, u2, 1, r)) * inv
        tmp[1, r] = (s[1, r] + u2[1, r] - d * u2_in[1, r] + c * around(beside, u2_in, 1, r)) * inv

    sweep(-2, 66, 90, defect)

    def final(r):
        q = co[Q, r]
        sol[0, r] = u2[1, r] + tmp[0, r] + q * around(beside, tmp, 0, r)
        sol[1, r] = u2_in[1, r] + tmp[1, r] + q * around(beside, tmp, 1, r)
        if HALO <= r < HALO + ROWS:
            sol_nat[0, tile_at(0, (r - HALO) // 8, (r - HALO) % 8), :] = sol[0, r]
            sol_nat[1, tile_at(0, (r - HALO) // 8, (r - HALO) % 8), :] = sol[1, r]

    sweep(-1, 65, 90, final)

    copy = pltpu.make_async_copy(sol_nat, sol_out.at[pl.ds(0, 2)], sem)
    copy.start()
    for i in range(ROWS // 8):
        for j in range(8):
            r = HALO + 8 * i + j
            c, d = co[C, r], co[D, r]
            first, second = sol[0, r], sol[1, r]
            spot = tile_at(0, i, j)
            res[0, spot, :] = s[0, r] + co[ST, r] - d * first + c * around(beside, sol, 0, r)
            res[1, spot, :] = s[1, r] + first - d * second + c * around(beside, sol, 1, r)
            res[2, spot, :] = s[2, r] + second - d * sol2[0, r] + c * around(beside, sol2, 0, r)
    copy.wait()


def tail(t4, res, res_in, res_out, total, sems):
    del res_in
    ready = pltpu.make_async_copy(res.at[pl.ds(1, 2)], res_out.at[pl.ds(1, 2)], sems.at[0])
    ready.start()
    total[...] = res[pl.ds(0, 1)] + t4[...][None]
    copy = pltpu.make_async_copy(total, res_out.at[pl.ds(0, 1)], sems.at[1])
    copy.start()
    ready.wait()
    copy.wait()


def call(kernel, ins, outs, scratch=(), aliases=None, specs=None, out_specs=None, limit=24):
    return pl.pallas_call(
        kernel,
        out_shape=outs,
        in_specs=specs or [FULL] * len(ins),
        out_specs=out_specs or [FULL] * len(outs),
        scratch_shapes=list(scratch),
        input_output_aliases=aliases or {},
        compiler_params=pltpu.CompilerParams(vmem_limit_bytes=limit * 2**20),
    )(*ins)


def along(block, axis, route):
    count = lax.axis_size(axis)
    pairs = [(i, route(i)) for i in range(count)]
    return lax.ppermute(block, axis, [(i, j) for i, j in pairs if 0 <= j < count])


def ahead(i):
    return i + 1


def on_chip(i):
    return i ^ 1


def off_chip(i):
    return ((i + 1) ^ 1) - 1


def cycle(source, guess, start_state, conduct):
    is_first = (lax.axis_index("tm") == 0).astype(F32).reshape(1)
    is_odd = (lax.axis_index("space") % 2).astype(jnp.int32).reshape(1)
    guess_v, source_v = view(guess), view(source)
    start_v, conduct_v = view(start_state[None]), view(conduct[None])
    vmem = lambda steps: pltpu.VMEM((steps, EXT, 8, 128), F32)
    dma = pltpu.SemaphoreType.DMA
    one = jax.ShapeDtypeStruct((ROWS * 8, 128), F32)

    by_step = lambda x: pltpu.with_memory_space_constraint(x.reshape(-1, ROWS * 8, 128), pltpu.HBM)
    stepped = lambda steps: jax.ShapeDtypeStruct((steps, ROWS * 8, 128), F32)
    near, far, near_late, far_late, guess_v, source_v, start_v, conduct_v = call(
        edge_pack,
        (is_first, is_odd, by_step(guess_v), by_step(source_v), by_step(start_v), by_step(conduct_v)),
        [rows_of(66), rows_of(66), rows_of(122), rows_of(122), stepped(8), stepped(8), stepped(1), stepped(1)],
        [dma((4, 3))],
        specs=[SMEM, SMEM] + [ANY] * 4,
        limit=1,
    )
    guess_v, source_v, start_v, conduct_v = (x.reshape(-1, 128) for x in (guess_v, source_v, start_v, conduct_v))
    (send0,) = call(
        last_step_pack,
        (guess_v, source_v, conduct_v),
        [rows_of(130)],
        [pltpu.VMEM((2, ROWS, 8, 128), F32), pltpu.VMEM((ROWS, 8, 128), F32)],
        limit=4,
    )
    t0 = along(send0, "tm", ahead)
    far_in = along(far, "space", off_chip)
    near_in = along(near, "space", on_chip)
    far_late_in = along(far_late, "space", off_chip)
    near_late_in = along(near_late, "space", on_chip)
    g, s, co, u, rs, e0, e1 = call(
        interior,
        (is_first, guess_v, source_v, start_v, conduct_v),
        [ext(8), ext(8), ext(9), ext(8), ext(4), ext(4), ext(4)],
        [vmem(8)],
        specs=[SMEM] + [FULL] * 4,
        limit=6,
    )
    g, s, co, u, rs, e0, e1, send2 = call(
        edges,
        (is_odd, near_in, far_in, g, s, co, u, rs, e0, e1),
        [ext(8), ext(8), ext(9), ext(8), ext(4), ext(4), ext(4), rows_of(128)],
        [vmem(8)],
        aliases={n + 3: n for n in range(7)},
        specs=[SMEM] + [FULL] * 9,
        limit=6,
    )
    t2 = along(send2, "tm", ahead)
    near, far = call(relay, (is_odd, t0), [rows_of(19), rows_of(19)], specs=[SMEM, FULL], limit=1)
    far_in = along(far, "space", off_chip)
    near_in = along(near, "space", on_chip)
    g, s, co, u, rs, e0, e1, e2, send3 = call(
        rest,
        (is_odd, near_late_in, far_late_in, g, s, co, u, rs, e0, e1),
        [ext(8), ext(8), ext(9), ext(8), ext(4), ext(4), ext(4), ext(4), rows_of(70)],
        [vmem(8)],
        aliases={n + 3: n for n in range(7)},
        specs=[SMEM] + [FULL] * 9,
        limit=6,
    )
    t3 = along(send3, "tm", ahead)
    u, rs, e0, e1, e2, before, sol7, send4 = call(
        middle,
        (is_odd, t0, near_in, far_in, g, s, co, u, rs, e0, e1, e2),
        [ext(8), ext(4), ext(4), ext(4), ext(4), rows_of(EXT), ext(1), one],
        [vmem(1), pltpu.VMEM((EXT, 8, 128), F32), pltpu.VMEM((EXT, 8, 128), F32), vmem(4), vmem(2)],
        aliases={n + 7: n for n in range(5)},
        specs=[SMEM] + [FULL] * 11,
        limit=6,
    )
    t4 = along(send4, "tm", ahead)
    nat3 = lambda steps: pltpu.VMEM((steps, ROWS * 8, 128), F32)
    near, far = call(relay_late, (is_odd, t2), [rows_of(10), rows_of(10)], specs=[SMEM, FULL], limit=1)
    far_in = along(far, "space", off_chip)
    near_in = along(near, "space", on_chip)
    sol, res, u2, sol2 = call(
        late,
        (is_odd, t2, near_in, far_in, s, co, u, rs, e0, e1, e2, sol7),
        [stepped(8), stepped(8), ext(2), ext(1)],
        [vmem(2), vmem(2), vmem(8), vmem(8), vmem(8), nat3(6), nat3(5), dma((3,))],
        specs=[SMEM] + [FULL] * 11,
        out_specs=[ANY, ANY, FULL, FULL],
        limit=16,
    )
    sol, first_res = call(
        finish,
        (t3, s, co, before, u2, sol2, sol),
        [stepped(8), stepped(3)],
        [vmem(2), vmem(2), vmem(2), nat3(2), dma],
        aliases={6: 0},
        specs=[FULL] * 6 + [ANY],
        out_specs=[ANY, FULL],
        limit=6,
    )
    (res,) = call(
        tail,
        (t4, first_res, res),
        [stepped(8)],
        [nat3(1), dma((2,))],
        aliases={2: 0},
        specs=[FULL, FULL, ANY],
        out_specs=[ANY],
        limit=2,
    )
    return unview(sol, 8), unview(res, 8)


def solution(mesh):
    return jax.shard_map(
        cycle,
        mesh=mesh,
        in_specs=(P("tm", "space", None), P("tm", "space", None), P("space", None), P("space", None)),
        out_specs=(P("tm", "space", None), P("tm", "space", None)),
        check_vma=False,
    )
```

```python
import jax
import jax.numpy as jnp
from jax import lax
from jax.experimental import pallas as pl
from jax.experimental.pallas import tpu as pltpu
from jax.sharding import PartitionSpec as P


F32 = jnp.float32
ROWS = 64
HALO = 11
EXT = ROWS + 2 * HALO
DAMP = 0.8
C, D, INV, Q, K, KD, KINV, KQ, ST = range(9)
FULL = pl.BlockSpec(memory_space=pltpu.VMEM)
SMEM = pl.BlockSpec(memory_space=pltpu.SMEM)
ANY = pl.BlockSpec(memory_space=pltpu.HBM)


def ext(steps):
    return jax.ShapeDtypeStruct((steps, EXT, 8, 128), F32)


def rows_of(count):
    return jax.ShapeDtypeStruct((count, 8, 128), F32)


def view(x):
    steps = x.shape[0]
    return x.reshape(steps, ROWS // 8, 8, 8, 128).transpose(0, 1, 3, 2, 4).reshape(steps * ROWS * 8, 128)


def unview(y, steps):
    return y.reshape(steps, ROWS // 8, 8, 8, 128).transpose(0, 1, 3, 2, 4).reshape(steps, ROWS, 1024)


def tile_at(step, tile, row):
    return pl.ds(step * ROWS * 8 + tile * 64 + row, 8, 8)


def beside_maker():
    lane = lax.broadcasted_iota(jnp.int32, (8, 128), 1)
    sub = lax.broadcasted_iota(jnp.int32, (8, 128), 0)
    first, last = lane == 0, lane == 127
    top, bottom = sub == 0, sub == 7

    def beside(x):
        before = jnp.where(top, 0.0, pltpu.roll(x, 1, 0))
        after = jnp.where(bottom, 0.0, pltpu.roll(x, 7, 0))
        return pltpu.roll(jnp.where(last, before, x), 1, 1) + pltpu.roll(jnp.where(first, after, x), 127, 1)

    return beside


def around(beside, ref, step, r):
    return ref[step, r - 1] + ref[step, r + 1] + beside(ref[step, r])


def sweep(low, high, unroll, body):
    low, high = low + HALO, high + HALO
    count = high - low
    unroll = min(unroll, count)
    blocks = -(-count // unroll)
    if blocks == 1:
        for j in range(unroll):
            body(low + j)
        return

    def step(i, carry):
        start = jnp.minimum(low + i * unroll, high - unroll)
        for j in range(unroll):
            body(start + j)
        return carry

    lax.fori_loop(0, blocks, step, 0)


def coefficients(co, r, c):
    diag = 1.0 + 4.0 * c
    coarse = 1.0 + 8.0 * c
    recip = 1.0 / diag
    coarse_recip = 1.0 / coarse
    co[C, r] = c
    co[D, r] = diag
    co[INV, r] = DAMP * recip
    co[Q, r] = c * recip
    co[K, r] = 2.0 * c
    co[KD, r] = coarse
    co[KINV, r] = DAMP * coarse_recip
    co[KQ, r] = 2.0 * c * coarse_recip


class Stages:
    def __init__(self, beside, co):
        self.beside, self.co = beside, co

    def fine_defect(self, out, field, earlier, source, steps):
        def body(r):
            c, d, inv = self.co[C, r], self.co[D, r], self.co[INV, r]
            for t in steps:
                out[t, r] = (source[t, r] + earlier(t, r) - d * field[t, r] + c * around(self.beside, field, t, r)) * inv

        return body

    def coarse_defect(self, out, field, earlier, rhs, steps):
        def body(r):
            k, kd, kinv = self.co[K, r], self.co[KD, r], self.co[KINV, r]
            for m in steps:
                out[m, r] = (rhs[m, r] + earlier(m, r) - kd * field[m, r] + k * around(self.beside, field, m, r)) * kinv

        return body

    def smoothed(self, out, field, defect, steps, plane):
        def body(r):
            q = self.co[plane, r]
            for t in steps:
                base = defect[t, r] if field is None else field[t, r] + defect[t, r]
                out[t, r] = base + q * around(self.beside, defect, t, r)

        return body

    def restricted(self, out, scaled, field, earlier, source, pairs):
        def body(r):
            c, d, kinv = self.co[C, r], self.co[D, r], self.co[KINV, r]
            for m in pairs:
                parts = [
                    source[t, r] + earlier(t, r) - d * field[t, r] + c * around(self.beside, field, t, r)
                    for t in (2 * m, 2 * m + 1)
                ]
                both = parts[0] + parts[1]
                out[m, r] = both
                scaled[m, r] = both * kinv

        return body


def edge_pack(
    is_first, is_odd, guess, source, start, conduct, near, far, near_late, far_late, gb, sb, tb, cb, sems
):
    pairs = ((guess, gb), (source, sb), (start, tb), (conduct, cb))

    def copies(spans):
        return [
            pltpu.make_async_copy(src.at[:, pl.ds(low, size)], dst.at[:, pl.ds(low, size)], sems.at[n, k])
            for k, low, size in spans
            for n, (src, dst) in enumerate(pairs)
        ]

    outer_tiles, inner_tiles = copies(((0, 0, 128), (1, 384, 128))), copies(((2, 128, 256),))
    for copy in outer_tiles + inner_tiles:
        copy.start()
    for copy in outer_tiles:
        copy.wait()
    odd = is_odd[0]

    def grab(out, base, ref, t, low, count, scale=None):
        def body(j, carry):
            r = low + j
            value = ref[t, pl.ds((r // 8) * 64 + r % 8, 8, 8), :]
            out[base + j] = value if scale is None else value * scale
            return carry

        lax.fori_loop(0, count, body, 0, unroll=True)

    for out, late_out, side in ((near, near_late, 1 - odd), (far, far_late, odd)):
        for t in range(2, 8):
            grab(out, (t - 2) * 10, gb, t, 54 * side, 10)
        for t in range(3, 8):
            grab(out, 60 + (t - 3) * 9, sb, t, 55 * side, 9)
        grab(out, 105, cb, 0, 55 * side, 9)
        for t in range(2):
            grab(late_out, t * 11, gb, t, 53 * side, 11)
        for t in range(2, 8):
            grab(late_out, 20 + t, gb, t, 10 + 43 * side, 1)
        for t in range(3):
            grab(late_out, 28 + t * 10, sb, t, 54 * side, 10)
        for t in range(3, 8):
            grab(late_out, 55 + t, sb, t, 9 + 45 * side, 1)
        grab(late_out, 63, cb, 0, 9 + 45 * side, 1)
        grab(late_out, 64, tb, 0, 54 * side, 10, is_first[0])
    for copy in inner_tiles:
        copy.wait()


def last_step_pack(guess, source, out):
    for i in range(ROWS // 8):
        for j in range(8):
            r = 8 * i + j
            out[r] = guess[tile_at(7, i, j), :]
            out[ROWS + r] = source[tile_at(7, i, j), :] + guess[tile_at(6, i, j), :]


def interior(is_first, guess, source, start, conduct, g, s, co, u, rs, e0, e1, tmp):
    beside = beside_maker()

    def fill(i, carry):
        for j in range(8):
            r = HALO + 8 * i + j
            for t in range(8):
                g[t, r] = guess[tile_at(t, i, j), :]
                s[t, r] = source[tile_at(t, i, j), :]
            coefficients(co, r, conduct[tile_at(0, i, j), :])
            co[ST, r] = start[tile_at(0, i, j), :] * is_first[0]
        return carry

    lax.fori_loop(0, ROWS // 8, fill, 0)
    st = Stages(beside, co)
    sweep(1, 63, 90, st.fine_defect(tmp, g, lambda t, r: g[t - 1, r], s, range(3, 8)))
    sweep(2, 62, 90, st.smoothed(u, g, tmp, range(3, 8), Q))
    sweep(3, 61, 90, st.restricted(rs, tmp, u, lambda t, r: u[t - 1, r], s, (2, 3)))
    sweep(4, 60, 90, st.smoothed(e0, None, tmp, (2, 3), KQ))
    sweep(5, 59, 90, st.coarse_defect(tmp, e0, lambda m, r: e0[m - 1, r], rs, (3,)))
    sweep(6, 58, 90, st.smoothed(e1, e0, tmp, (3,), KQ))


def both(inner, depth, body):
    sweep(-depth, inner, 99, body)
    sweep(ROWS - inner, ROWS + depth, 99, body)


def scaled(co, rs, tmp):
    def body(r):
        for m in (2, 3):
            tmp[m, r] = rs[m, r] * co[KINV, r]

    return body


def edges(is_odd, near, far, g_in, s_in, co_in, u_in, rs_in, e0_in, e1_in, g, s, co, u, rs, e0, e1, out, tmp):
    del g_in, s_in, co_in, u_in, rs_in, e0_in, e1_in
    beside = beside_maker()
    odd = is_odd[0]
    for source, side in ((near, 1 - odd), (far, odd)):
        for j in range(10):
            for t in range(2, 8):
                g[t, 1 + 74 * side + j] = source[(t - 2) * 10 + j]
        for j in range(9):
            for t in range(3, 8):
                s[t, 2 + 73 * side + j] = source[60 + (t - 3) * 9 + j]
            coefficients(co, 2 + 73 * side + j, source[105 + j])
    st = Stages(beside, co)
    both(3, 9, st.fine_defect(tmp, g, lambda t, r: g[t - 1, r], s, range(3, 8)))
    both(2, 8, st.smoothed(u, g, tmp, range(3, 8), Q))
    both(3, 7, st.restricted(rs, tmp, u, lambda t, r: u[t - 1, r], s, (2, 3)))
    both(5, -3, scaled(co, rs, tmp))
    both(4, 6, st.smoothed(e0, None, tmp, (2, 3), KQ))
    both(7, 5, st.coarse_defect(tmp, e0, lambda m, r: e0[m - 1, r], rs, (3,)))
    both(6, 4, st.smoothed(e1, e0, tmp, (3,), KQ))
    for r in range(76):
        out[r] = e0[3, HALO - 6 + r]
    for r in range(72):
        out[76 + r] = e1[3, HALO - 4 + r]


def rest(
    is_odd, near, far, g_in, s_in, co_in, u_in, rs_in, e0_in, e1_in, g, s, co, u, rs, e0, e1, e2, send, tmp
):
    del g_in, s_in, co_in, u_in, rs_in, e0_in, e1_in
    beside = beside_maker()
    st = Stages(beside, co)
    odd = is_odd[0]
    for source, side in ((near, 1 - odd), (far, odd)):
        for j in range(11):
            for t in range(2):
                g[t, 75 * side + j] = source[t * 11 + j]
        for t in range(2, 8):
            g[t, 85 * side] = source[20 + t]
        for t in range(3, 8):
            s[t, 1 + 83 * side] = source[55 + t]
        coefficients(co, 1 + 83 * side, source[63])
        for j in range(10):
            for t in range(3):
                s[t, 1 + 74 * side + j] = source[28 + t * 10 + j]
            co[ST, 1 + 74 * side + j] = source[64 + j]
    both(-7, 10, st.fine_defect(tmp, g, lambda t, r: g[t - 1, r], s, range(3, 8)))
    both(-8, 9, st.smoothed(u, g, tmp, range(3, 8), Q))
    both(-7, 8, st.restricted(rs, tmp, u, lambda t, r: u[t - 1, r], s, (2, 3)))
    both(-5, 7, scaled(co, rs, tmp))
    both(-6, 7, st.smoothed(e0, None, tmp, (2, 3), KQ))
    both(-3, 6, st.coarse_defect(tmp, e0, lambda m, r: e0[m - 1, r], rs, (3,)))
    both(-4, 5, st.smoothed(e1, e0, tmp, (3,), KQ))
    sweep(-10, 74, 90, st.fine_defect(tmp, g, lambda t, r: g[t - 1, r], s, (1, 2)))
    sweep(-9, 73, 90, st.smoothed(u, g, tmp, (1, 2), Q))
    sweep(-8, 72, 90, st.restricted(rs, tmp, u, lambda t, r: u[t - 1, r], s, (1,)))
    sweep(-7, 71, 90, st.smoothed(e0, None, tmp, (1,), KQ))
    sweep(-6, 70, 90, st.coarse_defect(tmp, e0, lambda m, r: e0[m - 1, r], rs, (2,)))
    sweep(-5, 69, 90, st.smoothed(e1, e0, tmp, (2,), KQ))
    sweep(-4, 68, 90, st.coarse_defect(tmp, e1, lambda m, r: e1[m - 1, r], rs, (3,)))
    smooth = st.smoothed(e2, e1, tmp, (3,), KQ)

    def final(r):
        smooth(r)
        send[r - (HALO - 3)] = e2[3, r]

    sweep(-3, 67, 90, final)


def relay(is_odd, t0, near, far):
    odd = is_odd[0]
    for out, side in ((near, 1 - odd), (far, odd)):
        for j in range(10):
            out[j] = t0[54 * side + j]
        for j in range(9):
            out[10 + j] = t0[ROWS + 55 * side + j]


def middle(
    is_odd, t0, near, far, g, s, co, u_in, rs_in, e0_in, e1_in, e2_in,
    u, rs, e0, e1, e2, before, sol7, send, gb, er, br, tmp, u2,
):
    del u_in, rs_in, e0_in, e1_in, e2_in
    beside = beside_maker()
    st = Stages(beside, co)
    odd = is_odd[0]

    for r in range(ROWS):
        gb[0, HALO + r] = t0[r]
        br[0, HALO + r] = t0[ROWS + r]
    for source, side in ((near, 1 - odd), (far, odd)):
        for j in range(10):
            gb[0, 1 + 74 * side + j] = source[j]
        for j in range(9):
            br[0, 2 + 73 * side + j] = source[10 + j]

    def earlier_defect(r):
        er[0, r] = (br[0, r] - co[D, r] * gb[0, r] + co[C, r] * around(beside, gb, 0, r)) * co[INV, r]

    def earlier_smooth(r):
        value = gb[0, r] + er[0, r] + co[Q, r] * around(beside, er, 0, r)
        before[r] = value + co[ST, r]

    sweep(-9, 73, 90, earlier_defect)
    sweep(-8, 72, 90, earlier_smooth)
    sweep(-10, 74, 90, st.fine_defect(tmp, g, lambda t, r: gb[0, r] + co[ST, r], s, (0,)))
    sweep(-9, 73, 90, st.smoothed(u, g, tmp, (0,), Q))
    sweep(-8, 72, 90, st.restricted(rs, tmp, u, lambda t, r: u[0, r] if t else before[r], s, (0,)))
    sweep(-7, 71, 90, st.smoothed(e0, None, tmp, (0,), KQ))
    sweep(-6, 70, 90, st.coarse_defect(tmp, e0, lambda m, r: e0[0, r], rs, (1,)))
    sweep(-5, 69, 90, st.smoothed(e1, e0, tmp, (1,), KQ))
    sweep(-4, 68, 90, st.coarse_defect(tmp, e1, lambda m, r: e1[1, r], rs, (2,)))

    def corrected(r):
        q = co[KQ, r]
        late = e1[2, r] + tmp[2, r] + q * around(beside, tmp, 2, r)
        e2[2, r] = late
        u2[0, r] = u[6, r] + 0.5 * (late + e2[3, r])
        u2[1, r] = u[7, r] + e2[3, r]

    sweep(-3, 67, 90, corrected)

    def defect(r):
        tmp[0, r] = (
            s[7, r] + u2[0, r] - co[D, r] * u2[1, r] + co[C, r] * around(beside, u2, 1, r)
        ) * co[INV, r]

    sweep(-2, 66, 90, defect)

    def final(r):
        sol7[0, r] = u2[1, r] + tmp[0, r] + co[Q, r] * around(beside, tmp, 0, r)

    sweep(-1, 65, 90, final)

    def copy(i, carry):
        for j in range(8):
            send[tile_at(0, i, j), :] = sol7[0, HALO + 8 * i + j]
        return carry

    lax.fori_loop(0, ROWS // 8, copy, 0)


def late(
    t2, s, co, u, rs, e0, e1_in, e2_in, sol7, sol_out, res_out, u2_out, sol2, e1, u2, tmp, sol, sol_nat, res_nat, sems
):
    beside = beside_maker()
    st = Stages(beside, co)

    def first_defect(r):
        tmp[0, r] = (
            rs[0, r] + t2[r - (HALO - 6)] - co[KD, r] * e0[0, r] + co[K, r] * around(beside, e0, 0, r)
        ) * co[KINV, r]

    sweep(-6, 70, 90, first_defect)

    def first_smooth(r):
        e1[0, r] = e0[0, r] + tmp[0, r] + co[KQ, r] * around(beside, tmp, 0, r)
        e1[1, r] = e1_in[1, r]

    sweep(-5, 69, 90, first_smooth)

    def second_defect(r):
        k, kd, kinv = co[K, r], co[KD, r], co[KINV, r]
        earlier = (t2[76 + r - (HALO - 4)], e1[0, r])
        for m in (0, 1):
            tmp[m, r] = (rs[m, r] + earlier[m] - kd * e1[m, r] + k * around(beside, e1, m, r)) * kinv

    sweep(-4, 68, 90, second_defect)

    def corrected(r):
        q = co[KQ, r]
        e20 = e1[0, r] + tmp[0, r] + q * around(beside, tmp, 0, r)
        e21 = e1[1, r] + tmp[1, r] + q * around(beside, tmp, 1, r)
        e22, e23 = e2_in[2, r], e2_in[3, r]
        u2_out[0, r] = u[0, r] + 0.5 * e20
        first = u[1, r] + e20
        u2_out[1, r] = first
        u2[1, r] = first
        u2[2, r] = u[2, r] + 0.5 * (e20 + e21)
        u2[3, r] = u[3, r] + e21
        u2[4, r] = u[4, r] + 0.5 * (e21 + e22)
        u2[5, r] = u[5, r] + e22
        u2[6, r] = u[6, r] + 0.5 * (e22 + e23)

    sweep(-3, 67, 90, corrected)
    sweep(-2, 66, 90, st.fine_defect(tmp, u2, lambda t, r: u2[t - 1, r], s, range(2, 7)))
    final = st.smoothed(sol, u2, tmp, range(2, 7), Q)

    def final_all(r):
        final(r)
        sol[7, r] = sol7[0, r]
        sol2[0, r] = sol[2, r]

    sweep(-1, 0, 90, final_all)
    sweep(64, 65, 90, final_all)

    for i in range(ROWS // 8):
        for j in range(8):
            r = HALO + 8 * i + j
            final_all(r)
            for t in range(2, 8):
                sol_nat[t - 2, tile_at(0, i, j), :] = sol[t, r]
    copies = [pltpu.make_async_copy(sol_nat, sol_out.at[pl.ds(2, 6)], sems.at[0])]
    copies[0].start()
    for part in range(2):
        for i in range(4 * part, 4 * part + 4):
            for j in range(8):
                r = HALO + 8 * i + j
                c, d = co[C, r], co[D, r]
                for t in range(3, 8):
                    res_nat[t - 3, tile_at(0, i, j), :] = (
                        s[t, r] + sol[t - 1, r] - d * sol[t, r] + c * around(beside, sol, t, r)
                    )
        rows = pl.ds(part * ROWS * 4, ROWS * 4)
        copies.append(pltpu.make_async_copy(res_nat.at[:, rows], res_out.at[pl.ds(3, 5), rows], sems.at[1 + part]))
        copies[-1].start()
    for copy in copies:
        copy.wait()


def finish(t3, s, co, before, u2_in, sol2, sol_in, res_in, sol_out, res_out, base, u2, tmp, sol, sol_nat, res, sems):
    del sol_in, res_in
    beside = beside_maker()

    def corrected(r):
        boundary = t3[r - (HALO - 3)]
        u2[0, r] = before[r] + boundary
        u2[1, r] = u2_in[0, r] + 0.5 * boundary

    sweep(-3, 67, 90, corrected)

    def defect(r):
        c, d, inv = co[C, r], co[D, r], co[INV, r]
        tmp[0, r] = (s[0, r] + u2[0, r] - d * u2[1, r] + c * around(beside, u2, 1, r)) * inv
        tmp[1, r] = (s[1, r] + u2[1, r] - d * u2_in[1, r] + c * around(beside, u2_in, 1, r)) * inv

    sweep(-2, 66, 90, defect)

    def final(r):
        q = co[Q, r]
        sol[0, r] = u2[1, r] + tmp[0, r] + q * around(beside, tmp, 0, r)
        sol[1, r] = u2_in[1, r] + tmp[1, r] + q * around(beside, tmp, 1, r)
        if HALO <= r < HALO + ROWS:
            sol_nat[0, tile_at(0, (r - HALO) // 8, (r - HALO) % 8), :] = sol[0, r]
            sol_nat[1, tile_at(0, (r - HALO) // 8, (r - HALO) % 8), :] = sol[1, r]

    sweep(-1, 65, 90, final)

    copies = [pltpu.make_async_copy(sol_nat, sol_out.at[pl.ds(0, 2)], sems.at[0])]
    copies[0].start()
    for i in range(ROWS // 8):
        for j in range(8):
            r = HALO + 8 * i + j
            c, d = co[C, r], co[D, r]
            first, second = sol[0, r], sol[1, r]
            spot = tile_at(0, i, j)
            base[spot, :] = s[0, r] + co[ST, r] - d * first + c * around(beside, sol, 0, r)
            res[0, spot, :] = s[1, r] + first - d * second + c * around(beside, sol, 1, r)
            res[1, spot, :] = s[2, r] + second - d * sol2[0, r] + c * around(beside, sol2, 0, r)
    copies.append(pltpu.make_async_copy(res, res_out.at[pl.ds(1, 2)], sems.at[1]))
    copies[1].start()
    for copy in copies:
        copy.wait()


def tail(t4, base, res_in, res_out, total, sem):
    del res_in
    total[0] = base[...] + t4[...]
    copy = pltpu.make_async_copy(total, res_out.at[pl.ds(0, 1)], sem)
    copy.start()
    copy.wait()


def call(kernel, ins, outs, scratch=(), aliases=None, specs=None, out_specs=None, limit=24):
    return pl.pallas_call(
        kernel,
        out_shape=outs,
        in_specs=specs or [FULL] * len(ins),
        out_specs=out_specs or [FULL] * len(outs),
        scratch_shapes=list(scratch),
        input_output_aliases=aliases or {},
        compiler_params=pltpu.CompilerParams(vmem_limit_bytes=limit * 2**20),
    )(*ins)


def along(block, axis, route):
    count = lax.axis_size(axis)
    pairs = [(i, route(i)) for i in range(count)]
    return lax.ppermute(block, axis, [(i, j) for i, j in pairs if 0 <= j < count])


def ahead(i):
    return i + 1


def on_chip(i):
    return i ^ 1


def off_chip(i):
    return ((i + 1) ^ 1) - 1


def cycle(source, guess, start_state, conduct):
    is_first = (lax.axis_index("tm") == 0).astype(F32).reshape(1)
    is_odd = (lax.axis_index("space") % 2).astype(jnp.int32).reshape(1)
    guess_v, source_v = view(guess), view(source)
    start_v, conduct_v = view(start_state[None]), view(conduct[None])
    vmem = lambda steps: pltpu.VMEM((steps, EXT, 8, 128), F32)
    dma = pltpu.SemaphoreType.DMA
    one = jax.ShapeDtypeStruct((ROWS * 8, 128), F32)

    by_step = lambda x: pltpu.with_memory_space_constraint(x.reshape(-1, ROWS * 8, 128), pltpu.HBM)
    stepped = lambda steps: jax.ShapeDtypeStruct((steps, ROWS * 8, 128), F32)
    near, far, near_late, far_late, guess_v, source_v, start_v, conduct_v = call(
        edge_pack,
        (is_first, is_odd, by_step(guess_v), by_step(source_v), by_step(start_v), by_step(conduct_v)),
        [rows_of(114), rows_of(114), rows_of(74), rows_of(74), stepped(8), stepped(8), stepped(1), stepped(1)],
        [dma((4, 3))],
        specs=[SMEM, SMEM] + [ANY] * 4,
        limit=1,
    )
    guess_v, source_v, start_v, conduct_v = (x.reshape(-1, 128) for x in (guess_v, source_v, start_v, conduct_v))
    far_in = along(far, "space", off_chip)
    (send0,) = call(last_step_pack, (guess_v, source_v), [rows_of(128)], limit=1)
    t0 = along(send0, "tm", ahead)
    near_in = along(near, "space", on_chip)
    far_late_in = along(far_late, "space", off_chip)
    near_late_in = along(near_late, "space", on_chip)
    g, s, co, u, rs, e0, e1 = call(
        interior,
        (is_first, guess_v, source_v, start_v, conduct_v),
        [ext(8), ext(8), ext(9), ext(8), ext(4), ext(4), ext(4)],
        [vmem(8)],
        specs=[SMEM] + [FULL] * 4,
        limit=6,
    )
    g, s, co, u, rs, e0, e1, send2 = call(
        edges,
        (is_odd, near_in, far_in, g, s, co, u, rs, e0, e1),
        [ext(8), ext(8), ext(9), ext(8), ext(4), ext(4), ext(4), rows_of(148)],
        [vmem(8)],
        aliases={n + 3: n for n in range(7)},
        specs=[SMEM] + [FULL] * 9,
        limit=6,
    )
    t2 = along(send2, "tm", ahead)
    near, far = call(relay, (is_odd, t0), [rows_of(19), rows_of(19)], specs=[SMEM, FULL], limit=1)
    far_in = along(far, "space", off_chip)
    near_in = along(near, "space", on_chip)
    g, s, co, u, rs, e0, e1, e2, send3 = call(
        rest,
        (is_odd, near_late_in, far_late_in, g, s, co, u, rs, e0, e1),
        [ext(8), ext(8), ext(9), ext(8), ext(4), ext(4), ext(4), ext(4), rows_of(70)],
        [vmem(8)],
        aliases={n + 3: n for n in range(7)},
        specs=[SMEM] + [FULL] * 9,
        limit=6,
    )
    t3 = along(send3, "tm", ahead)
    u, rs, e0, e1, e2, before, sol7, send4 = call(
        middle,
        (is_odd, t0, near_in, far_in, g, s, co, u, rs, e0, e1, e2),
        [ext(8), ext(4), ext(4), ext(4), ext(4), rows_of(EXT), ext(1), one],
        [vmem(1), vmem(1), vmem(1), vmem(4), vmem(2)],
        aliases={n + 7: n for n in range(5)},
        specs=[SMEM] + [FULL] * 11,
        limit=6,
    )
    t4 = along(send4, "tm", ahead)
    nat3 = lambda steps: pltpu.VMEM((steps, ROWS * 8, 128), F32)
    sol, res, u2, sol2 = call(
        late,
        (t2, s, co, u, rs, e0, e1, e2, sol7),
        [stepped(8), stepped(8), ext(2), ext(1)],
        [vmem(2), vmem(8), vmem(8), vmem(8), nat3(6), nat3(5), dma((3,))],
        out_specs=[ANY, ANY, FULL, FULL],
        limit=16,
    )
    sol, res, base = call(
        finish,
        (t3, s, co, before, u2, sol2, sol, res),
        [stepped(8), stepped(8), jax.ShapeDtypeStruct((ROWS * 8, 128), F32)],
        [vmem(2), vmem(2), vmem(2), nat3(2), nat3(2), dma((2,))],
        aliases={6: 0, 7: 1},
        specs=[FULL] * 6 + [ANY] * 2,
        out_specs=[ANY, ANY, FULL],
        limit=6,
    )
    (res,) = call(
        tail,
        (t4, base, res),
        [stepped(8)],
        [nat3(1), dma],
        aliases={2: 0},
        specs=[FULL, FULL, ANY],
        out_specs=[ANY],
        limit=2,
    )
    return unview(sol, 8), unview(res, 8)


def solution(mesh):
    return jax.shard_map(
        cycle,
        mesh=mesh,
        in_specs=(P("tm", "space", None), P("tm", "space", None), P("space", None), P("space", None)),
        out_specs=(P("tm", "space", None), P("tm", "space", None)),
        check_vma=False,
    )
```

```python
import jax
import jax.numpy as jnp
from jax import lax
from jax.experimental import pallas as pl
from jax.experimental.pallas import tpu as pltpu
from jax.sharding import PartitionSpec as P


F32 = jnp.float32
ROWS = 64
HALO = 11
EXT = ROWS + 2 * HALO
DAMP = 0.8
C, D, INV, Q, K, KD, KINV, KQ, ST = range(9)
FULL = pl.BlockSpec(memory_space=pltpu.VMEM)
SMEM = pl.BlockSpec(memory_space=pltpu.SMEM)
ANY = pl.BlockSpec(memory_space=pltpu.HBM)


def ext(steps):
    return jax.ShapeDtypeStruct((steps, EXT, 8, 128), F32)


def rows_of(count):
    return jax.ShapeDtypeStruct((count, 8, 128), F32)


def view(x):
    steps = x.shape[0]
    return x.reshape(steps, ROWS // 8, 8, 8, 128).transpose(0, 1, 3, 2, 4).reshape(steps * ROWS * 8, 128)


def unview(y, steps):
    return y.reshape(steps, ROWS // 8, 8, 8, 128).transpose(0, 1, 3, 2, 4).reshape(steps, ROWS, 1024)


def tile_at(step, tile, row):
    return pl.ds(step * ROWS * 8 + tile * 64 + row, 8, 8)


def beside_maker():
    lane = lax.broadcasted_iota(jnp.int32, (8, 128), 1)
    sub = lax.broadcasted_iota(jnp.int32, (8, 128), 0)
    first, last = lane == 0, lane == 127
    top, bottom = sub == 0, sub == 7

    def beside(x):
        before = jnp.where(top, 0.0, pltpu.roll(x, 1, 0))
        after = jnp.where(bottom, 0.0, pltpu.roll(x, 7, 0))
        return pltpu.roll(jnp.where(last, before, x), 1, 1) + pltpu.roll(jnp.where(first, after, x), 127, 1)

    return beside


def around(beside, ref, step, r):
    return ref[step, r - 1] + ref[step, r + 1] + beside(ref[step, r])


def sweep(low, high, unroll, body):
    low, high = low + HALO, high + HALO
    count = high - low
    unroll = min(unroll, count)
    blocks = -(-count // unroll)
    if blocks == 1:
        for j in range(unroll):
            body(low + j)
        return

    def step(i, carry):
        start = jnp.minimum(low + i * unroll, high - unroll)
        for j in range(unroll):
            body(start + j)
        return carry

    lax.fori_loop(0, blocks, step, 0)


def coefficients(co, r, c):
    diag = 1.0 + 4.0 * c
    coarse = 1.0 + 8.0 * c
    recip = 1.0 / diag
    coarse_recip = 1.0 / coarse
    co[C, r] = c
    co[D, r] = diag
    co[INV, r] = DAMP * recip
    co[Q, r] = c * recip
    co[K, r] = 2.0 * c
    co[KD, r] = coarse
    co[KINV, r] = DAMP * coarse_recip
    co[KQ, r] = 2.0 * c * coarse_recip


class Stages:
    def __init__(self, beside, co):
        self.beside, self.co = beside, co

    def fine_defect(self, out, field, earlier, source, steps):
        def body(r):
            c, d, inv = self.co[C, r], self.co[D, r], self.co[INV, r]
            for t in steps:
                out[t, r] = (source[t, r] + earlier(t, r) - d * field[t, r] + c * around(self.beside, field, t, r)) * inv

        return body

    def coarse_defect(self, out, field, earlier, rhs, steps):
        def body(r):
            k, kd, kinv = self.co[K, r], self.co[KD, r], self.co[KINV, r]
            for m in steps:
                out[m, r] = (rhs[m, r] + earlier(m, r) - kd * field[m, r] + k * around(self.beside, field, m, r)) * kinv

        return body

    def smoothed(self, out, field, defect, steps, plane):
        def body(r):
            q = self.co[plane, r]
            for t in steps:
                base = defect[t, r] if field is None else field[t, r] + defect[t, r]
                out[t, r] = base + q * around(self.beside, defect, t, r)

        return body

    def restricted(self, out, scaled, field, earlier, source, pairs):
        def body(r):
            c, d, kinv = self.co[C, r], self.co[D, r], self.co[KINV, r]
            for m in pairs:
                parts = [
                    source[t, r] + earlier(t, r) - d * field[t, r] + c * around(self.beside, field, t, r)
                    for t in (2 * m, 2 * m + 1)
                ]
                both = parts[0] + parts[1]
                out[m, r] = both
                scaled[m, r] = both * kinv

        return body


def edge_pack(
    is_first, is_odd, guess, source, start, conduct, near, far, gb, sb, tb, cb, sems
):
    pairs = ((guess, gb), (source, sb), (start, tb), (conduct, cb))

    def copies(spans):
        return [
            pltpu.make_async_copy(src.at[:, pl.ds(low, size)], dst.at[:, pl.ds(low, size)], sems.at[n, k])
            for k, low, size in spans
            for n, (src, dst) in enumerate(pairs)
        ]

    outer_tiles, inner_tiles = copies(((0, 0, 128), (1, 384, 128))), copies(((2, 128, 256),))
    for copy in outer_tiles + inner_tiles:
        copy.start()
    for copy in outer_tiles:
        copy.wait()
    odd = is_odd[0]

    def grab(out, base, ref, t, low, count, scale=None):
        def body(j, carry):
            r = low + j
            value = ref[t, pl.ds((r // 8) * 64 + r % 8, 8, 8), :]
            out[base + j] = value if scale is None else value * scale
            return carry

        lax.fori_loop(0, count, body, 0, unroll=True)

    for out, side in ((near, 1 - odd), (far, odd)):
        for t in range(8):
            grab(out, t * 11, gb, t, 53 * side, 11)
            grab(out, 88 + t * 10, sb, t, 54 * side, 10)
        grab(out, 168, cb, 0, 54 * side, 10)
        grab(out, 178, tb, 0, 54 * side, 10, is_first[0])
    for copy in inner_tiles:
        copy.wait()


def last_step_pack(guess, source, out):
    for i in range(ROWS // 8):
        for j in range(8):
            r = 8 * i + j
            out[r] = guess[tile_at(7, i, j), :]
            out[ROWS + r] = source[tile_at(7, i, j), :] + guess[tile_at(6, i, j), :]


def interior(is_first, guess, source, start, conduct, g, s, co, u, rs, e0, e1, send, tmp):
    beside = beside_maker()

    def fill(i, carry):
        for j in range(8):
            r = HALO + 8 * i + j
            for t in range(8):
                g[t, r] = guess[tile_at(t, i, j), :]
                s[t, r] = source[tile_at(t, i, j), :]
            coefficients(co, r, conduct[tile_at(0, i, j), :])
            co[ST, r] = start[tile_at(0, i, j), :] * is_first[0]
        return carry

    lax.fori_loop(0, ROWS // 8, fill, 0)
    st = Stages(beside, co)
    sweep(1, 63, 90, st.fine_defect(tmp, g, lambda t, r: g[t - 1, r], s, range(3, 8)))
    sweep(2, 62, 90, st.smoothed(u, g, tmp, range(3, 8), Q))
    sweep(3, 61, 90, st.restricted(rs, tmp, u, lambda t, r: u[t - 1, r], s, (2, 3)))
    sweep(4, 60, 90, st.smoothed(e0, None, tmp, (2, 3), KQ))
    sweep(5, 59, 90, st.coarse_defect(tmp, e0, lambda m, r: e0[m - 1, r], rs, (3,)))
    sweep(6, 58, 90, st.smoothed(e1, e0, tmp, (3,), KQ))
    for r in range(4, 60):
        send[r - 4] = e0[3, HALO + r]
    for r in range(6, 58):
        send[50 + r] = e1[3, HALO + r]


def both(inner, depth, body):
    sweep(-depth, inner, 99, body)
    sweep(ROWS - inner, ROWS + depth, 99, body)


def scaled(co, rs, tmp):
    def body(r):
        for m in (2, 3):
            tmp[m, r] = rs[m, r] * co[KINV, r]

    return body


def edges(is_odd, near, far, g_in, s_in, co_in, u_in, rs_in, e0_in, e1_in, g, s, co, u, rs, e0, e1, out, tmp):
    del g_in, s_in, co_in, u_in, rs_in, e0_in, e1_in
    beside = beside_maker()
    odd = is_odd[0]
    for source, side in ((near, 1 - odd), (far, odd)):
        for j in range(11):
            for t in range(8):
                g[t, 75 * side + j] = source[t * 11 + j]
        for j in range(10):
            for t in range(8):
                s[t, 1 + 74 * side + j] = source[88 + t * 10 + j]
            coefficients(co, 1 + 74 * side + j, source[168 + j])
            co[ST, 1 + 74 * side + j] = source[178 + j]
    st = Stages(beside, co)
    both(3, 10, st.fine_defect(tmp, g, lambda t, r: g[t - 1, r], s, range(3, 8)))
    both(2, 9, st.smoothed(u, g, tmp, range(3, 8), Q))
    both(3, 8, st.restricted(rs, tmp, u, lambda t, r: u[t - 1, r], s, (2, 3)))
    both(5, -3, scaled(co, rs, tmp))
    both(4, 7, st.smoothed(e0, None, tmp, (2, 3), KQ))
    both(7, 6, st.coarse_defect(tmp, e0, lambda m, r: e0[m - 1, r], rs, (3,)))
    both(6, 5, st.smoothed(e1, e0, tmp, (3,), KQ))
    for j in range(10):
        out[j] = e0[3, HALO - 6 + j]
        out[10 + j] = e0[3, HALO + 60 + j]
        out[20 + j] = e1[3, HALO - 4 + j]
        out[30 + j] = e1[3, HALO + 58 + j]


def rest(g, s, co, u_in, rs_in, e0_in, e1_in, u, rs, e0, e1, e2, send, tmp):
    del u_in, rs_in, e0_in, e1_in
    beside = beside_maker()
    st = Stages(beside, co)
    sweep(-10, 74, 90, st.fine_defect(tmp, g, lambda t, r: g[t - 1, r], s, (1, 2)))
    sweep(-9, 73, 90, st.smoothed(u, g, tmp, (1, 2), Q))
    sweep(-8, 72, 90, st.restricted(rs, tmp, u, lambda t, r: u[t - 1, r], s, (1,)))
    sweep(-7, 71, 90, st.smoothed(e0, None, tmp, (1,), KQ))
    sweep(-6, 70, 90, st.coarse_defect(tmp, e0, lambda m, r: e0[m - 1, r], rs, (2,)))
    sweep(-5, 69, 90, st.smoothed(e1, e0, tmp, (2,), KQ))
    sweep(-4, 68, 90, st.coarse_defect(tmp, e1, lambda m, r: e1[m - 1, r], rs, (3,)))
    smooth = st.smoothed(e2, e1, tmp, (3,), KQ)

    def final(r):
        smooth(r)
        send[r - (HALO - 3)] = e2[3, r]

    sweep(-3, 67, 90, final)


def relay(is_odd, t0, near, far):
    odd = is_odd[0]
    for out, side in ((near, 1 - odd), (far, odd)):
        for j in range(10):
            out[j] = t0[54 * side + j]
        for j in range(9):
            out[10 + j] = t0[ROWS + 55 * side + j]


def middle(
    is_odd, t0, near, far, g, s, co, u_in, rs_in, e0_in, e1_in, e2_in,
    u, rs, e0, e1, e2, before, sol7, send, gb, er, br, tmp, u2,
):
    del u_in, rs_in, e0_in, e1_in, e2_in
    beside = beside_maker()
    st = Stages(beside, co)
    odd = is_odd[0]

    for r in range(ROWS):
        gb[0, HALO + r] = t0[r]
        br[0, HALO + r] = t0[ROWS + r]
    for source, side in ((near, 1 - odd), (far, odd)):
        for j in range(10):
            gb[0, 1 + 74 * side + j] = source[j]
        for j in range(9):
            br[0, 2 + 73 * side + j] = source[10 + j]

    def earlier_defect(r):
        er[0, r] = (br[0, r] - co[D, r] * gb[0, r] + co[C, r] * around(beside, gb, 0, r)) * co[INV, r]

    def earlier_smooth(r):
        value = gb[0, r] + er[0, r] + co[Q, r] * around(beside, er, 0, r)
        before[r] = value + co[ST, r]

    sweep(-9, 73, 90, earlier_defect)
    sweep(-8, 72, 90, earlier_smooth)
    sweep(-10, 74, 90, st.fine_defect(tmp, g, lambda t, r: gb[0, r] + co[ST, r], s, (0,)))
    sweep(-9, 73, 90, st.smoothed(u, g, tmp, (0,), Q))
    sweep(-8, 72, 90, st.restricted(rs, tmp, u, lambda t, r: u[0, r] if t else before[r], s, (0,)))
    sweep(-7, 71, 90, st.smoothed(e0, None, tmp, (0,), KQ))
    sweep(-6, 70, 90, st.coarse_defect(tmp, e0, lambda m, r: e0[0, r], rs, (1,)))
    sweep(-5, 69, 90, st.smoothed(e1, e0, tmp, (1,), KQ))
    sweep(-4, 68, 90, st.coarse_defect(tmp, e1, lambda m, r: e1[1, r], rs, (2,)))

    def corrected(r):
        q = co[KQ, r]
        late = e1[2, r] + tmp[2, r] + q * around(beside, tmp, 2, r)
        e2[2, r] = late
        u2[0, r] = u[6, r] + 0.5 * (late + e2[3, r])
        u2[1, r] = u[7, r] + e2[3, r]

    sweep(-3, 67, 90, corrected)

    def defect(r):
        tmp[0, r] = (
            s[7, r] + u2[0, r] - co[D, r] * u2[1, r] + co[C, r] * around(beside, u2, 1, r)
        ) * co[INV, r]

    sweep(-2, 66, 90, defect)

    def final(r):
        sol7[0, r] = u2[1, r] + tmp[0, r] + co[Q, r] * around(beside, tmp, 0, r)

    sweep(-1, 65, 90, final)

    def copy(i, carry):
        for j in range(8):
            send[tile_at(0, i, j), :] = sol7[0, HALO + 8 * i + j]
        return carry

    lax.fori_loop(0, ROWS // 8, copy, 0)


def late(
    t2, t2e, s, co, u, rs, e0, e1_in, e2_in, sol7, sol_out, res_out, u2_out, sol2, e1, u2, tmp, sol, sol_nat, res_nat, sems
):
    beside = beside_maker()
    st = Stages(beside, co)

    def old0(r):
        r -= HALO
        return t2[r - 4] if 4 <= r < 60 else t2e[r + 6 if r < 4 else r - 50]

    def old1(r):
        r -= HALO
        return t2[50 + r] if 6 <= r < 58 else t2e[r + 24 if r < 6 else r - 28]

    def first_defect(r):
        tmp[0, r] = (
            rs[0, r] + old0(r) - co[KD, r] * e0[0, r] + co[K, r] * around(beside, e0, 0, r)
        ) * co[KINV, r]

    sweep(-6, 70, 90, first_defect)

    def first_smooth(r):
        e1[0, r] = e0[0, r] + tmp[0, r] + co[KQ, r] * around(beside, tmp, 0, r)
        e1[1, r] = e1_in[1, r]

    sweep(-5, 69, 90, first_smooth)

    def second_defect(r):
        k, kd, kinv = co[K, r], co[KD, r], co[KINV, r]
        earlier = (old1(r), e1[0, r])
        for m in (0, 1):
            tmp[m, r] = (rs[m, r] + earlier[m] - kd * e1[m, r] + k * around(beside, e1, m, r)) * kinv

    sweep(-4, 68, 90, second_defect)

    def corrected(r):
        q = co[KQ, r]
        e20 = e1[0, r] + tmp[0, r] + q * around(beside, tmp, 0, r)
        e21 = e1[1, r] + tmp[1, r] + q * around(beside, tmp, 1, r)
        e22, e23 = e2_in[2, r], e2_in[3, r]
        u2_out[0, r] = u[0, r] + 0.5 * e20
        first = u[1, r] + e20
        u2_out[1, r] = first
        u2[1, r] = first
        u2[2, r] = u[2, r] + 0.5 * (e20 + e21)
        u2[3, r] = u[3, r] + e21
        u2[4, r] = u[4, r] + 0.5 * (e21 + e22)
        u2[5, r] = u[5, r] + e22
        u2[6, r] = u[6, r] + 0.5 * (e22 + e23)

    sweep(-3, 67, 90, corrected)
    sweep(-2, 66, 90, st.fine_defect(tmp, u2, lambda t, r: u2[t - 1, r], s, range(2, 7)))
    final = st.smoothed(sol, u2, tmp, range(2, 7), Q)

    def final_all(r):
        final(r)
        sol[7, r] = sol7[0, r]
        sol2[0, r] = sol[2, r]

    sweep(-1, 0, 90, final_all)
    sweep(64, 65, 90, final_all)

    for i in range(ROWS // 8):
        for j in range(8):
            r = HALO + 8 * i + j
            final_all(r)
            for t in range(2, 8):
                sol_nat[t - 2, tile_at(0, i, j), :] = sol[t, r]
    copies = [pltpu.make_async_copy(sol_nat, sol_out.at[pl.ds(2, 6)], sems.at[0])]
    copies[0].start()
    for part in range(2):
        for i in range(4 * part, 4 * part + 4):
            for j in range(8):
                r = HALO + 8 * i + j
                c, d = co[C, r], co[D, r]
                for t in range(3, 8):
                    res_nat[t - 3, tile_at(0, i, j), :] = (
                        s[t, r] + sol[t - 1, r] - d * sol[t, r] + c * around(beside, sol, t, r)
                    )
        rows = pl.ds(part * ROWS * 4, ROWS * 4)
        copies.append(pltpu.make_async_copy(res_nat.at[:, rows], res_out.at[pl.ds(3, 5), rows], sems.at[1 + part]))
        copies[-1].start()
    for copy in copies:
        copy.wait()


def finish(t3, s, co, before, u2_in, sol2, sol_in, res_in, sol_out, res_out, base, u2, tmp, sol, sol_nat, res, sems):
    del sol_in, res_in
    beside = beside_maker()

    def corrected(r):
        boundary = t3[r - (HALO - 3)]
        u2[0, r] = before[r] + boundary
        u2[1, r] = u2_in[0, r] + 0.5 * boundary

    sweep(-3, 67, 90, corrected)

    def defect(r):
        c, d, inv = co[C, r], co[D, r], co[INV, r]
        tmp[0, r] = (s[0, r] + u2[0, r] - d * u2[1, r] + c * around(beside, u2, 1, r)) * inv
        tmp[1, r] = (s[1, r] + u2[1, r] - d * u2_in[1, r] + c * around(beside, u2_in, 1, r)) * inv

    sweep(-2, 66, 90, defect)

    def final(r):
        q = co[Q, r]
        sol[0, r] = u2[1, r] + tmp[0, r] + q * around(beside, tmp, 0, r)
        sol[1, r] = u2_in[1, r] + tmp[1, r] + q * around(beside, tmp, 1, r)
        if HALO <= r < HALO + ROWS:
            sol_nat[0, tile_at(0, (r - HALO) // 8, (r - HALO) % 8), :] = sol[0, r]
            sol_nat[1, tile_at(0, (r - HALO) // 8, (r - HALO) % 8), :] = sol[1, r]

    sweep(-1, 65, 90, final)

    copies = [pltpu.make_async_copy(sol_nat, sol_out.at[pl.ds(0, 2)], sems.at[0])]
    copies[0].start()
    for i in range(ROWS // 8):
        for j in range(8):
            r = HALO + 8 * i + j
            c, d = co[C, r], co[D, r]
            first, second = sol[0, r], sol[1, r]
            spot = tile_at(0, i, j)
            base[spot, :] = s[0, r] + co[ST, r] - d * first + c * around(beside, sol, 0, r)
            res[0, spot, :] = s[1, r] + first - d * second + c * around(beside, sol, 1, r)
            res[1, spot, :] = s[2, r] + second - d * sol2[0, r] + c * around(beside, sol2, 0, r)
    copies.append(pltpu.make_async_copy(res, res_out.at[pl.ds(1, 2)], sems.at[1]))
    copies[1].start()
    for copy in copies:
        copy.wait()


def tail(t4, base, res_in, res_out, total, sem):
    del res_in
    total[0] = base[...] + t4[...]
    copy = pltpu.make_async_copy(total, res_out.at[pl.ds(0, 1)], sem)
    copy.start()
    copy.wait()


def call(kernel, ins, outs, scratch=(), aliases=None, specs=None, out_specs=None, limit=24):
    return pl.pallas_call(
        kernel,
        out_shape=outs,
        in_specs=specs or [FULL] * len(ins),
        out_specs=out_specs or [FULL] * len(outs),
        scratch_shapes=list(scratch),
        input_output_aliases=aliases or {},
        compiler_params=pltpu.CompilerParams(vmem_limit_bytes=limit * 2**20),
    )(*ins)


def along(block, axis, route):
    count = lax.axis_size(axis)
    pairs = [(i, route(i)) for i in range(count)]
    return lax.ppermute(block, axis, [(i, j) for i, j in pairs if 0 <= j < count])


def ahead(i):
    return i + 1


def on_chip(i):
    return i ^ 1


def off_chip(i):
    return ((i + 1) ^ 1) - 1


def cycle(source, guess, start_state, conduct):
    is_first = (lax.axis_index("tm") == 0).astype(F32).reshape(1)
    is_odd = (lax.axis_index("space") % 2).astype(jnp.int32).reshape(1)
    guess_v, source_v = view(guess), view(source)
    start_v, conduct_v = view(start_state[None]), view(conduct[None])
    vmem = lambda steps: pltpu.VMEM((steps, EXT, 8, 128), F32)
    dma = pltpu.SemaphoreType.DMA
    one = jax.ShapeDtypeStruct((ROWS * 8, 128), F32)

    by_step = lambda x: pltpu.with_memory_space_constraint(x.reshape(-1, ROWS * 8, 128), pltpu.HBM)
    stepped = lambda steps: jax.ShapeDtypeStruct((steps, ROWS * 8, 128), F32)
    near, far, guess_v, source_v, start_v, conduct_v = call(
        edge_pack,
        (is_first, is_odd, by_step(guess_v), by_step(source_v), by_step(start_v), by_step(conduct_v)),
        [rows_of(188), rows_of(188), stepped(8), stepped(8), stepped(1), stepped(1)],
        [dma((4, 3))],
        specs=[SMEM, SMEM] + [ANY] * 4,
        limit=1,
    )
    guess_v, source_v, start_v, conduct_v = (x.reshape(-1, 128) for x in (guess_v, source_v, start_v, conduct_v))
    (send0,) = call(last_step_pack, (guess_v, source_v), [rows_of(128)], limit=1)
    t0 = along(send0, "tm", ahead)
    far_in = along(far, "space", off_chip)
    near_in = along(near, "space", on_chip)
    g, s, co, u, rs, e0, e1, send2 = call(
        interior,
        (is_first, guess_v, source_v, start_v, conduct_v),
        [ext(8), ext(8), ext(9), ext(8), ext(4), ext(4), ext(4), rows_of(108)],
        [vmem(8)],
        specs=[SMEM] + [FULL] * 4,
        limit=6,
    )
    t2 = along(send2, "tm", ahead)
    near, far = call(relay, (is_odd, t0), [rows_of(19), rows_of(19)], specs=[SMEM, FULL], limit=1)
    far_relayed = along(far, "space", off_chip)
    near_relayed = along(near, "space", on_chip)
    g, s, co, u, rs, e0, e1, send2e = call(
        edges,
        (is_odd, near_in, far_in, g, s, co, u, rs, e0, e1),
        [ext(8), ext(8), ext(9), ext(8), ext(4), ext(4), ext(4), rows_of(40)],
        [vmem(8)],
        aliases={n + 3: n for n in range(7)},
        specs=[SMEM] + [FULL] * 9,
        limit=6,
    )
    t2e = along(send2e, "tm", ahead)
    u, rs, e0, e1, e2, send3 = call(
        rest,
        (g, s, co, u, rs, e0, e1),
        [ext(8), ext(4), ext(4), ext(4), ext(4), rows_of(70)],
        [vmem(4)],
        aliases={n + 3: n for n in range(4)},
        limit=6,
    )
    t3 = along(send3, "tm", ahead)
    u, rs, e0, e1, e2, before, sol7, send4 = call(
        middle,
        (is_odd, t0, near_relayed, far_relayed, g, s, co, u, rs, e0, e1, e2),
        [ext(8), ext(4), ext(4), ext(4), ext(4), rows_of(EXT), ext(1), one],
        [vmem(1), vmem(1), vmem(1), vmem(4), vmem(2)],
        aliases={n + 7: n for n in range(5)},
        specs=[SMEM] + [FULL] * 11,
        limit=6,
    )
    t4 = along(send4, "tm", ahead)
    nat3 = lambda steps: pltpu.VMEM((steps, ROWS * 8, 128), F32)
    sol, res, u2, sol2 = call(
        late,
        (t2, t2e, s, co, u, rs, e0, e1, e2, sol7),
        [stepped(8), stepped(8), ext(2), ext(1)],
        [vmem(2), vmem(8), vmem(8), vmem(8), nat3(6), nat3(5), dma((3,))],
        out_specs=[ANY, ANY, FULL, FULL],
        limit=16,
    )
    sol, res, base = call(
        finish,
        (t3, s, co, before, u2, sol2, sol, res),
        [stepped(8), stepped(8), jax.ShapeDtypeStruct((ROWS * 8, 128), F32)],
        [vmem(2), vmem(2), vmem(2), nat3(2), nat3(2), dma((2,))],
        aliases={6: 0, 7: 1},
        specs=[FULL] * 6 + [ANY] * 2,
        out_specs=[ANY, ANY, FULL],
        limit=6,
    )
    (res,) = call(
        tail,
        (t4, base, res),
        [stepped(8)],
        [nat3(1), dma],
        aliases={2: 0},
        specs=[FULL, FULL, ANY],
        out_specs=[ANY],
        limit=2,
    )
    return unview(sol, 8), unview(res, 8)


def solution(mesh):
    return jax.shard_map(
        cycle,
        mesh=mesh,
        in_specs=(P("tm", "space", None), P("tm", "space", None), P("space", None), P("space", None)),
        out_specs=(P("tm", "space", None), P("tm", "space", None)),
        check_vma=False,
    )
```

```python
import jax
import jax.numpy as jnp
from jax import lax
from jax.experimental import pallas as pl
from jax.experimental.pallas import tpu as pltpu
from jax.sharding import PartitionSpec as P


F32 = jnp.float32
ROWS = 64
HALO = 11
EXT = ROWS + 2 * HALO
DAMP = 0.8
C, D, INV, Q, K, KD, KINV, KQ, ST = range(9)
FULL = pl.BlockSpec(memory_space=pltpu.VMEM)
SMEM = pl.BlockSpec(memory_space=pltpu.SMEM)
ANY = pl.BlockSpec(memory_space=pltpu.HBM)


def ext(steps):
    return jax.ShapeDtypeStruct((steps, EXT, 8, 128), F32)


def rows_of(count):
    return jax.ShapeDtypeStruct((count, 8, 128), F32)


def view(x):
    steps = x.shape[0]
    return x.reshape(steps, ROWS // 8, 8, 8, 128).transpose(0, 1, 3, 2, 4).reshape(steps * ROWS * 8, 128)


def unview(y, steps):
    return y.reshape(steps, ROWS // 8, 8, 8, 128).transpose(0, 1, 3, 2, 4).reshape(steps, ROWS, 1024)


def tile_at(step, tile, row):
    return pl.ds(step * ROWS * 8 + tile * 64 + row, 8, 8)


def beside_maker():
    lane = lax.broadcasted_iota(jnp.int32, (8, 128), 1)
    sub = lax.broadcasted_iota(jnp.int32, (8, 128), 0)
    first, last = lane == 0, lane == 127
    top, bottom = sub == 0, sub == 7

    def beside(x):
        before = jnp.where(top, 0.0, pltpu.roll(x, 1, 0))
        after = jnp.where(bottom, 0.0, pltpu.roll(x, 7, 0))
        return pltpu.roll(jnp.where(last, before, x), 1, 1) + pltpu.roll(jnp.where(first, after, x), 127, 1)

    return beside


def around(beside, ref, step, r):
    return ref[step, r - 1] + ref[step, r + 1] + beside(ref[step, r])


def sweep(low, high, unroll, body):
    low, high = low + HALO, high + HALO
    count = high - low
    unroll = min(unroll, count)
    blocks = -(-count // unroll)
    if blocks == 1:
        for j in range(unroll):
            body(low + j)
        return

    def step(i, carry):
        start = jnp.minimum(low + i * unroll, high - unroll)
        for j in range(unroll):
            body(start + j)
        return carry

    lax.fori_loop(0, blocks, step, 0)


def coefficients(co, r, c):
    diag = 1.0 + 4.0 * c
    coarse = 1.0 + 8.0 * c
    recip = 1.0 / diag
    coarse_recip = 1.0 / coarse
    co[C, r] = c
    co[D, r] = diag
    co[INV, r] = DAMP * recip
    co[Q, r] = c * recip
    co[K, r] = 2.0 * c
    co[KD, r] = coarse
    co[KINV, r] = DAMP * coarse_recip
    co[KQ, r] = 2.0 * c * coarse_recip


class Stages:
    def __init__(self, beside, co):
        self.beside, self.co = beside, co

    def fine_defect(self, out, field, earlier, source, steps):
        def body(r):
            c, d, inv = self.co[C, r], self.co[D, r], self.co[INV, r]
            for t in steps:
                out[t, r] = (source[t, r] + earlier(t, r) - d * field[t, r] + c * around(self.beside, field, t, r)) * inv

        return body

    def coarse_defect(self, out, field, earlier, rhs, steps):
        def body(r):
            k, kd, kinv = self.co[K, r], self.co[KD, r], self.co[KINV, r]
            for m in steps:
                out[m, r] = (rhs[m, r] + earlier(m, r) - kd * field[m, r] + k * around(self.beside, field, m, r)) * kinv

        return body

    def smoothed(self, out, field, defect, steps, plane):
        def body(r):
            q = self.co[plane, r]
            for t in steps:
                base = defect[t, r] if field is None else field[t, r] + defect[t, r]
                out[t, r] = base + q * around(self.beside, defect, t, r)

        return body

    def restricted(self, out, scaled, field, earlier, source, pairs):
        def body(r):
            c, d, kinv = self.co[C, r], self.co[D, r], self.co[KINV, r]
            for m in pairs:
                parts = [
                    source[t, r] + earlier(t, r) - d * field[t, r] + c * around(self.beside, field, t, r)
                    for t in (2 * m, 2 * m + 1)
                ]
                both = parts[0] + parts[1]
                out[m, r] = both
                scaled[m, r] = both * kinv

        return body


def edge_pack(
    is_first, is_odd, guess, source, start, conduct, near, far, gb, sb, tb, cb, sems
):
    pairs = ((guess, gb), (source, sb), (start, tb), (conduct, cb))

    def copies(spans):
        return [
            pltpu.make_async_copy(src.at[:, pl.ds(low, size)], dst.at[:, pl.ds(low, size)], sems.at[n, k])
            for k, low, size in spans
            for n, (src, dst) in enumerate(pairs)
        ]

    outer_tiles, inner_tiles = copies(((0, 0, 128), (1, 384, 128))), copies(((2, 128, 256),))
    for copy in outer_tiles + inner_tiles:
        copy.start()
    for copy in outer_tiles:
        copy.wait()
    odd = is_odd[0]

    def grab(out, base, ref, t, low, count, scale=None):
        def body(j, carry):
            r = low + j
            value = ref[t, pl.ds((r // 8) * 64 + r % 8, 8, 8), :]
            out[base + j] = value if scale is None else value * scale
            return carry

        lax.fori_loop(0, count, body, 0, unroll=True)

    for out, side in ((near, 1 - odd), (far, odd)):
        for t in range(8):
            grab(out, t * 11, gb, t, 53 * side, 11)
            grab(out, 88 + t * 10, sb, t, 54 * side, 10)
        grab(out, 168, cb, 0, 54 * side, 10)
        grab(out, 178, tb, 0, 54 * side, 10, is_first[0])
    for copy in inner_tiles:
        copy.wait()


def last_step_pack(guess, source, out):
    for i in range(ROWS // 8):
        for j in range(8):
            r = 8 * i + j
            out[r] = guess[tile_at(7, i, j), :]
            out[ROWS + r] = source[tile_at(7, i, j), :] + guess[tile_at(6, i, j), :]


def interior(is_first, guess, source, start, conduct, g, s, co, u, rs, e0, e1, send, tmp):
    beside = beside_maker()

    def fill(i, carry):
        for j in range(8):
            r = HALO + 8 * i + j
            for t in range(8):
                g[t, r] = guess[tile_at(t, i, j), :]
                s[t, r] = source[tile_at(t, i, j), :]
            coefficients(co, r, conduct[tile_at(0, i, j), :])
            co[ST, r] = start[tile_at(0, i, j), :] * is_first[0]
        return carry

    lax.fori_loop(0, ROWS // 8, fill, 0)
    st = Stages(beside, co)
    sweep(1, 63, 90, st.fine_defect(tmp, g, lambda t, r: g[t - 1, r], s, range(3, 8)))
    sweep(2, 62, 90, st.smoothed(u, g, tmp, range(3, 8), Q))
    sweep(3, 61, 90, st.restricted(rs, tmp, u, lambda t, r: u[t - 1, r], s, (2, 3)))
    sweep(4, 60, 90, st.smoothed(e0, None, tmp, (2, 3), KQ))
    sweep(5, 59, 90, st.coarse_defect(tmp, e0, lambda m, r: e0[m - 1, r], rs, (3,)))
    sweep(6, 58, 90, st.smoothed(e1, e0, tmp, (3,), KQ))
    for r in range(4, 60):
        send[r - 4] = e0[3, HALO + r]
    for r in range(6, 58):
        send[50 + r] = e1[3, HALO + r]


def both(inner, depth, body):
    sweep(-depth, inner, 99, body)
    sweep(ROWS - inner, ROWS + depth, 99, body)


def scaled(co, rs, tmp, pairs=(2, 3)):
    def body(r):
        for m in pairs:
            tmp[m, r] = rs[m, r] * co[KINV, r]

    return body


def edges(is_odd, near, far, g_in, s_in, co_in, u_in, rs_in, e0_in, e1_in, g, s, co, u, rs, e0, e1, out, tmp):
    del g_in, s_in, co_in, u_in, rs_in, e0_in, e1_in
    beside = beside_maker()
    odd = is_odd[0]
    for source, side in ((near, 1 - odd), (far, odd)):
        for j in range(11):
            for t in range(8):
                g[t, 75 * side + j] = source[t * 11 + j]
        for j in range(10):
            for t in range(8):
                s[t, 1 + 74 * side + j] = source[88 + t * 10 + j]
            coefficients(co, 1 + 74 * side + j, source[168 + j])
            co[ST, 1 + 74 * side + j] = source[178 + j]
    st = Stages(beside, co)
    both(3, 10, st.fine_defect(tmp, g, lambda t, r: g[t - 1, r], s, range(3, 8)))
    both(2, 9, st.smoothed(u, g, tmp, range(3, 8), Q))
    both(3, 8, st.restricted(rs, tmp, u, lambda t, r: u[t - 1, r], s, (2, 3)))
    both(5, -3, scaled(co, rs, tmp))
    both(4, 7, st.smoothed(e0, None, tmp, (2, 3), KQ))
    both(7, 6, st.coarse_defect(tmp, e0, lambda m, r: e0[m - 1, r], rs, (3,)))
    both(6, 5, st.smoothed(e1, e0, tmp, (3,), KQ))
    for j in range(10):
        out[j] = e0[3, HALO - 6 + j]
        out[10 + j] = e0[3, HALO + 60 + j]
        out[20 + j] = e1[3, HALO - 4 + j]
        out[30 + j] = e1[3, HALO + 58 + j]


def rest_inner(g, s, co, u_in, rs_in, e0_in, u, rs, e0, tmp):
    del u_in, rs_in, e0_in
    st = Stages(beside_maker(), co)
    sweep(1, 63, 90, st.fine_defect(tmp, g, lambda t, r: g[t - 1, r], s, (1, 2)))
    sweep(2, 62, 90, st.smoothed(u, g, tmp, (1, 2), Q))
    sweep(3, 61, 90, st.restricted(rs, tmp, u, lambda t, r: u[t - 1, r], s, (1,)))
    sweep(4, 60, 90, st.smoothed(e0, None, tmp, (1,), KQ))


def rest(g, s, co, u_in, rs_in, e0_in, e1_in, u, rs, e0, e1, e2, send, tmp):
    del u_in, rs_in, e0_in, e1_in
    beside = beside_maker()
    st = Stages(beside, co)
    both(3, 10, st.fine_defect(tmp, g, lambda t, r: g[t - 1, r], s, (1, 2)))
    both(2, 9, st.smoothed(u, g, tmp, (1, 2), Q))
    both(3, 8, st.restricted(rs, tmp, u, lambda t, r: u[t - 1, r], s, (1,)))
    both(5, -3, scaled(co, rs, tmp, (1,)))
    both(4, 7, st.smoothed(e0, None, tmp, (1,), KQ))
    sweep(-6, 70, 90, st.coarse_defect(tmp, e0, lambda m, r: e0[m - 1, r], rs, (2,)))
    sweep(-5, 69, 90, st.smoothed(e1, e0, tmp, (2,), KQ))
    sweep(-4, 68, 90, st.coarse_defect(tmp, e1, lambda m, r: e1[m - 1, r], rs, (3,)))
    smooth = st.smoothed(e2, e1, tmp, (3,), KQ)

    def final(r):
        smooth(r)
        send[r - (HALO - 3)] = e2[3, r]

    sweep(-3, 67, 90, final)


def relay(is_odd, t0, near, far):
    odd = is_odd[0]
    for out, side in ((near, 1 - odd), (far, odd)):
        for j in range(10):
            out[j] = t0[54 * side + j]
        for j in range(9):
            out[10 + j] = t0[ROWS + 55 * side + j]


def middle(
    is_odd, t0, near, far, g, s, co, u_in, rs_in, e0_in, e1_in, e2_in,
    u, rs, e0, e1, e2, before, sol7, send, gb, er, br, tmp, u2,
):
    del u_in, rs_in, e0_in, e1_in, e2_in
    beside = beside_maker()
    st = Stages(beside, co)
    odd = is_odd[0]

    for r in range(ROWS):
        gb[0, HALO + r] = t0[r]
        br[0, HALO + r] = t0[ROWS + r]
    for source, side in ((near, 1 - odd), (far, odd)):
        for j in range(10):
            gb[0, 1 + 74 * side + j] = source[j]
        for j in range(9):
            br[0, 2 + 73 * side + j] = source[10 + j]

    def earlier_defect(r):
        er[0, r] = (br[0, r] - co[D, r] * gb[0, r] + co[C, r] * around(beside, gb, 0, r)) * co[INV, r]

    def earlier_smooth(r):
        value = gb[0, r] + er[0, r] + co[Q, r] * around(beside, er, 0, r)
        before[r] = value + co[ST, r]

    sweep(-9, 73, 90, earlier_defect)
    sweep(-8, 72, 90, earlier_smooth)
    sweep(-10, 74, 90, st.fine_defect(tmp, g, lambda t, r: gb[0, r] + co[ST, r], s, (0,)))
    sweep(-9, 73, 90, st.smoothed(u, g, tmp, (0,), Q))
    sweep(-8, 72, 90, st.restricted(rs, tmp, u, lambda t, r: u[0, r] if t else before[r], s, (0,)))
    sweep(-7, 71, 90, st.smoothed(e0, None, tmp, (0,), KQ))
    sweep(-6, 70, 90, st.coarse_defect(tmp, e0, lambda m, r: e0[0, r], rs, (1,)))
    sweep(-5, 69, 90, st.smoothed(e1, e0, tmp, (1,), KQ))
    sweep(-4, 68, 90, st.coarse_defect(tmp, e1, lambda m, r: e1[1, r], rs, (2,)))

    def corrected(r):
        q = co[KQ, r]
        late = e1[2, r] + tmp[2, r] + q * around(beside, tmp, 2, r)
        e2[2, r] = late
        u2[0, r] = u[6, r] + 0.5 * (late + e2[3, r])
        u2[1, r] = u[7, r] + e2[3, r]

    sweep(-3, 67, 90, corrected)

    def defect(r):
        tmp[0, r] = (
            s[7, r] + u2[0, r] - co[D, r] * u2[1, r] + co[C, r] * around(beside, u2, 1, r)
        ) * co[INV, r]

    sweep(-2, 66, 90, defect)

    def final(r):
        sol7[0, r] = u2[1, r] + tmp[0, r] + co[Q, r] * around(beside, tmp, 0, r)

    sweep(-1, 65, 90, final)

    def copy(i, carry):
        for j in range(8):
            send[tile_at(0, i, j), :] = sol7[0, HALO + 8 * i + j]
        return carry

    lax.fori_loop(0, ROWS // 8, copy, 0)


def late(
    t2, t2e, s, co, u, rs, e0, e1_in, e2_in, sol7, sol_out, res_out, u2_out, sol2, e1, u2, tmp, sol, sol_nat, res_nat, sems
):
    beside = beside_maker()
    st = Stages(beside, co)

    def old0(r):
        r -= HALO
        return t2[r - 4] if 4 <= r < 60 else t2e[r + 6 if r < 4 else r - 50]

    def old1(r):
        r -= HALO
        return t2[50 + r] if 6 <= r < 58 else t2e[r + 24 if r < 6 else r - 28]

    def first_defect(r):
        tmp[0, r] = (
            rs[0, r] + old0(r) - co[KD, r] * e0[0, r] + co[K, r] * around(beside, e0, 0, r)
        ) * co[KINV, r]

    sweep(-6, 70, 90, first_defect)

    def first_smooth(r):
        e1[0, r] = e0[0, r] + tmp[0, r] + co[KQ, r] * around(beside, tmp, 0, r)
        e1[1, r] = e1_in[1, r]

    sweep(-5, 69, 90, first_smooth)

    def second_defect(r):
        k, kd, kinv = co[K, r], co[KD, r], co[KINV, r]
        earlier = (old1(r), e1[0, r])
        for m in (0, 1):
            tmp[m, r] = (rs[m, r] + earlier[m] - kd * e1[m, r] + k * around(beside, e1, m, r)) * kinv

    sweep(-4, 68, 90, second_defect)

    def corrected(r):
        q = co[KQ, r]
        e20 = e1[0, r] + tmp[0, r] + q * around(beside, tmp, 0, r)
        e21 = e1[1, r] + tmp[1, r] + q * around(beside, tmp, 1, r)
        e22, e23 = e2_in[2, r], e2_in[3, r]
        u2_out[0, r] = u[0, r] + 0.5 * e20
        first = u[1, r] + e20
        u2_out[1, r] = first
        u2[1, r] = first
        u2[2, r] = u[2, r] + 0.5 * (e20 + e21)
        u2[3, r] = u[3, r] + e21
        u2[4, r] = u[4, r] + 0.5 * (e21 + e22)
        u2[5, r] = u[5, r] + e22
        u2[6, r] = u[6, r] + 0.5 * (e22 + e23)

    sweep(-3, 67, 90, corrected)
    sweep(-2, 66, 90, st.fine_defect(tmp, u2, lambda t, r: u2[t - 1, r], s, range(2, 7)))
    final = st.smoothed(sol, u2, tmp, range(2, 7), Q)

    def final_all(r):
        final(r)
        sol[7, r] = sol7[0, r]
        sol2[0, r] = sol[2, r]

    sweep(-1, 0, 90, final_all)
    sweep(64, 65, 90, final_all)

    for i in range(ROWS // 8):
        for j in range(8):
            r = HALO + 8 * i + j
            final_all(r)
            for t in range(2, 8):
                sol_nat[t - 2, tile_at(0, i, j), :] = sol[t, r]
    copies = [pltpu.make_async_copy(sol_nat, sol_out.at[pl.ds(2, 6)], sems.at[0])]
    copies[0].start()
    for part in range(2):
        for i in range(4 * part, 4 * part + 4):
            for j in range(8):
                r = HALO + 8 * i + j
                c, d = co[C, r], co[D, r]
                for t in range(3, 8):
                    res_nat[t - 3, tile_at(0, i, j), :] = (
                        s[t, r] + sol[t - 1, r] - d * sol[t, r] + c * around(beside, sol, t, r)
                    )
        rows = pl.ds(part * ROWS * 4, ROWS * 4)
        copies.append(pltpu.make_async_copy(res_nat.at[:, rows], res_out.at[pl.ds(3, 5), rows], sems.at[1 + part]))
        copies[-1].start()
    for copy in copies:
        copy.wait()


def finish(t3, s, co, before, u2_in, sol2, sol_in, res_in, sol_out, res_out, base, u2, tmp, sol, sol_nat, res, sems):
    del sol_in, res_in
    beside = beside_maker()

    def corrected(r):
        boundary = t3[r - (HALO - 3)]
        u2[0, r] = before[r] + boundary
        u2[1, r] = u2_in[0, r] + 0.5 * boundary

    sweep(-3, 67, 90, corrected)

    def defect(r):
        c, d, inv = co[C, r], co[D, r], co[INV, r]
        tmp[0, r] = (s[0, r] + u2[0, r] - d * u2[1, r] + c * around(beside, u2, 1, r)) * inv
        tmp[1, r] = (s[1, r] + u2[1, r] - d * u2_in[1, r] + c * around(beside, u2_in, 1, r)) * inv

    sweep(-2, 66, 90, defect)

    def final(r):
        q = co[Q, r]
        sol[0, r] = u2[1, r] + tmp[0, r] + q * around(beside, tmp, 0, r)
        sol[1, r] = u2_in[1, r] + tmp[1, r] + q * around(beside, tmp, 1, r)
        if HALO <= r < HALO + ROWS:
            sol_nat[0, tile_at(0, (r - HALO) // 8, (r - HALO) % 8), :] = sol[0, r]
            sol_nat[1, tile_at(0, (r - HALO) // 8, (r - HALO) % 8), :] = sol[1, r]

    sweep(-1, 65, 90, final)

    copies = [pltpu.make_async_copy(sol_nat, sol_out.at[pl.ds(0, 2)], sems.at[0])]
    copies[0].start()
    for i in range(ROWS // 8):
        for j in range(8):
            r = HALO + 8 * i + j
            c, d = co[C, r], co[D, r]
            first, second = sol[0, r], sol[1, r]
            spot = tile_at(0, i, j)
            base[spot, :] = s[0, r] + co[ST, r] - d * first + c * around(beside, sol, 0, r)
            res[0, spot, :] = s[1, r] + first - d * second + c * around(beside, sol, 1, r)
            res[1, spot, :] = s[2, r] + second - d * sol2[0, r] + c * around(beside, sol2, 0, r)
    copies.append(pltpu.make_async_copy(res, res_out.at[pl.ds(1, 2)], sems.at[1]))
    copies[1].start()
    for copy in copies:
        copy.wait()


def tail(t4, base, res_in, res_out, total, sem):
    del res_in
    total[0] = base[...] + t4[...]
    copy = pltpu.make_async_copy(total, res_out.at[pl.ds(0, 1)], sem)
    copy.start()
    copy.wait()


def call(kernel, ins, outs, scratch=(), aliases=None, specs=None, out_specs=None, limit=24):
    return pl.pallas_call(
        kernel,
        out_shape=outs,
        in_specs=specs or [FULL] * len(ins),
        out_specs=out_specs or [FULL] * len(outs),
        scratch_shapes=list(scratch),
        input_output_aliases=aliases or {},
        compiler_params=pltpu.CompilerParams(vmem_limit_bytes=limit * 2**20),
    )(*ins)


def along(block, axis, route):
    count = lax.axis_size(axis)
    pairs = [(i, route(i)) for i in range(count)]
    return lax.ppermute(block, axis, [(i, j) for i, j in pairs if 0 <= j < count])


def ahead(i):
    return i + 1


def on_chip(i):
    return i ^ 1


def off_chip(i):
    return ((i + 1) ^ 1) - 1


def cycle(source, guess, start_state, conduct):
    is_first = (lax.axis_index("tm") == 0).astype(F32).reshape(1)
    is_odd = (lax.axis_index("space") % 2).astype(jnp.int32).reshape(1)
    guess_v, source_v = view(guess), view(source)
    start_v, conduct_v = view(start_state[None]), view(conduct[None])
    vmem = lambda steps: pltpu.VMEM((steps, EXT, 8, 128), F32)
    dma = pltpu.SemaphoreType.DMA
    one = jax.ShapeDtypeStruct((ROWS * 8, 128), F32)

    by_step = lambda x: pltpu.with_memory_space_constraint(x.reshape(-1, ROWS * 8, 128), pltpu.HBM)
    stepped = lambda steps: jax.ShapeDtypeStruct((steps, ROWS * 8, 128), F32)
    near, far, guess_v, source_v, start_v, conduct_v = call(
        edge_pack,
        (is_first, is_odd, by_step(guess_v), by_step(source_v), by_step(start_v), by_step(conduct_v)),
        [rows_of(188), rows_of(188), stepped(8), stepped(8), stepped(1), stepped(1)],
        [dma((4, 3))],
        specs=[SMEM, SMEM] + [ANY] * 4,
        limit=1,
    )
    guess_v, source_v, start_v, conduct_v = (x.reshape(-1, 128) for x in (guess_v, source_v, start_v, conduct_v))
    (send0,) = call(last_step_pack, (guess_v, source_v), [rows_of(128)], limit=1)
    t0 = along(send0, "tm", ahead)
    far_in = along(far, "space", off_chip)
    near_in = along(near, "space", on_chip)
    g, s, co, u, rs, e0, e1, send2 = call(
        interior,
        (is_first, guess_v, source_v, start_v, conduct_v),
        [ext(8), ext(8), ext(9), ext(8), ext(4), ext(4), ext(4), rows_of(108)],
        [vmem(8)],
        specs=[SMEM] + [FULL] * 4,
        limit=6,
    )
    t2 = along(send2, "tm", ahead)
    u, rs, e0 = call(
        rest_inner, (g, s, co, u, rs, e0), [ext(8), ext(4), ext(4)], [vmem(4)], aliases={3: 0, 4: 1, 5: 2}, limit=3
    )
    near, far = call(relay, (is_odd, t0), [rows_of(19), rows_of(19)], specs=[SMEM, FULL], limit=1)
    far_relayed = along(far, "space", off_chip)
    near_relayed = along(near, "space", on_chip)
    g, s, co, u, rs, e0, e1, send2e = call(
        edges,
        (is_odd, near_in, far_in, g, s, co, u, rs, e0, e1),
        [ext(8), ext(8), ext(9), ext(8), ext(4), ext(4), ext(4), rows_of(40)],
        [vmem(8)],
        aliases={n + 3: n for n in range(7)},
        specs=[SMEM] + [FULL] * 9,
        limit=6,
    )
    t2e = along(send2e, "tm", ahead)
    u, rs, e0, e1, e2, send3 = call(
        rest,
        (g, s, co, u, rs, e0, e1),
        [ext(8), ext(4), ext(4), ext(4), ext(4), rows_of(70)],
        [vmem(4)],
        aliases={n + 3: n for n in range(4)},
        limit=6,
    )
    t3 = along(send3, "tm", ahead)
    u, rs, e0, e1, e2, before, sol7, send4 = call(
        middle,
        (is_odd, t0, near_relayed, far_relayed, g, s, co, u, rs, e0, e1, e2),
        [ext(8), ext(4), ext(4), ext(4), ext(4), rows_of(EXT), ext(1), one],
        [vmem(1), vmem(1), vmem(1), vmem(4), vmem(2)],
        aliases={n + 7: n for n in range(5)},
        specs=[SMEM] + [FULL] * 11,
        limit=6,
    )
    t4 = along(send4, "tm", ahead)
    nat3 = lambda steps: pltpu.VMEM((steps, ROWS * 8, 128), F32)
    sol, res, u2, sol2 = call(
        late,
        (t2, t2e, s, co, u, rs, e0, e1, e2, sol7),
        [stepped(8), stepped(8), ext(2), ext(1)],
        [vmem(2), vmem(8), vmem(8), vmem(8), nat3(6), nat3(5), dma((3,))],
        out_specs=[ANY, ANY, FULL, FULL],
        limit=16,
    )
    sol, res, base = call(
        finish,
        (t3, s, co, before, u2, sol2, sol, res),
        [stepped(8), stepped(8), jax.ShapeDtypeStruct((ROWS * 8, 128), F32)],
        [vmem(2), vmem(2), vmem(2), nat3(2), nat3(2), dma((2,))],
        aliases={6: 0, 7: 1},
        specs=[FULL] * 6 + [ANY] * 2,
        out_specs=[ANY, ANY, FULL],
        limit=6,
    )
    (res,) = call(
        tail,
        (t4, base, res),
        [stepped(8)],
        [nat3(1), dma],
        aliases={2: 0},
        specs=[FULL, FULL, ANY],
        out_specs=[ANY],
        limit=2,
    )
    return unview(sol, 8), unview(res, 8)


def solution(mesh):
    return jax.shard_map(
        cycle,
        mesh=mesh,
        in_specs=(P("tm", "space", None), P("tm", "space", None), P("space", None), P("space", None)),
        out_specs=(P("tm", "space", None), P("tm", "space", None)),
        check_vma=False,
    )
```
